128 devices in a mesh: rb: 2 (over core), lb: 64 (over z, y, x).
Axes of the slice: x: 4, y: 4, z: 4, core: 2. Of those that a mesh axis runs over, the one named last changes fastest.
Arguments:
- psi_start: float32 [2, 1024, 2, 2, 1024], P(None, 'lb', None, None, 'rb')
- left_env: float32 [1024, 20, 1024], P('lb')
- right_env: float32 [1024, 20, 1024], P('rb')
- mpo_pair: float32 [20, 20, 2, 2, 2, 2], replicated
Outputs:
- output 1: float32 [2, 4], replicated
- output 2: float32 [2, 4], replicated
- output 3: float32 [2, 1024, 2, 2, 1024], P(None, 'lb', None, None, 'rb')
All inputs are finite; a program needn't handle non-finite values.
Results may differ from the reference program's by a relative error of at most 0.001.
Values sent between devices are 32-bit elements.
A program may use at most 1 GiB of HBM per device.

```python
import math
import jax
import jax.numpy as jnp
from jax import lax

BOND_DIM = 1024
PHYS_DIM = 2
MPO_DIM = 20
LANCZOS_STEPS = 4
TARGETS = 2
COL_BLOCK = min(BOND_DIM, 128)
MATMUL_PREC = lax.Precision.HIGHEST


def sym_env(key):
    key_mat, key_shift = jax.random.split(key)
    gauss = jax.random.normal(key_mat, (MPO_DIM, BOND_DIM, BOND_DIM), jnp.float32)
    shifts = jax.random.uniform(key_shift, (MPO_DIM, 1, 1), jnp.float32, 0.5, 1.5)
    sym_part = (gauss + jnp.swapaxes(gauss, 1, 2)) / math.sqrt(2.0 * BOND_DIM)
    env_mat = sym_part + shifts * jnp.eye(BOND_DIM, dtype=jnp.float32)
    return jnp.transpose(env_mat, (1, 0, 2))


def setup_inputs(seed: int = 0) -> dict:
    key_psi, key_left, key_right, key_mpo, key_diag = jax.random.split(jax.random.key(seed), 5)
    psi_start = jax.random.normal(key_psi, (TARGETS, BOND_DIM, PHYS_DIM, PHYS_DIM, BOND_DIM), jnp.float32)
    pair_dim = PHYS_DIM * PHYS_DIM
    gauss = jax.random.normal(key_mpo, (MPO_DIM, MPO_DIM, pair_dim, pair_dim), jnp.float32)
    sym_part = (gauss + jnp.swapaxes(gauss, 2, 3)) * (0.5 / (math.sqrt(2.0) * MPO_DIM * PHYS_DIM))
    diag_wts = jax.random.uniform(key_diag, (MPO_DIM, MPO_DIM, 1, 1), jnp.float32, 0.0, 3.0 / (MPO_DIM * MPO_DIM))
    mpo_flat = sym_part + diag_wts * jnp.eye(pair_dim, dtype=jnp.float32)
    mpo_pair = mpo_flat.reshape(MPO_DIM, MPO_DIM, PHYS_DIM, PHYS_DIM, PHYS_DIM, PHYS_DIM)
    return {"psi_start": psi_start, "left_env": sym_env(key_left), "right_env": sym_env(key_right), "mpo_pair": mpo_pair}


def apply_ham(in_vec, left_env, right_env, mpo_pair):
    num_blocks = BOND_DIM // COL_BLOCK
    vec_blocks = jnp.moveaxis(in_vec.reshape(BOND_DIM, PHYS_DIM, PHYS_DIM, num_blocks, COL_BLOCK), 3, 0)
    env_blocks = right_env.reshape(num_blocks, COL_BLOCK, MPO_DIM, BOND_DIM)

    def body(total_out, block_pair):
        vec_blk, env_blk = block_pair
        left_part = jnp.einsum("alc,aijb->lcijb", left_env, vec_blk, precision=MATMUL_PREC)
        mid_part = jnp.einsum("lrijmn,lcijb->rcmnb", mpo_pair, left_part, precision=MATMUL_PREC)
        return total_out + jnp.einsum("rcmnb,brd->cmnd", mid_part, env_blk, precision=MATMUL_PREC), None

    zero_out = jnp.zeros((BOND_DIM, PHYS_DIM, PHYS_DIM, BOND_DIM), jnp.float32)
    out_vec, unused = lax.scan(body, zero_out, (vec_blocks, env_blocks))
    return out_vec


def lanczos(start_vec, left_env, right_env, mpo_pair):
    first_vec = start_vec / jnp.sqrt(jnp.mean(start_vec * start_vec))

    def step(carry, unused):
        cur_vec, prev_vec, beta_prev = carry
        ham_vec = apply_ham(cur_vec, left_env, right_env, mpo_pair)
        alpha = jnp.mean(cur_vec * ham_vec)
        residual = ham_vec - alpha * cur_vec - beta_prev * prev_vec
        beta = jnp.sqrt(jnp.mean(residual * residual))
        return (residual / beta, cur_vec, beta), (alpha, beta)

    carry_init = (first_vec, jnp.zeros_like(first_vec), jnp.zeros((), jnp.float32))
    (last_vec, unused_prev, unused_beta), (alphas, betas) = lax.scan(step, carry_init, None, length=LANCZOS_STEPS)
    return alphas, betas, last_vec


def reference(psi_start, left_env, right_env, mpo_pair):
    alpha_vals, beta_vals, psi_next = lax.map(lambda start_vec: lanczos(start_vec, left_env, right_env, mpo_pair), psi_start)
    return alpha_vals, beta_vals, psi_next
```

```python
import functools

import jax
import jax.numpy as jnp
from jax import lax
from jax.experimental import pallas as pl
from jax.experimental.pallas import tpu as pltpu
from jax.sharding import PartitionSpec as P

STEPS = 4
HI = lax.Precision.HIGHEST
F32 = jnp.float32
BF16 = jnp.bfloat16
MESH = pl.DeviceIdType.MESH
LN = 128
EC = 64
PH = 4
WID = PH * LN
NX = 40
NY = 72
FAR = (7, 6, 5, 3)
NEAR = (4, 2, 1)
SEVEN = NEAR + FAR
ALPHA, BETA, NORM = range(3)
RS, GA, FW, PS, PF, FI, AG, AR, LD = range(9)
THIRDS = ((0, 4), (4, 3), (7, 3))
ORDERS = ((4, 2, 1), (2, 1, 4), (1, 4, 2))


def split3(val):
    top = val.astype(BF16)
    rest = val - top.astype(F32)
    mid = rest.astype(BF16)
    low = (rest - mid.astype(F32)).astype(BF16)
    return top, mid, low


def fold(val):
    acc = sum(val[:, j:j + LN] for j in range(0, val.shape[1], LN))
    return sum(acc[j:j + 8] for j in range(0, val.shape[0], 8))


def bits(m):
    return m // 4, (m // 2) % 2, m % 2


def number(trip, base=2):
    return (trip[0] * base + trip[1]) * base + trip[2]


def flip(trip, m):
    return number([q + b * (1 - 2 * q) for q, b in zip(trip, bits(m))])


def places(lb):
    place = (lb // 16, (lb // 4) % 4, lb % 4)
    return place, [q % 2 for q in place], [q // 2 for q in place], [((q + 1) // 2) % 2 for q in place]


def kernel(cfg, psi_ref, left_ref, right_ref, wmat_ref, psi_out, alpha_out, beta_out,
           rf, ls, lst, gat, vec, pg, praw, xf, yf, outb, rsb, wpk, gbuf, rbuf, asend, scal, fsend, frecv, ssem, rsem, l_s, l_r, lf_s, lf_r):
    bond, mpo, elems = cfg
    core, lb = lax.axis_index("rb"), lax.axis_index("lb")
    place, low, high, side = places(lb)
    pos, aset, eset = number(low), number(high), number(side)
    half = bond // 2
    own = pl.multiple_of(core * half + eset * EC, EC)
    other = 1 - core
    myrows = pl.ds(pl.multiple_of(pos * 16, 16), 16)
    mycols = pl.ds(pl.multiple_of(core * half, half), half)

    def gpeer(m):
        return number([q + b * (1 - 2 * p) for q, b, p in zip(place, bits(m), low)], 4)

    def rpeer(m):
        return number([q + b * (3 - 2 * q) for q, b in zip(place, bits(m))], 4)

    def remote(src, dst, ssm, rsm, c, chip):
        return pltpu.make_async_remote_copy(src_ref=src, dst_ref=dst, send_sem=ssm, recv_sem=rsm, device_id=(c, chip), device_id_type=MESH)

    def tagged(src, dst, kind, t, m, c, chip):
        return remote(src, dst, ssem.at[kind, t, m], rsem.at[kind, t, m], c, chip)

    def rs_copy(t, m):
        return tagged(outb.at[t, flip(high, m)], rsb.at[t, m], RS, t, m, core, rpeer(m))

    def g_copy(t, m):
        reg = gat.at[t, pl.ds(own, EC)]
        return tagged(reg, reg, GA, t, m, core, gpeer(m))

    def fw_copy(t, m):
        reg = gat.at[t, pl.ds(pl.multiple_of(core * half + flip(side, m) * EC, EC), EC)]
        return tagged(reg, reg, FW, t, m, other, lb)

    def p_copy(t, m):
        reg = pg.at[t, :, myrows, mycols]
        return tagged(reg, reg, PS, t, m, core, gpeer(m))

    def pf_copy(t):
        reg = pg.at[t, :, :, mycols]
        return tagged(reg, reg, PF, t, 0, other, lb)

    def f_copy(t, m):
        src = fsend.at[t, :, pl.ds(pl.multiple_of(flip(low, m) * 16, 16), 16)]
        return tagged(src, frecv.at[t, eset], FI, t, m, core, gpeer(m))

    def l_region(m, j):
        first, count = THIRDS[j]
        return ls.at[pl.ds(core * (mpo // 2) + first, count), pl.ds(pl.multiple_of(flip(low, m) * 16, 16), 16)]

    def l_copy(m, j, d):
        reg = l_region(m, j)
        return remote(reg, reg, l_s.at[j, m, d], l_r.at[j, m + d], core, gpeer(d))

    def lf_copy(m, j):
        reg = l_region(m, j)
        return remote(reg, reg, lf_s.at[j, m], lf_r.at[j, m], other, lb)

    group = [(c, m) for c in range(2) for m in range(8) if c or m]

    def ag_copy(t, kind, c, m):
        return remote(asend.at[kind, t, 0], gbuf.at[kind, t, core * 8 + eset], ssem.at[AG + 2 * kind, t, m + 8 * c], rsem.at[AG + 2 * kind, t, m + 8 * c], core + c * (1 - 2 * core), gpeer(m))

    def ar_copy(t, kind, m):
        return remote(asend.at[kind, t, 1], rbuf.at[kind, t, aset], ssem.at[AR + 2 * kind, t, m], rsem.at[AR + 2 * kind, t, m], core, rpeer(m))

    def g_send(t, kind, part):
        asend[kind, t, 0] = part
        gbuf[kind, t, core * 8 + eset] = part
        for c, m in group:
            ag_copy(t, kind, c, m).start()

    def g_sum(t, kind):
        for c, m in group:
            ag_copy(t, kind, c, m).wait_recv()
        return sum(gbuf[kind, t, j] for j in range(16))

    def r_send(t, kind, part):
        asend[kind, t, 1] = part
        rbuf[kind, t, aset] = part
        for m in SEVEN:
            ar_copy(t, kind, m).start()

    def r_sum(t, kind):
        for m in SEVEN:
            ar_copy(t, kind, m).wait_recv()
        return sum(rbuf[kind, t, j] for j in range(8))

    def total(t, kind, tile):
        for c, m in group:
            ag_copy(t, kind, c, m).wait_send()
        for m in SEVEN:
            ar_copy(t, kind, m).wait_send()
        return jnp.sum(jnp.sum(tile, axis=0, keepdims=True), axis=1, keepdims=True) / elems

    def put(t, kind, val):
        scal[kind, t] = jnp.broadcast_to(val, (8, LN))

    def get(t, kind):
        return scal[kind, t][0:1, 0:1]

    def record(out, t, s, val):
        rows = lax.broadcasted_iota(jnp.int32, out.shape, 0)
        cols = lax.broadcasted_iota(jnp.int32, out.shape, 1)
        out[...] = jnp.where(jnp.logical_and(rows == t, cols == s), val, out[...])

    psi_ld = pltpu.make_async_copy(psi_ref, praw, ssem.at[LD + 6, 0, 0])
    psi_ld.start()
    l_ld = pltpu.make_async_copy(left_ref, lst, ssem.at[LD + 6, 0, 1])
    l_ld.start()
    r_ld = pltpu.make_async_copy(right_ref.at[:, pl.ds(pl.multiple_of(eset * EC, EC), EC)], rf, ssem.at[LD + 6, 0, 2])
    r_ld.start()
    barrier = pltpu.get_barrier_semaphore()
    for c, m in group:
        pl.semaphore_signal(barrier, inc=1, device_id=(core + c * (1 - 2 * core), gpeer(m)), device_id_type=MESH)
    for m in SEVEN:
        pl.semaphore_signal(barrier, inc=1, device_id=(core, rpeer(m)), device_id_type=MESH)
    psi_ld.wait()
    parts = []
    for t in range(2):
        acc = 0
        for ij in range(PH):
            val = praw[t, :, ij // 2, ij % 2, :]
            pg[t, ij, myrows, mycols] = val
            acc = acc + val * val
        parts.append(fold(acc))
    alpha_out[...] = jnp.zeros(alpha_out.shape, F32)
    beta_out[...] = jnp.zeros(beta_out.shape, F32)
    pl.semaphore_wait(barrier, len(group) + len(SEVEN))
    for t in range(2):
        g_send(t, NORM, parts[t])
    for m in SEVEN:
        p_copy(0, m).start()
    l_ld.wait()

    def perm_body(l, carry):
        lane = lax.broadcasted_iota(jnp.int32, (16, LN), 1) // 32
        for hz in range(2):
            for hy in range(2):
                src = [lst[l, :, pl.ds((4 * hz + 2 * q + hy) * LN, LN)] for q in range(2)]
                for hx in range(2):
                    pick = None
                    for c in range(PH):
                        shift = (c - 2 * (c % 2) - hx) * 32 % LN
                        val = pltpu.roll(src[c // 2], shift, 1) if shift else src[c // 2]
                        pick = val if pick is None else jnp.where(lane == c, val, pick)
                    ls[l, myrows, pl.ds(number((hz, hy, hx)) * LN, LN)] = pick
        return carry

    lax.fori_loop(0, mpo, perm_body, 0)
    for j in range(3):
        for d in NEAR:
            l_copy(0, j, d).start()
    w0, w1, w2 = split3(wmat_ref[...])
    wpk[...] = jnp.concatenate([w0, w0, w0, w1, w1, w2], axis=1)
    for t in range(2):
        r_send(t, NORM, g_sum(t, NORM))

    def l_spread():
        for j in range(3):
            a, b, c = ORDERS[j]
            l_r_wait(a, j, (b, c))
            l_r_wait(b, j, (c,))
            l_r_wait(c, j, ())
        for j in range(3):
            a, b, c = ORDERS[j]
            l_r_wait(a + b, j, (c,))
        for m in SEVEN:
            p_copy(1, m).start()
        for j in range(3):
            a, b, c = ORDERS[j]
            for m in (a + c, b + c, a + b + c):
                l_r_wait(m, j, ())
        for j in range(3):
            for m in SEVEN:
                lf_copy(m, j).wait_recv()
        for j in range(3):
            a, b, c = ORDERS[j]
            for m, d in ((0, a), (0, b), (0, c), (a, b), (a, c), (b, c), (a + b, c)):
                l_copy(m, j, d).wait_send()
            for m in SEVEN:
                lf_copy(m, j).wait_send()

    def l_r_wait(m, j, links):
        l_copy_in(m, j).wait_recv()
        for d in links:
            l_copy(m, j, d).start()
        lf_copy(m, j).start()

    def l_copy_in(m, j):
        reg = l_region(m, j)
        return remote(reg, reg, l_s.at[j, 0, 0], l_r.at[j, m], core, lb)

    def ev_init(t):
        for m in SEVEN:
            p_copy(t, m).wait_recv()
        pf_copy(t).start()
        rinv = 1.0 / jnp.sqrt(total(t, NORM, r_sum(t, NORM)))
        put(t, BETA, jnp.zeros((1, 1), F32))
        pf_copy(t).wait_recv()

        def tr_body(b, carry):
            rows = pl.ds(pl.multiple_of(b * LN, LN), LN)
            for ij in range(PH):
                vec[t, 0, rows, ij * LN:(ij + 1) * LN] = pg[t, ij, :, rows].T * rinv
            vec[t, 1, rows] = jnp.zeros((LN, WID), F32)
            return carry

        lax.fori_loop(0, bond // LN, tr_body, 0)
        for m in SEVEN:
            p_copy(t, m).wait_send()
        pf_copy(t).wait_send()

    def ev_sum(t, s, more):
        for m in SEVEN:
            rs_copy(t, m).wait_recv()
        hv = outb[t, aset] + sum(rsb[t, m] for m in SEVEN)
        gat[t, pl.ds(own, EC)] = hv
        g_send(t, ALPHA, fold(hv * vec[t, s % 2, pl.ds(own, EC)]))

        @pl.when(more)
        def _():
            for m in SEVEN:
                g_copy(t, m).start()
            fw_copy(t, 0).start()

        for m in SEVEN:
            rs_copy(t, m).wait_send()

    def new_w(t, s, rows):
        return gat[t, rows] - get(t, ALPHA) * vec[t, s % 2, rows] - get(t, BETA) * vec[t, (s + 1) % 2, rows]

    def ev_mid(t):
        r_send(t, ALPHA, g_sum(t, ALPHA))

    def ev_alpha(t, s):
        alpha = total(t, ALPHA, r_sum(t, ALPHA))
        put(t, ALPHA, alpha)
        record(alpha_out, t, s, alpha)
        res = new_w(t, s, pl.ds(own, EC))
        r_send(t, BETA, fold(res * res))

    def ev_mid2(t):
        g_send(t, BETA, r_sum(t, BETA))

    def ev_fwd(t, which):
        for m in which:
            g_copy(t, m).wait_recv()
            fw_copy(t, m).start()

    def ev_beta(t, s):
        beta = jnp.sqrt(total(t, BETA, g_sum(t, BETA)))
        record(beta_out, t, s, beta)
        return beta

    def ev_vec(t, s):
        beta = ev_beta(t, s)
        rinv = 1.0 / beta

        def rows_of(first):
            def body(j, carry):
                rows = pl.ds(pl.multiple_of(first + j * LN, LN), LN)
                vec[t, (s + 1) % 2, rows] = new_w(t, s, rows) * rinv
                return carry

            lax.fori_loop(0, half // LN, body, 0)

        rows_of(core * half)
        for m in range(8):
            fw_copy(t, m).wait_recv()
        rows_of(other * half)
        put(t, BETA, beta)
        for m in range(8):
            fw_copy(t, m).wait_send()
        for m in SEVEN:
            g_copy(t, m).wait_send()

    def r_phase(t, s, first, count):
        xv = jnp.dot(rf[:, pl.ds(first, count), :].reshape(mpo * count, bond), vec[t, s % 2], preferred_element_type=F32, precision=HI)
        for r in range(mpo):
            for ij in range(PH):
                xf[pl.ds((ij * mpo + r) * NX, count), :] = xv[r * count:(r + 1) * count, ij * LN:(ij + 1) * LN]

    def w_phase(first, count):
        for e in range(0, count, 2):
            xs = jnp.concatenate([xf[pl.ds(e + q, PH * mpo, stride=NX), :] for q in range(2)], axis=1)
            x0, x1, x2 = split3(xs)
            yv = jnp.dot(wpk[...], jnp.concatenate([x0, x1, x2, x0, x1, x0], axis=0), preferred_element_type=F32)
            for q in range(2):
                yf[pl.ds(first + e + q, PH * mpo, stride=NY), :] = yv[:, q * LN:(q + 1) * LN]

    def step_body(it, carry):
        t, s = it % 2, it // 2
        ot = 1 - t
        os = (it + 1) // 2 - 1
        has = it >= 1
        more = jnp.logical_and(has, it < 2 * STEPS - 1)

        @pl.when(it < 2)
        def _():
            ev_init(t)

        @pl.when(it >= 2)
        def _():
            ev_vec(t, s - 1)

        @pl.when(it == 0)
        def _():
            r_ld.wait()

        r_phase(t, s, 0, 32)

        @pl.when(has)
        def _():
            ev_sum(ot, os, more)

        w_phase(0, 32)

        def quarter(j, c2):
            first = pl.multiple_of(32 + j * 16, 16)
            r_phase(t, s, first, 16)

            @pl.when(jnp.logical_and(has, j == 0))
            def _():
                ev_mid(ot)

            w_phase(first, 16)
            return c2

        lax.fori_loop(0, 2, quarter, 0)

        @pl.when(has)
        def _():
            ev_alpha(ot, os)

        @pl.when(more)
        def _():
            ev_fwd(ot, NEAR)

        @pl.when(it == 0)
        def _():
            l_spread()

        def l_body(n, c2):
            ms = [FAR[j] + n * ((NEAR + (0,))[j] - FAR[j]) for j in range(PH)]
            blks = [flip(high, m) for m in ms]
            lhs = jnp.concatenate([jnp.concatenate([yf[pl.ds((l * PH + mn) * NY, EC), :] for mn in range(PH)], axis=0) for l in range(mpo)], axis=1)
            rhs = jnp.concatenate([ls[:, :, pl.ds(pl.multiple_of(b * LN, LN), LN)].reshape(mpo * LN, LN) for b in blks], axis=1)
            ov = jnp.dot(lhs, rhs, preferred_element_type=F32, precision=HI)
            for j in range(PH):
                for mn in range(PH):
                    outb[t, blks[j], :, mn * LN:(mn + 1) * LN] = ov[mn * EC:(mn + 1) * EC, j * LN:(j + 1) * LN]
            for m in ms[:3]:
                rs_copy(t, m).start()

            @pl.when(n == 0)
            def _():
                rs_copy(t, FAR[3]).start()

            @pl.when(jnp.logical_and(has, n == 0))
            def _():
                ev_mid2(ot)

            @pl.when(jnp.logical_and(more, n == 0))
            def _():
                ev_fwd(ot, FAR[1:])

            @pl.when(jnp.logical_and(more, n == 1))
            def _():
                ev_fwd(ot, FAR[:1])

            return c2

        lax.fori_loop(0, 2, l_body, 0)
        return carry

    lax.fori_loop(0, 2 * STEPS, step_body, 0)

    last = STEPS - 1

    def finish(t):
        res = new_w(t, last, pl.ds(own, EC)) * (1.0 / ev_beta(t, last))
        for q in range(2):
            pair = [res[:, j * LN:(j + 1) * LN] for j in (2 * q, 2 * q + 1)]
            fsend[t, q] = jnp.concatenate(pair, axis=0).T
        for m in SEVEN:
            f_copy(t, m).start()
        frecv[t, eset] = fsend[t, :, myrows]

    def assemble(t):
        for m in SEVEN:
            f_copy(t, m).wait_recv()
        for i in range(2):
            for j in range(2):
                psi_out[t, :, i, j, :] = jnp.concatenate([frecv[t, g, i][:, j * EC:(j + 1) * EC] for g in range(8)], axis=1)
        for m in SEVEN:
            f_copy(t, m).wait_send()

    ev_sum(1, last, False)
    finish(0)
    ev_mid(1)
    assemble(0)
    ev_alpha(1, last)
    ev_mid2(1)
    finish(1)
    assemble(1)


def solution(mesh):
    psi_spec = P(None, "lb", None, None, "rb")

    def local_run(psi_loc, left_loc, right_loc, mpo_pair):
        targets, rows, phys, _, half = psi_loc.shape
        mpo, bond = left_loc.shape[1:]
        left_t = jnp.transpose(left_loc, (1, 0, 2))
        right_t = jnp.transpose(right_loc, (1, 0, 2))
        wmat = jnp.transpose(mpo_pair.reshape(mpo, mpo, PH, PH), (0, 3, 2, 1)).reshape(PH * mpo, PH * mpo)
        dma = pltpu.SemaphoreType.DMA
        any_spec = pl.BlockSpec(memory_space=pl.ANY)
        vm = pl.BlockSpec(memory_space=pltpu.VMEM)
        f32_shapes = [
            (mpo, EC, bond),
            (mpo, LN, bond),
            (mpo, rows, bond),
            (2, bond, WID),
            (2, 2, bond, WID),
            (2, PH, LN, bond),
            psi_loc.shape,
            (PH * mpo * NX, LN),
            (PH * mpo * NY, LN),
            (2, 8, EC, WID),
            (2, 8, EC, WID),
        ]
        small = [(3, 2, 16, 8, LN), (3, 2, 8, 8, LN), (3, 2, 2, 8, LN), (2, 2, 8, LN), (2, 2, LN, LN), (2, 8, 2, 16, LN)]
        call = pl.pallas_call(
            functools.partial(kernel, (bond, mpo, float(bond * bond * PH))),
            out_shape=[jax.ShapeDtypeStruct(shape, F32) for shape in (psi_loc.shape, (targets, STEPS), (targets, STEPS))],
            in_specs=[any_spec, any_spec, any_spec, vm],
            out_specs=[vm] * 3,
            scratch_shapes=[pltpu.VMEM(shape, F32) for shape in f32_shapes]
            + [pltpu.VMEM((PH * mpo, 6 * PH * mpo), BF16)]
            + [pltpu.VMEM(shape, F32) for shape in small]
            + [dma((16, 2, 16))] * 2
            + [dma((3, 8, 8)), dma((3, 8)), dma((3, 8)), dma((3, 8))],
            compiler_params=pltpu.CompilerParams(vmem_limit_bytes=63 << 20, has_side_effects=True, collective_id=0),
            name="lanczos",
        )
        psi_next, alpha_vals, beta_vals = call(psi_loc, left_t, right_t, wmat)
        return alpha_vals, beta_vals, psi_next

    return jax.shard_map(local_run, mesh=mesh, in_specs=(psi_spec, P("lb", None, None), P("rb", None, None), P()), out_specs=(P(), P(), psi_spec), check_vma=False)
```

```python
import functools

import jax
import jax.numpy as jnp
from jax import lax
from jax.experimental import pallas as pl
from jax.experimental.pallas import tpu as pltpu
from jax.sharding import PartitionSpec as P

STEPS = 4
HI = lax.Precision.HIGHEST
F32 = jnp.float32
BF16 = jnp.bfloat16
MESH = pl.DeviceIdType.MESH
LN = 128
EC = 64
EH = EC // 2
PH = 4
WID = PH * LN
NX = 40
NY = 72
FAR = (3, 5, 6, 7)
CLOSE = (4, 2, 1, 0)
NEAR = CLOSE[:3]
SEVEN = FAR + NEAR
ALPHA, BETA, NORM, FAC = range(4)
SIZE = FAC + 2
RS, GA, FW = 0, 2, 4
PS, PF, FI, AG = range(6, 10)
AR = AG + 3
LS, LF = AR + 3, AR + 4
KINDS = AR + 5
THIRDS = ((0, 4), (4, 3), (7, 3))
ORDERS = ((4, 2, 1), (2, 1, 4), (1, 4, 2))


def split3(val):
    top = val.astype(BF16)
    rest = val - top.astype(F32)
    mid = rest.astype(BF16)
    low = (rest - mid.astype(F32)).astype(BF16)
    return top, mid, low


def fold(val):
    acc = sum(val[:, j:j + LN] for j in range(0, val.shape[1], LN))
    return sum(acc[j:j + 8] for j in range(0, val.shape[0], 8))


def bits(m):
    return m // 4, (m // 2) % 2, m % 2


def number(trip, base=2):
    return (trip[0] * base + trip[1]) * base + trip[2]


def flip(trip, m):
    return number([q + b * (1 - 2 * q) for q, b in zip(trip, bits(m))])


def places(lb):
    place = (lb // 16, (lb // 4) % 4, lb % 4)
    return place, [q % 2 for q in place], [q // 2 for q in place], [((q + 1) // 2) % 2 for q in place]


def kernel(cfg, psi_ref, left_ref, right_ref, wmat_ref, psi_out, sums_out,
           rf, ls, lst, gat, vec, pg, praw, xf, yf, outb, rsb, l3, wpk, gbuf, rbuf, asend, scal, fsend, frecv, ssem, rsem, lsem, ldsem):
    bond, mpo, elems = cfg
    core, lb = lax.axis_index("rb"), lax.axis_index("lb")
    place, low, high, side = places(lb)
    pos, aset, eset = number(low), number(high), number(side)
    half, lhalf = bond // 2, mpo // 2
    own = core * half + eset * EC
    other = 1 - core
    myrows = pl.ds(pl.multiple_of(pos * 16, 16), 16)
    mycols = pl.ds(pl.multiple_of(core * half, half), half)

    def gpeer(m):
        return number([q + b * (1 - 2 * p) for q, b, p in zip(place, bits(m), low)], 4)

    def rpeer(m):
        return number([q + b * (3 - 2 * q) for q, b in zip(place, bits(m))], 4)

    def remote(src, dst, ssm, rsm, c, chip):
        return pltpu.make_async_remote_copy(src_ref=src, dst_ref=dst, send_sem=ssm, recv_sem=rsm, device_id=(c, chip), device_id_type=MESH)

    def tagged(src, dst, kind, t, c, chip):
        return remote(src, dst, ssem.at[kind, t], rsem.at[kind, t], c, chip)

    def sent(region, kind, t):
        tagged(region, region, kind, t, other, lb).wait_send()

    def came(region, kind, t):
        tagged(region, region, kind, t, other, lb).wait_recv()

    def half_rows(h):
        return pl.ds(pl.multiple_of(h * EH, EH), EH)

    def rs_copy(t, h, m):
        return tagged(outb.at[t, m, half_rows(h)], rsb.at[t, h, m - 1], RS + h, t, core, rpeer(m))

    def gat_rows(m, h):
        return pl.ds(pl.multiple_of(core * half + flip(side, m) * EC + h * EH, EH), EH)

    def g_copy(t, h, m):
        reg = gat.at[t, gat_rows(0, h)]
        return tagged(reg, reg, GA + h, t, core, gpeer(m))

    def fw_copy(t, h, m):
        reg = gat.at[t, gat_rows(m, h)]
        return tagged(reg, reg, FW + h, t, other, lb)

    seven_halves = gat.at[0, pl.ds(0, 7 * EH)]
    eight_halves = gat.at[0, pl.ds(0, 8 * EH)]

    def p_copy(t, m):
        reg = pg.at[t, :, myrows, mycols]
        return tagged(reg, reg, PS, t, core, gpeer(m))

    def pf_copy(t):
        reg = pg.at[t, :, :, mycols]
        return tagged(reg, reg, PF, t, other, lb)

    seven_psi = pg.at[0, :, pl.ds(0, 7 * 16), pl.ds(0, half)]

    def f_copy(t, m):
        src = fsend.at[t, :, pl.ds(pl.multiple_of(flip(low, m) * 16, 16), 16)]
        return tagged(src, frecv.at[t, eset], FI, t, core, gpeer(m))

    seven_fin = frecv.at[0, pl.ds(0, 7)]

    def l_region(n, m, j):
        first, count = THIRDS[j]
        return ls.at[n, pl.ds(core * lhalf + first, count), pl.ds(pl.multiple_of(flip(low, m) * 16, 16), 16)]

    def l_copy(n, m, j, d):
        reg = l_region(n, m, j)
        return remote(reg, reg, ssem.at[LS, n], lsem.at[n, j, m + d], core, gpeer(d))

    def lf_copy(n, m, j):
        reg = l_region(n, m, j)
        return tagged(reg, reg, LF, n, other, lb)

    seven_l = ls.at[0, pl.ds(0, lhalf), pl.ds(0, 7 * 16)]

    group = [(c, m) for c in range(2) for m in range(8) if c or m]

    def flip_core(c):
        return core + c * (1 - 2 * core)

    def g_send(t, kind, part):
        asend[kind, t, 0] = part
        gbuf[kind, t, core * 8 + eset] = part
        for c, m in group:
            tagged(asend.at[kind, t, 0], gbuf.at[kind, t, core * 8 + eset], AG + kind, t, flip_core(c), gpeer(m)).start()

    def g_sum(t, kind):
        came(gbuf.at[kind, t, pl.ds(0, 15)], AG + kind, t)
        return sum(gbuf[kind, t, j] for j in range(16))

    def r_send(t, kind, part):
        asend[kind, t, 1] = part
        rbuf[kind, t, aset] = part
        for m in SEVEN:
            tagged(asend.at[kind, t, 1], rbuf.at[kind, t, aset], AR + kind, t, core, rpeer(m)).start()

    def r_sum(t, kind):
        came(rbuf.at[kind, t, pl.ds(0, 7)], AR + kind, t)
        return sum(rbuf[kind, t, j] for j in range(8))

    def mean(tile):
        return jnp.sum(jnp.sum(tile, axis=0, keepdims=True), axis=1, keepdims=True) / elems

    def total(t, kind):
        tile = r_sum(t, kind)
        sent(gbuf.at[kind, t, pl.ds(0, 15)], AG + kind, t)
        sent(rbuf.at[kind, t, pl.ds(0, 7)], AR + kind, t)
        return mean(tile)

    def put(t, kind, val):
        scal[kind, t] = jnp.broadcast_to(val, (8, LN))

    def get(t, kind):
        return scal[kind, t][0:1, 0:1]

    def record(kind, t, s, val):
        rows = lax.broadcasted_iota(jnp.int32, (2, STEPS), 0)
        cols = lax.broadcasted_iota(jnp.int32, (2, STEPS), 1)
        sums_out[kind] = jnp.where(jnp.logical_and(rows == t, cols == s), val, sums_out[kind])

    psi_ld = pltpu.make_async_copy(psi_ref, praw, ldsem.at[0])
    psi_ld.start()
    l_ld = pltpu.make_async_copy(left_ref, lst, ldsem.at[1])
    l_ld.start()
    r_ld = pltpu.make_async_copy(right_ref.at[:, pl.ds(pl.multiple_of(eset * EC, EC), EC)], rf, ldsem.at[2])
    r_ld.start()
    barrier = pltpu.get_barrier_semaphore()
    for c, m in group:
        pl.semaphore_signal(barrier, inc=1, device_id=(flip_core(c), gpeer(m)), device_id_type=MESH)
    for m in SEVEN:
        pl.semaphore_signal(barrier, inc=1, device_id=(core, rpeer(m)), device_id_type=MESH)
    psi_ld.wait()
    parts = []
    for t in range(2):
        acc = 0
        for ij in range(PH):
            val = praw[t, :, ij // 2, ij % 2, :]
            pg[t, ij, myrows, mycols] = val
            acc = acc + val * val
        parts.append(fold(acc))
    sums_out[...] = jnp.zeros(sums_out.shape, F32)
    pl.semaphore_wait(barrier, len(group) + len(SEVEN))
    for t in range(2):
        g_send(t, NORM, parts[t])
    for m in SEVEN:
        p_copy(0, m).start()
    l_ld.wait()

    def perm_body(l, carry):
        lane = lax.broadcasted_iota(jnp.int32, (16, LN), 1) // 32
        for hz in range(2):
            for hy in range(2):
                src = [lst[l, :, pl.ds((4 * hz + 2 * q + hy) * LN, LN)] for q in range(2)]
                for hx in range(2):
                    pick = None
                    for c in range(PH):
                        shift = (c - 2 * (c % 2) - hx) * 32 % LN
                        val = pltpu.roll(src[c // 2], shift, 1) if shift else src[c // 2]
                        pick = val if pick is None else jnp.where(lane == c, val, pick)
                    rel = [p + q * (1 - 2 * p) for p, q in zip((hz, hy, hx), high)]
                    far = sum(rel) // 2
                    rank = [p + far * (1 - 2 * p) for p in rel]
                    j = 3 - (3 * rank[0] + 2 * rank[1] + rank[2])
                    ls[1 - far, l, myrows, pl.ds(pl.multiple_of(j * LN, LN), LN)] = pick
        return carry

    lax.fori_loop(0, mpo, perm_body, 0)
    for n in range(2):
        for j in range(3):
            for d in NEAR:
                l_copy(n, 0, j, d).start()
    w0, w1, w2 = split3(wmat_ref[...])
    wpk[...] = jnp.concatenate([w0, w0, w0, w1, w1, w2], axis=1)
    for t in range(2):
        r_send(t, NORM, g_sum(t, NORM))

    def l_take(n, m, j, links):
        reg = l_region(n, m, j)
        remote(reg, reg, ssem.at[LS, n], lsem.at[n, j, m], other, lb).wait_recv()
        for d in links:
            l_copy(n, m, j, d).start()
        lf_copy(n, m, j).start()

    def l_rest(n):
        for j in range(3):
            a, b, c = ORDERS[j]
            for m in (a + c, b + c, a + b + c):
                l_take(n, m, j, ())
        came(seven_l, LF, n)

        def split_body(l, carry):
            for k, part in enumerate(split3(ls[n, l])):
                l3[k, n, l] = part
            return carry

        lax.fori_loop(0, mpo, split_body, 0)

    def l_first():
        for n in range(2):
            for j in range(3):
                a, b, c = ORDERS[j]
                l_take(n, a, j, (b, c))
                l_take(n, b, j, (c,))
                l_take(n, c, j, ())
        for n in range(2):
            for j in range(3):
                a, b, c = ORDERS[j]
                l_take(n, a + b, j, (c,))
        for m in SEVEN:
            p_copy(1, m).start()
        l_rest(0)

    def l_second():
        l_rest(1)
        for n in range(2):
            sent(seven_l, LS, n)
            sent(seven_l, LF, n)

    def ev_init(t):
        came(seven_psi, PS, t)
        pf_copy(t).start()
        rinv = 1.0 / jnp.sqrt(total(t, NORM))
        put(t, BETA, jnp.zeros((1, 1), F32))
        for slot in range(2):
            put(t, FAC + slot, jnp.ones((1, 1), F32))
        pf_copy(t).wait_recv()

        def tr_body(b, carry):
            rows = pl.ds(pl.multiple_of(b * LN, LN), LN)
            for ij in range(PH):
                vec[t, 0, rows, ij * LN:(ij + 1) * LN] = pg[t, ij, :, rows].T * rinv
            vec[t, 1, rows] = jnp.zeros((LN, WID), F32)
            return carry

        lax.fori_loop(0, bond // LN, tr_body, 0)
        sent(seven_psi, PS, t)
        pf_copy(t).wait_send()

    def ev_sum(t, s, h, more):
        came(rsb.at[t, h], RS + h, t)
        hv = outb[t, 0, half_rows(h)] + sum(rsb[t, h, m - 1] for m in SEVEN)
        gat[t, gat_rows(0, h)] = hv
        if h:
            rows = pl.ds(pl.multiple_of(own, EC), EC)
            g_send(t, ALPHA, fold(gat[t, rows] * vec[t, s % 2, rows]) * get(t, FAC + s % 2))

        @pl.when(more)
        def _():
            for m in SEVEN:
                g_copy(t, h, m).start()
            fw_copy(t, h, 0).start()

        sent(rsb.at[t, h], RS + h, t)

    def new_w(t, s, rows):
        cur, prev = s % 2, (s + 1) % 2
        return gat[t, rows] - get(t, ALPHA) * get(t, FAC + cur) * vec[t, cur, rows] - get(t, BETA) * get(t, FAC + prev) * vec[t, prev, rows]

    def ev_mid(t):
        r_send(t, ALPHA, g_sum(t, ALPHA))

    def ev_alpha(t, s):
        alpha = total(t, ALPHA)
        put(t, ALPHA, alpha)
        record(0, t, s, alpha)
        res = new_w(t, s, pl.ds(pl.multiple_of(own, EC), EC))
        g_send(t, BETA, fold(res * res))

    def ev_size(t):
        tile = g_sum(t, BETA)
        r_send(t, BETA, tile)
        put(t, SIZE, jnp.sqrt(mean(tile)))

    def ev_fwd(t, h):
        came(seven_halves, GA + h, t)
        for m in SEVEN:
            fw_copy(t, h, m).start()

    def ev_beta(t, s):
        beta = jnp.sqrt(total(t, BETA))
        put(t, BETA, beta)
        record(1, t, s, beta)
        put(t, FAC + (s + 1) % 2, get(t, SIZE) / beta)
        return beta

    def ev_vec(t, s):
        size = get(t, SIZE)
        rinv = jnp.where(size > 0, 1.0 / size, 0.0)

        def rows_of(first):
            def body(j, carry):
                rows = pl.ds(pl.multiple_of(first + j * LN, LN), LN)
                vec[t, (s + 1) % 2, rows] = new_w(t, s, rows) * rinv
                return carry

            lax.fori_loop(0, half // LN, body, 0)

        rows_of(core * half)
        for h in range(2):
            came(eight_halves, FW + h, t)
        rows_of(other * half)
        for h in range(2):
            sent(eight_halves, FW + h, t)
            sent(seven_halves, GA + h, t)

    def r_phase(t, s, h):
        xv = jnp.dot(rf[:, half_rows(h), :].reshape(mpo * EH, bond), vec[t, s % 2], preferred_element_type=F32, precision=HI)
        for r in range(mpo):
            for ij in range(PH):
                xf[pl.ds((ij * mpo + r) * NX, EH), :] = xv[r * EH:(r + 1) * EH, ij * LN:(ij + 1) * LN]

    def w_phase(t, s, h):
        fac = get(t, FAC + s % 2)
        for e in range(0, EH, 2):
            xs = jnp.concatenate([xf[pl.ds(e + q, PH * mpo, stride=NX), :] for q in range(2)], axis=1) * fac
            x0, x1, x2 = split3(xs)
            yv = jnp.dot(wpk[...], jnp.concatenate([x0, x1, x2, x0, x1, x0], axis=0), preferred_element_type=F32)
            for q in range(2):
                yf[pl.ds(h * EH + e + q, PH * mpo, stride=NY), :] = yv[:, q * LN:(q + 1) * LN]

    def l_phase(t, h, n):
        lhs = [jnp.concatenate([yf[pl.ds(pl.multiple_of((l * PH + mn) * NY + h * EH, 8), EH), :] for mn in range(PH)], axis=0) for l in range(mpo)]
        y0, y1, y2 = split3(jnp.concatenate(lhs, axis=1))
        b0, b1, b2 = [l3[k, n].reshape(mpo * LN, PH * LN) for k in range(3)]
        p0 = jnp.dot(jnp.concatenate([y0, y1, y2], axis=0), b0, preferred_element_type=F32)
        p1 = jnp.dot(jnp.concatenate([y0, y1], axis=0), b1, preferred_element_type=F32)
        p2 = jnp.dot(y0, b2, preferred_element_type=F32)
        ov = ((p0[2 * LN:] + p1[LN:]) + p2) + (p0[LN:2 * LN] + p1[:LN]) + p0[:LN]
        for j in range(PH):
            m = FAR[j] + n * (CLOSE[j] - FAR[j])
            for mn in range(PH):
                outb[t, m, half_rows(h), mn * LN:(mn + 1) * LN] = ov[mn * EH:(mn + 1) * EH, j * LN:(j + 1) * LN]

    def step_body(it, carry):
        t, s = it % 2, it // 2
        ot = 1 - t
        os = (it + 1) // 2 - 1
        first = 1 - (it + 2 * STEPS - 1) // (2 * STEPS)
        has = it >= 1
        more = jnp.logical_and(has, it < 2 * STEPS - 1)

        @pl.when(it < 2)
        def _():
            ev_init(t)

        @pl.when(it >= 2)
        def _():
            ev_vec(t, s - 1)

        @pl.when(has)
        def _():
            ev_sum(ot, os, 0, more)

        @pl.when(it == 0)
        def _():
            r_ld.wait()

        def slot_body(q, c2):
            h = first * (q % 2) + (1 - first) * (q // 3)
            n = first * ((q - 2) // 2) + (1 - first) * (q % 3 - 1)
            is_rw = jnp.logical_or(jnp.logical_and(it == 0, q < 2), jnp.logical_and(has, q % 3 == 0))

            def at(cond, slot, event, *args):
                @pl.when(jnp.logical_and(cond, q == slot))
                def _():
                    event(*args)

            @pl.when(is_rw)
            def _():
                r_phase(t, s, h)
                at(has, 0, ev_sum, ot, os, 1, more)
                at(it >= 2, 0, ev_beta, t, s - 1)
                at(has, 3, ev_alpha, ot, os)
                at(more, 3, ev_fwd, ot, 1)
                w_phase(t, s, h)

            @pl.when(jnp.logical_not(is_rw))
            def _():
                at(it == 0, 2, l_first)
                at(it == 0, 4, l_second)
                l_phase(t, h, n)
                at(has, 1, ev_mid, ot)
                at(more, 2, ev_fwd, ot, 0)
                at(has, 4, ev_size, ot)

                @pl.when(n == 0)
                def _():
                    for m in FAR:
                        rs_copy(t, h, m).start()

                @pl.when(n == 1)
                def _():
                    for m in NEAR:
                        rs_copy(t, h, m).start()

            return c2

        lax.fori_loop(0, 6, slot_body, 0)
        return carry

    lax.fori_loop(0, 2 * STEPS, step_body, 0)

    last = STEPS - 1

    def finish(t):
        beta = ev_beta(t, last)
        res = new_last[t] * (1.0 / beta)
        for q in range(2):
            pair = [res[:, j * LN:(j + 1) * LN] for j in (2 * q, 2 * q + 1)]
            fsend[t, q] = jnp.concatenate(pair, axis=0).T
        for m in SEVEN:
            f_copy(t, m).start()
        frecv[t, eset] = fsend[t, :, myrows]

    def assemble(t):
        came(seven_fin, FI, t)
        for i in range(2):
            for j in range(2):
                psi_out[t, :, i, j, :] = jnp.concatenate([frecv[t, g, i][:, j * EC:(j + 1) * EC] for g in range(8)], axis=1)
        sent(seven_fin, FI, t)

    ownrows = pl.ds(pl.multiple_of(own, EC), EC)
    new_last = {}
    ev_sum(1, last, 0, False)
    ev_sum(1, last, 1, False)
    new_last[0] = new_w(0, last, ownrows)
    finish(0)
    ev_mid(1)
    assemble(0)
    ev_alpha(1, last)
    new_last[1] = new_w(1, last, ownrows)
    ev_size(1)
    finish(1)
    assemble(1)


def solution(mesh):
    psi_spec = P(None, "lb", None, None, "rb")

    def local_run(psi_loc, left_loc, right_loc, mpo_pair):
        rows = psi_loc.shape[1]
        mpo, bond = left_loc.shape[1:]
        left_t = jnp.transpose(left_loc, (1, 0, 2))
        right_t = jnp.transpose(right_loc, (1, 0, 2))
        wmat = jnp.transpose(mpo_pair.reshape(mpo, mpo, PH, PH), (0, 3, 2, 1)).reshape(PH * mpo, PH * mpo)
        dma = pltpu.SemaphoreType.DMA
        any_spec = pl.BlockSpec(memory_space=pl.ANY)
        vm = pl.BlockSpec(memory_space=pltpu.VMEM)
        f32_shapes = [
            (mpo, EC, bond),
            (2, mpo, LN, WID),
            (mpo, rows, bond),
            (2, bond, WID),
            (2, 2, bond, WID),
            (2, PH, LN, bond),
            psi_loc.shape,
            (PH * mpo * NX, LN),
            (PH * mpo * NY, LN),
            (2, 8, EC, WID),
            (2, 2, 7, EH, WID),
        ]
        small = [(3, 2, 16, 8, LN), (3, 2, 8, 8, LN), (3, 2, 2, 8, LN), (SIZE + 1, 2, 8, LN), (2, 2, LN, LN), (2, 8, 2, 16, LN)]
        call = pl.pallas_call(
            functools.partial(kernel, (bond, mpo, float(bond * bond * PH))),
            out_shape=[jax.ShapeDtypeStruct(shape, F32) for shape in (psi_loc.shape, (2, 2, STEPS))],
            in_specs=[any_spec, any_spec, any_spec, vm],
            out_specs=[vm] * 2,
            scratch_shapes=[pltpu.VMEM(shape, F32) for shape in f32_shapes]
            + [pltpu.VMEM((3, 2, mpo, LN, WID), BF16), pltpu.VMEM((PH * mpo, 6 * PH * mpo), BF16)]
            + [pltpu.VMEM(shape, F32) for shape in small]
            + [dma((KINDS, 2))] * 2
            + [dma((2, 3, 8)), dma((3,))],
            compiler_params=pltpu.CompilerParams(vmem_limit_bytes=63 << 20, has_side_effects=True, collective_id=0),
            name="lanczos",
        )
        psi_next, sums = call(psi_loc, left_t, right_t, wmat)
        return sums[0], sums[1], psi_next

    return jax.shard_map(local_run, mesh=mesh, in_specs=(psi_spec, P("lb", None, None), P("rb", None, None), P()), out_specs=(P(), P(), psi_spec), check_vma=False)
```

```python
import functools

import jax
import jax.numpy as jnp
from jax import lax
from jax.experimental import pallas as pl
from jax.experimental.pallas import tpu as pltpu
from jax.sharding import PartitionSpec as P

STEPS = 4
HI = lax.Precision.HIGHEST
F32 = jnp.float32
BF16 = jnp.bfloat16
MESH = pl.DeviceIdType.MESH
LN = 128
EC = 64
EH = EC // 2
PH = 4
WID = PH * LN
NX = 40
NY = 72
FAR = (3, 5, 6, 7)
CLOSE = (4, 2, 1, 0)
NEAR = CLOSE[:3]
SEVEN = FAR[::-1] + NEAR
ALPHA, BETA, NORM, FAC = range(4)
SIZE = FAC + 2
RS, GA, FW = 0, 2, 4
PS, PF, FI, AG = range(6, 10)
AR = AG + 3
LS, LF = AR + 3, AR + 4
KINDS = AR + 6
THIRDS = ((0, 4), (4, 3), (7, 3))
ORDERS = ((4, 2, 1), (2, 1, 4), (1, 4, 2))


def split3(val):
    top = val.astype(BF16)
    rest = val - top.astype(F32)
    mid = rest.astype(BF16)
    low = (rest - mid.astype(F32)).astype(BF16)
    return top, mid, low


def fold(val):
    acc = sum(val[:, j:j + LN] for j in range(0, val.shape[1], LN))
    return sum(acc[j:j + 8] for j in range(0, val.shape[0], 8))


def bits(m):
    return m // 4, (m // 2) % 2, m % 2


def number(trip, base=2):
    return (trip[0] * base + trip[1]) * base + trip[2]


def flip(trip, m):
    return number([q + b * (1 - 2 * q) for q, b in zip(trip, bits(m))])


def places(lb):
    place = (lb // 16, (lb // 4) % 4, lb % 4)
    return place, [q % 2 for q in place], [q // 2 for q in place], [((q + 1) // 2) % 2 for q in place]


def kernel(cfg, psi_ref, left_ref, right_ref, wmat_ref, psi_out, sums_out,
           rf, ls, lst, gat, vec, pg, praw, xf, yf, outb, rsb, l3, wpk, gbuf, rbuf, asend, scal, fsend, frecv, ssem, rsem, lsem, ldsem):
    bond, mpo, elems = cfg
    core, lb = lax.axis_index("rb"), lax.axis_index("lb")
    place, low, high, side = places(lb)
    pos, aset, eset = number(low), number(high), number(side)
    half, lhalf = bond // 2, mpo // 2
    own = core * half + eset * EC
    other = 1 - core
    myrows = pl.ds(pl.multiple_of(pos * 16, 16), 16)
    mycols = pl.ds(pl.multiple_of(core * half, half), half)

    def gpeer(m):
        return number([q + b * (1 - 2 * p) for q, b, p in zip(place, bits(m), low)], 4)

    def rpeer(m):
        return number([q + b * (3 - 2 * q) for q, b in zip(place, bits(m))], 4)

    def remote(src, dst, ssm, rsm, c, chip):
        return pltpu.make_async_remote_copy(src_ref=src, dst_ref=dst, send_sem=ssm, recv_sem=rsm, device_id=(c, chip), device_id_type=MESH)

    def tagged(src, dst, kind, t, c, chip):
        return remote(src, dst, ssem.at[kind, t], rsem.at[kind, t], c, chip)

    def sent(region, kind, t):
        tagged(region, region, kind, t, other, lb).wait_send()

    def came(region, kind, t):
        tagged(region, region, kind, t, other, lb).wait_recv()

    def half_rows(h):
        return pl.ds(pl.multiple_of(h * EH, EH), EH)

    def rs_copy(t, h, m):
        return tagged(outb.at[t, m, half_rows(h)], rsb.at[t, h, m - 1], RS + h, t, core, rpeer(m))

    def gat_rows(m, h):
        return pl.ds(pl.multiple_of(core * half + flip(side, m) * EC + h * EH, EH), EH)

    def g_copy(t, h, m):
        reg = gat.at[t, gat_rows(0, h)]
        return tagged(reg, reg, GA + h, t, core, gpeer(m))

    def fw_copy(t, h, m):
        reg = gat.at[t, gat_rows(m, h)]
        return tagged(reg, reg, FW + h, t, other, lb)

    seven_halves = gat.at[0, pl.ds(0, 7 * EH)]
    eight_halves = gat.at[0, pl.ds(0, 8 * EH)]

    def p_copy(t, m):
        reg = pg.at[t, :, myrows, mycols]
        return tagged(reg, reg, PS, t, core, gpeer(m))

    def pf_copy(t):
        reg = pg.at[t, :, :, mycols]
        return tagged(reg, reg, PF, t, other, lb)

    seven_psi = pg.at[0, :, pl.ds(0, 7 * 16), pl.ds(0, half)]

    def f_copy(t, m):
        src = fsend.at[t, :, pl.ds(pl.multiple_of(flip(low, m) * 16, 16), 16)]
        return tagged(src, frecv.at[t, eset], FI, t, core, gpeer(m))

    seven_fin = frecv.at[0, pl.ds(0, 7)]

    def l_region(n, m, j):
        first, count = THIRDS[j]
        return ls.at[n, pl.ds(core * lhalf + first, count), pl.ds(pl.multiple_of(flip(low, m) * 16, 16), 16)]

    def l_copy(n, m, j, d):
        reg = l_region(n, m, j)
        return remote(reg, reg, ssem.at[LS, n], lsem.at[n, j, m + d], core, gpeer(d))

    def lf_copy(n, m, j):
        reg = l_region(n, m, j)
        return tagged(reg, reg, LF + (m in FAR), n, other, lb)

    seven_l = ls.at[0, pl.ds(0, lhalf), pl.ds(0, 7 * 16)]
    near_l, far_l = [ls.at[0, pl.ds(0, lhalf), pl.ds(0, len(part) * 16)] for part in (NEAR, FAR)]

    group = [(c, m) for c in range(2) for m in range(8) if c or m]

    def flip_core(c):
        return core + c * (1 - 2 * core)

    def g_send(t, kind, part):
        asend[kind, t, 0] = part
        gbuf[kind, t, core * 8 + eset] = part
        for c, m in group:
            tagged(asend.at[kind, t, 0], gbuf.at[kind, t, core * 8 + eset], AG + kind, t, flip_core(c), gpeer(m)).start()

    def g_sum(t, kind):
        came(gbuf.at[kind, t, pl.ds(0, 15)], AG + kind, t)
        return sum(gbuf[kind, t, j] for j in range(16))

    def r_send(t, kind, part):
        asend[kind, t, 1] = part
        rbuf[kind, t, aset] = part
        for m in SEVEN:
            tagged(asend.at[kind, t, 1], rbuf.at[kind, t, aset], AR + kind, t, core, rpeer(m)).start()

    def r_sum(t, kind):
        came(rbuf.at[kind, t, pl.ds(0, 7)], AR + kind, t)
        return sum(rbuf[kind, t, j] for j in range(8))

    def mean(tile):
        return jnp.sum(jnp.sum(tile, axis=0, keepdims=True), axis=1, keepdims=True) / elems

    def total(t, kind):
        tile = r_sum(t, kind)
        sent(gbuf.at[kind, t, pl.ds(0, 15)], AG + kind, t)
        sent(rbuf.at[kind, t, pl.ds(0, 7)], AR + kind, t)
        return mean(tile)

    def put(t, kind, val):
        scal[kind, t] = jnp.broadcast_to(val, (8, LN))

    def get(t, kind):
        return scal[kind, t][0:1, 0:1]

    def record(kind, t, s, val):
        rows = lax.broadcasted_iota(jnp.int32, (2, STEPS), 0)
        cols = lax.broadcasted_iota(jnp.int32, (2, STEPS), 1)
        sums_out[kind] = jnp.where(jnp.logical_and(rows == t, cols == s), val, sums_out[kind])

    psi_ld = pltpu.make_async_copy(psi_ref, praw, ldsem.at[0])
    psi_ld.start()
    l_ld = pltpu.make_async_copy(left_ref, lst, ldsem.at[1])
    l_ld.start()
    r_ld = pltpu.make_async_copy(right_ref.at[:, pl.ds(pl.multiple_of(eset * EC, EC), EC)], rf, ldsem.at[2])
    r_ld.start()
    barrier = pltpu.get_barrier_semaphore()
    for c, m in group:
        pl.semaphore_signal(barrier, inc=1, device_id=(flip_core(c), gpeer(m)), device_id_type=MESH)
    for m in SEVEN:
        pl.semaphore_signal(barrier, inc=1, device_id=(core, rpeer(m)), device_id_type=MESH)
    psi_ld.wait()
    parts = []
    for t in range(2):
        acc = 0
        for ij in range(PH):
            val = praw[t, :, ij // 2, ij % 2, :]
            pg[t, ij, myrows, mycols] = val
            acc = acc + val * val
        parts.append(fold(acc))
    sums_out[...] = jnp.zeros(sums_out.shape, F32)
    pl.semaphore_wait(barrier, len(group) + len(SEVEN))
    for t in range(2):
        g_send(t, NORM, parts[t])
    for m in SEVEN:
        p_copy(0, m).start()
    l_ld.wait()

    def perm_body(l, carry):
        lane = lax.broadcasted_iota(jnp.int32, (16, LN), 1) // 32
        for hz in range(2):
            for hy in range(2):
                src = [lst[l, :, pl.ds((4 * hz + 2 * q + hy) * LN, LN)] for q in range(2)]
                for hx in range(2):
                    pick = None
                    for c in range(PH):
                        shift = (c - 2 * (c % 2) - hx) * 32 % LN
                        val = pltpu.roll(src[c // 2], shift, 1) if shift else src[c // 2]
                        pick = val if pick is None else jnp.where(lane == c, val, pick)
                    rel = [p + q * (1 - 2 * p) for p, q in zip((hz, hy, hx), high)]
                    far = sum(rel) // 2
                    rank = [p + far * (1 - 2 * p) for p in rel]
                    j = 3 - (3 * rank[0] + 2 * rank[1] + rank[2])
                    ls[1 - far, l, myrows, pl.ds(pl.multiple_of(j * LN, LN), LN)] = pick
        return carry

    lax.fori_loop(0, mpo, perm_body, 0)
    for n in range(2):
        for j in range(3):
            for d in NEAR:
                l_copy(n, 0, j, d).start()
    w0, w1, w2 = split3(wmat_ref[...])
    wpk[...] = jnp.concatenate([w0, w0, w0, w1, w1, w2], axis=1)
    for t in range(2):
        r_send(t, NORM, g_sum(t, NORM))

    def l_take(n, m, j, links):
        reg = l_region(n, m, j)
        remote(reg, reg, ssem.at[LS, n], lsem.at[n, j, m], other, lb).wait_recv()
        for d in links:
            l_copy(n, m, j, d).start()
        lf_copy(n, m, j).start()

    def split_rows(n, offsets):
        def split_body(l, carry):
            for m in offsets:
                rows = pl.ds(pl.multiple_of(flip(low, m) * 16, 16), 16)
                for k, part in enumerate(split3(ls[n, l, rows])):
                    l3[k, n, l, rows] = part
            return carry

        lax.fori_loop(0, mpo, split_body, 0)

    def l_rest(n):
        for j in range(3):
            a, b, c = ORDERS[j]
            for m in (a + c, b + c, a + b + c):
                l_take(n, m, j, ())
        came(far_l, LF + 1, n)
        split_rows(n, FAR)

    def l_first():
        for n in range(2):
            for j in range(3):
                a, b, c = ORDERS[j]
                l_take(n, a, j, (b, c))
                l_take(n, b, j, (c,))
                l_take(n, c, j, ())
        for n in range(2):
            came(near_l, LF, n)
            split_rows(n, CLOSE)
        for n in range(2):
            for j in range(3):
                a, b, c = ORDERS[j]
                l_take(n, a + b, j, (c,))
        for m in SEVEN:
            p_copy(1, m).start()
        l_rest(0)

    def l_second():
        l_rest(1)
        for n in range(2):
            sent(seven_l, LS, n)
            sent(near_l, LF, n)
            sent(far_l, LF + 1, n)

    def psi_pass(t):
        came(seven_psi, PS, t)
        pf_copy(t).start()

    def ev_init(t):
        rinv = 1.0 / jnp.sqrt(total(t, NORM))
        put(t, BETA, jnp.zeros((1, 1), F32))
        for slot in range(2):
            put(t, FAC + slot, jnp.ones((1, 1), F32))

        def turn(first):
            def tr_body(b, carry):
                rows = pl.ds(pl.multiple_of(first + b * LN, LN), LN)
                for ij in range(PH):
                    vec[t, 0, rows, ij * LN:(ij + 1) * LN] = pg[t, ij, :, rows].T * rinv
                vec[t, 1, rows] = jnp.zeros((LN, WID), F32)
                return carry

            lax.fori_loop(0, half // LN, tr_body, 0)

        turn(core * half)
        pf_copy(t).wait_recv()
        turn(other * half)
        sent(seven_psi, PS, t)
        pf_copy(t).wait_send()

    def ev_sum(t, s, h, more):
        came(rsb.at[t, h], RS + h, t)
        hv = outb[t, 0, half_rows(h)] + sum(rsb[t, h, m - 1] for m in SEVEN)
        gat[t, gat_rows(0, h)] = hv
        if h:
            rows = pl.ds(pl.multiple_of(own, EC), EC)
            g_send(t, ALPHA, fold(gat[t, rows] * vec[t, s % 2, rows]) * get(t, FAC + s % 2))

        @pl.when(more)
        def _():
            for m in SEVEN:
                g_copy(t, h, m).start()
            fw_copy(t, h, 0).start()

        sent(rsb.at[t, h], RS + h, t)

    def new_w(t, s, rows):
        cur, prev = s % 2, (s + 1) % 2
        return gat[t, rows] - get(t, ALPHA) * get(t, FAC + cur) * vec[t, cur, rows] - get(t, BETA) * get(t, FAC + prev) * vec[t, prev, rows]

    def ev_mid(t):
        r_send(t, ALPHA, g_sum(t, ALPHA))

    def ev_alpha(t, s):
        alpha = total(t, ALPHA)
        put(t, ALPHA, alpha)
        record(0, t, s, alpha)
        res = new_w(t, s, pl.ds(pl.multiple_of(own, EC), EC))
        g_send(t, BETA, fold(res * res))

        @pl.when(s == STEPS - 1)
        def _():
            for q in range(2):
                pair = [res[:, j * LN:(j + 1) * LN] for j in (2 * q, 2 * q + 1)]
                fsend[t, q] = jnp.concatenate(pair, axis=0).T
            for m in SEVEN:
                f_copy(t, m).start()
            frecv[t, eset] = fsend[t, :, myrows]

    def ev_size(t):
        tile = g_sum(t, BETA)
        r_send(t, BETA, tile)
        put(t, SIZE, jnp.sqrt(mean(tile)))

    def ev_fwd(t, h):
        came(seven_halves, GA + h, t)
        for m in SEVEN:
            fw_copy(t, h, m).start()

    def ev_beta(t, s):
        beta = jnp.sqrt(total(t, BETA))
        put(t, BETA, beta)
        record(1, t, s, beta)
        put(t, FAC + (s + 1) % 2, get(t, SIZE) / beta)
        return beta

    def ev_vec(t, s):
        size = get(t, SIZE)
        rinv = jnp.where(size > 0, 1.0 / size, 0.0)

        def rows_of(first):
            def body(j, carry):
                rows = pl.ds(pl.multiple_of(first + j * LN, LN), LN)
                vec[t, (s + 1) % 2, rows] = new_w(t, s, rows) * rinv
                return carry

            lax.fori_loop(0, half // LN, body, 0)

        rows_of(core * half)
        for h in range(2):
            came(eight_halves, FW + h, t)
        rows_of(other * half)
        for h in range(2):
            sent(eight_halves, FW + h, t)
            sent(seven_halves, GA + h, t)

    def r_phase(t, s, first, count):
        rows = rf[:, pl.ds(pl.multiple_of(first, 16), count), :].reshape(mpo * count, bond)
        xv = jnp.dot(rows, vec[t, s % 2], preferred_element_type=F32, precision=HI)
        base = first % EH
        for r in range(mpo):
            for ij in range(PH):
                xf[pl.ds(pl.multiple_of((ij * mpo + r) * NX + base, 8), count), :] = xv[r * count:(r + 1) * count, ij * LN:(ij + 1) * LN]

    def w_phase(h):
        for e in range(0, EH, 2):
            xs = jnp.concatenate([xf[pl.ds(e + q, PH * mpo, stride=NX), :] for q in range(2)], axis=1)
            x0, x1, x2 = split3(xs)
            yv = jnp.dot(wpk[...], jnp.concatenate([x0, x1, x2, x0, x1, x0], axis=0), preferred_element_type=F32)
            for q in range(2):
                yf[pl.ds(h * EH + e + q, PH * mpo, stride=NY), :] = yv[:, q * LN:(q + 1) * LN]

    def l_phase(t, s, h, n):
        lhs = [jnp.concatenate([yf[pl.ds(pl.multiple_of((l * PH + mn) * NY + h * EH, 8), EH), :] for mn in range(PH)], axis=0) for l in range(mpo)]
        y0, y1, y2 = split3(jnp.concatenate(lhs, axis=1))
        b0, b1, b2 = [l3[k, n].reshape(mpo * LN, PH * LN) for k in range(3)]
        p0 = jnp.dot(jnp.concatenate([y0, y1, y2], axis=0), b0, preferred_element_type=F32)
        p1 = jnp.dot(jnp.concatenate([y0, y1], axis=0), b1, preferred_element_type=F32)
        p2 = jnp.dot(y0, b2, preferred_element_type=F32)
        ov = (((p0[2 * LN:] + p1[LN:]) + p2) + (p0[LN:2 * LN] + p1[:LN]) + p0[:LN]) * get(t, FAC + s % 2)
        for j in range(PH):
            m = FAR[j] + n * (CLOSE[j] - FAR[j])
            for mn in range(PH):
                outb[t, m, half_rows(h), mn * LN:(mn + 1) * LN] = ov[mn * EH:(mn + 1) * EH, j * LN:(j + 1) * LN]

    def step_body(it, carry):
        t, s = it % 2, it // 2
        ot = 1 - t
        os = (it + 1) // 2 - 1
        first = 1 - (it + 2 * STEPS - 1) // (2 * STEPS)
        has = it >= 1
        more = jnp.logical_and(has, it < 2 * STEPS - 1)

        @pl.when(it < 2)
        def _():
            ev_init(t)

        @pl.when(it >= 2)
        def _():
            ev_vec(t, s - 1)

        @pl.when(has)
        def _():
            ev_sum(ot, os, 0, more)

        @pl.when(it == 0)
        def _():
            r_ld.wait()

        def slot_body(q, c2):
            h = first * (q % 2) + (1 - first) * (q // 3)
            n = first * ((q - 2) // 2) + (1 - first) * (q % 3 - 1)
            is_rw = jnp.logical_or(jnp.logical_and(it == 0, q < 2), jnp.logical_and(has, q % 3 == 0))

            def at(cond, slot, event, *args):
                @pl.when(jnp.logical_and(cond, q == slot))
                def _():
                    event(*args)

            @pl.when(is_rw)
            def _():
                @pl.when(h == 0)
                def _():
                    r_phase(t, s, 0, EH)

                @pl.when(h == 1)
                def _():
                    def part(k, c3):
                        r_phase(t, s, EH + k * (EH // 2), EH // 2)

                        @pl.when(jnp.logical_and(has, k == 0))
                        def _():
                            ev_mid(ot)

                        return c3

                    lax.fori_loop(0, 2, part, 0)

                w_phase(h)
                at(it >= 2, 0, ev_beta, t, s - 1)
                at(has, 3, ev_alpha, ot, os)

            @pl.when(jnp.logical_not(is_rw))
            def _():
                at(it == 0, 2, l_first)
                at(it == 0, 4, l_second)
                l_phase(t, s, h, n)
                at(it == 0, 4, psi_pass, 1)
                at(has, 1, ev_sum, ot, os, 1, more)
                at(more, 2, ev_fwd, ot, 0)
                at(more, 4, ev_fwd, ot, 1)
                at(has, 5, ev_size, ot)

                @pl.when(n == 0)
                def _():
                    for m in FAR[::-1]:
                        rs_copy(t, h, m).start()

                @pl.when(n == 1)
                def _():
                    for m in NEAR:
                        rs_copy(t, h, m).start()

            return c2

        lax.fori_loop(0, 6, slot_body, 0)
        return carry

    psi_pass(0)
    lax.fori_loop(0, 2 * STEPS, step_body, 0)

    last = STEPS - 1

    def finish(t):
        rinv = 1.0 / ev_beta(t, last)
        came(seven_fin, FI, t)
        for i in range(2):
            for j in range(2):
                psi_out[t, :, i, j, :] = jnp.concatenate([frecv[t, g, i][:, j * EC:(j + 1) * EC] for g in range(8)], axis=1) * rinv
        sent(seven_fin, FI, t)

    ev_sum(1, last, 0, False)
    ev_sum(1, last, 1, False)
    finish(0)
    ev_mid(1)
    ev_alpha(1, last)
    ev_size(1)
    finish(1)


def solution(mesh):
    psi_spec = P(None, "lb", None, None, "rb")

    def local_run(psi_loc, left_loc, right_loc, mpo_pair):
        rows = psi_loc.shape[1]
        mpo, bond = left_loc.shape[1:]
        left_t = jnp.transpose(left_loc, (1, 0, 2))
        right_t = jnp.transpose(right_loc, (1, 0, 2))
        wmat = jnp.transpose(mpo_pair.reshape(mpo, mpo, PH, PH), (0, 3, 2, 1)).reshape(PH * mpo, PH * mpo)
        dma = pltpu.SemaphoreType.DMA
        any_spec = pl.BlockSpec(memory_space=pl.ANY)
        vm = pl.BlockSpec(memory_space=pltpu.VMEM)
        f32_shapes = [
            (mpo, EC, bond),
            (2, mpo, LN, WID),
            (mpo, rows, bond),
            (2, bond, WID),
            (2, 2, bond, WID),
            (2, PH, LN, bond),
            psi_loc.shape,
            (PH * mpo * NX, LN),
            (PH * mpo * NY, LN),
            (2, 8, EC, WID),
            (2, 2, 7, EH, WID),
        ]
        small = [(3, 2, 16, 8, LN), (3, 2, 8, 8, LN), (3, 2, 2, 8, LN), (SIZE + 1, 2, 8, LN), (2, 2, LN, LN), (2, 8, 2, 16, LN)]
        call = pl.pallas_call(
            functools.partial(kernel, (bond, mpo, float(bond * bond * PH))),
            out_shape=[jax.ShapeDtypeStruct(shape, F32) for shape in (psi_loc.shape, (2, 2, STEPS))],
            in_specs=[any_spec, any_spec, any_spec, vm],
            out_specs=[vm] * 2,
            scratch_shapes=[pltpu.VMEM(shape, F32) for shape in f32_shapes]
            + [pltpu.VMEM((3, 2, mpo, LN, WID), BF16), pltpu.VMEM((PH * mpo, 6 * PH * mpo), BF16)]
            + [pltpu.VMEM(shape, F32) for shape in small]
            + [dma((KINDS, 2))] * 2
            + [dma((2, 3, 8)), dma((3,))],
            compiler_params=pltpu.CompilerParams(vmem_limit_bytes=63 << 20, has_side_effects=True, collective_id=0),
            name="lanczos",
        )
        psi_next, sums = call(psi_loc, left_t, right_t, wmat)
        return sums[0], sums[1], psi_next

    return jax.shard_map(local_run, mesh=mesh, in_specs=(psi_spec, P("lb", None, None), P("rb", None, None), P()), out_specs=(P(), P(), psi_spec), check_vma=False)
```

```python
import functools

import jax
import jax.numpy as jnp
from jax import lax
from jax.experimental import pallas as pl
from jax.experimental.pallas import tpu as pltpu
from jax.sharding import PartitionSpec as P

STEPS = 4
HI = lax.Precision.HIGHEST
F32 = jnp.float32
BF16 = jnp.bfloat16
MESH = pl.DeviceIdType.MESH
LN = 128
EC = 64
EH = EC // 2
PH = 4
WID = PH * LN
NX = 40
NY = 72
FAR = (3, 5, 6, 7)
CLOSE = (4, 2, 1, 0)
NEAR = CLOSE[:3]
SEVEN = FAR[::-1] + NEAR
ALPHA, BETA, NORM, FAC = range(4)
SIZE = FAC + 2
RS, GA, FW = 0, 2, 4
PS, PF, FI, AG = range(6, 10)
AR = AG + 3
LS, LF = AR + 3, AR + 4
KINDS = AR + 6
THIRDS = ((0, 4), (4, 3), (7, 3))
ORDERS = ((4, 2, 1), (2, 1, 4), (1, 4, 2))


def split3(val):
    top = val.astype(BF16)
    rest = val - top.astype(F32)
    mid = rest.astype(BF16)
    low = (rest - mid.astype(F32)).astype(BF16)
    return top, mid, low


def fold(val):
    acc = sum(val[:, j:j + LN] for j in range(0, val.shape[1], LN))
    return sum(acc[j:j + 8] for j in range(0, val.shape[0], 8))


def fold_max(val):
    acc = functools.reduce(jnp.maximum, [val[:, j:j + LN] for j in range(0, val.shape[1], LN)])
    return functools.reduce(jnp.maximum, [acc[j:j + 8] for j in range(0, val.shape[0], 8)])


def bits(m):
    return m // 4, (m // 2) % 2, m % 2


def number(trip, base=2):
    return (trip[0] * base + trip[1]) * base + trip[2]


def flip(trip, m):
    return number([q + b * (1 - 2 * q) for q, b in zip(trip, bits(m))])


def places(lb):
    place = (lb // 16, (lb // 4) % 4, lb % 4)
    return place, [q % 2 for q in place], [q // 2 for q in place], [((q + 1) // 2) % 2 for q in place]


def kernel(cfg, psi_ref, left_ref, right_ref, wmat_ref, psi_out, sums_out,
           rf, ls, lst, gat, vec, pg, praw, xf, yf, outb, rsb, l3, wpk, gbuf, rbuf, asend, scal, fsend, frecv, ssem, rsem, lsem, ldsem):
    bond, mpo, elems = cfg
    core, lb = lax.axis_index("rb"), lax.axis_index("lb")
    place, low, high, side = places(lb)
    pos, aset, eset = number(low), number(high), number(side)
    half, lhalf = bond // 2, mpo // 2
    own = core * half + eset * EC
    other = 1 - core
    myrows = pl.ds(pl.multiple_of(pos * 16, 16), 16)
    mycols = pl.ds(pl.multiple_of(core * half, half), half)

    def gpeer(m):
        return number([q + b * (1 - 2 * p) for q, b, p in zip(place, bits(m), low)], 4)

    def rpeer(m):
        return number([q + b * (3 - 2 * q) for q, b in zip(place, bits(m))], 4)

    def remote(src, dst, ssm, rsm, c, chip):
        return pltpu.make_async_remote_copy(src_ref=src, dst_ref=dst, send_sem=ssm, recv_sem=rsm, device_id=(c, chip), device_id_type=MESH)

    def tagged(src, dst, kind, t, c, chip):
        return remote(src, dst, ssem.at[kind, t], rsem.at[kind, t], c, chip)

    def sent(region, kind, t):
        tagged(region, region, kind, t, other, lb).wait_send()

    def came(region, kind, t):
        tagged(region, region, kind, t, other, lb).wait_recv()

    def half_rows(h):
        return pl.ds(pl.multiple_of(h * EH, EH), EH)

    def rs_copy(t, h, m):
        return tagged(outb.at[t, m, half_rows(h)], rsb.at[t, h, m - 1], RS + h, t, core, rpeer(m))

    def gat_rows(m, h):
        return pl.ds(pl.multiple_of(core * half + flip(side, m) * EC + h * EH, EH), EH)

    def g_copy(t, h, m):
        reg = gat.at[t, gat_rows(0, h)]
        return tagged(reg, reg, GA + h, t, core, gpeer(m))

    def fw_copy(t, h, m):
        reg = gat.at[t, gat_rows(m, h)]
        return tagged(reg, reg, FW + h, t, other, lb)

    seven_halves = gat.at[0, pl.ds(0, 7 * EH)]
    eight_halves = gat.at[0, pl.ds(0, 8 * EH)]

    def p_copy(t, m):
        reg = pg.at[t, :, myrows, mycols]
        return tagged(reg, reg, PS, t, core, gpeer(m))

    def pf_copy(t):
        reg = pg.at[t, :, :, mycols]
        return tagged(reg, reg, PF, t, other, lb)

    seven_psi = pg.at[0, :, pl.ds(0, 7 * 16), pl.ds(0, half)]

    def f_copy(t, m):
        src = fsend.at[t, :, pl.ds(pl.multiple_of(flip(low, m) * 16, 16), 16)]
        return tagged(src, frecv.at[t, eset], FI, t, core, gpeer(m))

    seven_fin = frecv.at[0, pl.ds(0, 7)]

    def l_region(n, m, j):
        first, count = THIRDS[j]
        return ls.at[n, pl.ds(core * lhalf + first, count), pl.ds(pl.multiple_of(flip(low, m) * 16, 16), 16)]

    def l_copy(n, m, j, d):
        reg = l_region(n, m, j)
        return remote(reg, reg, ssem.at[LS, n], lsem.at[n, j, m + d], core, gpeer(d))

    def lf_copy(n, m, j):
        reg = l_region(n, m, j)
        return tagged(reg, reg, LF + (m in FAR), n, other, lb)

    seven_l = ls.at[0, pl.ds(0, lhalf), pl.ds(0, 7 * 16)]
    near_l, far_l = [ls.at[0, pl.ds(0, lhalf), pl.ds(0, len(part) * 16)] for part in (NEAR, FAR)]

    group = [(c, m) for c in range(2) for m in range(8) if c or m]

    def flip_core(c):
        return core + c * (1 - 2 * core)

    def g_send(t, kind, *parts):
        tiles = pl.ds(0, len(parts))
        for k, part in enumerate(parts):
            asend[kind, t, 0, k] = part
            gbuf[kind, t, core * 8 + eset, k] = part
        for c, m in group:
            tagged(asend.at[kind, t, 0, tiles], gbuf.at[kind, t, core * 8 + eset, tiles], AG + kind, t, flip_core(c), gpeer(m)).start()

    def g_bytes(t, kind):
        return gbuf.at[kind, t, pl.ds(0, 15), pl.ds(0, 2 if kind == ALPHA else 1)]

    def g_sum(t, kind):
        came(g_bytes(t, kind), AG + kind, t)
        return sum(gbuf[kind, t, j, 0] for j in range(16))

    def r_send(t, kind, part):
        asend[kind, t, 1, 0] = part
        rbuf[kind, t, aset] = part
        for m in SEVEN:
            tagged(asend.at[kind, t, 1, 0], rbuf.at[kind, t, aset], AR + kind, t, core, rpeer(m)).start()

    def r_sum(t, kind):
        came(rbuf.at[kind, t, pl.ds(0, 7)], AR + kind, t)
        return sum(rbuf[kind, t, j] for j in range(8))

    def mean(tile):
        return jnp.sum(jnp.sum(tile, axis=0, keepdims=True), axis=1, keepdims=True) / elems

    def total(t, kind):
        tile = r_sum(t, kind)
        sent(g_bytes(t, kind), AG + kind, t)
        sent(rbuf.at[kind, t, pl.ds(0, 7)], AR + kind, t)
        return mean(tile)

    def put(t, kind, val):
        scal[kind, t] = jnp.broadcast_to(val, (8, LN))

    def get(t, kind):
        return scal[kind, t][0:1, 0:1]

    def record(kind, t, s, val):
        rows = lax.broadcasted_iota(jnp.int32, (2, STEPS), 0)
        cols = lax.broadcasted_iota(jnp.int32, (2, STEPS), 1)
        sums_out[kind] = jnp.where(jnp.logical_and(rows == t, cols == s), val, sums_out[kind])

    psi_ld = pltpu.make_async_copy(psi_ref, praw, ldsem.at[0])
    psi_ld.start()
    l_ld = pltpu.make_async_copy(left_ref, lst, ldsem.at[1])
    l_ld.start()
    r_ld = pltpu.make_async_copy(right_ref.at[:, pl.ds(pl.multiple_of(eset * EC, EC), EC)], rf, ldsem.at[2])
    r_ld.start()
    barrier = pltpu.get_barrier_semaphore()
    for c, m in group:
        pl.semaphore_signal(barrier, inc=1, device_id=(flip_core(c), gpeer(m)), device_id_type=MESH)
    for m in SEVEN:
        pl.semaphore_signal(barrier, inc=1, device_id=(core, rpeer(m)), device_id_type=MESH)
    psi_ld.wait()
    parts = []
    for t in range(2):
        acc = 0
        for ij in range(PH):
            val = praw[t, :, ij // 2, ij % 2, :]
            pg[t, ij, myrows, mycols] = val
            acc = acc + val * val
        parts.append(fold(acc))
    sums_out[...] = jnp.zeros(sums_out.shape, F32)
    pl.semaphore_wait(barrier, len(group) + len(SEVEN))
    for t in range(2):
        g_send(t, NORM, parts[t])
    for m in SEVEN:
        p_copy(0, m).start()
    l_ld.wait()

    def perm_body(l, carry):
        lane = lax.broadcasted_iota(jnp.int32, (16, LN), 1) // 32
        for hz in range(2):
            for hy in range(2):
                src = [lst[l, :, pl.ds((4 * hz + 2 * q + hy) * LN, LN)] for q in range(2)]
                for hx in range(2):
                    pick = None
                    for c in range(PH):
                        shift = (c - 2 * (c % 2) - hx) * 32 % LN
                        val = pltpu.roll(src[c // 2], shift, 1) if shift else src[c // 2]
                        pick = val if pick is None else jnp.where(lane == c, val, pick)
                    rel = [p + q * (1 - 2 * p) for p, q in zip((hz, hy, hx), high)]
                    far = sum(rel) // 2
                    rank = [p + far * (1 - 2 * p) for p in rel]
                    j = 3 - (3 * rank[0] + 2 * rank[1] + rank[2])
                    ls[1 - far, l, myrows, pl.ds(pl.multiple_of(j * LN, LN), LN)] = pick
        return carry

    lax.fori_loop(0, mpo, perm_body, 0)
    for n in range(2):
        for j in range(3):
            for d in NEAR:
                l_copy(n, 0, j, d).start()
    w0, w1, w2 = split3(wmat_ref[...])
    wpk[...] = jnp.concatenate([w0, w0, w0, w1, w1, w2], axis=1)
    for t in range(2):
        r_send(t, NORM, g_sum(t, NORM))

    def l_take(n, m, j, links):
        reg = l_region(n, m, j)
        remote(reg, reg, ssem.at[LS, n], lsem.at[n, j, m], other, lb).wait_recv()
        for d in links:
            l_copy(n, m, j, d).start()
        lf_copy(n, m, j).start()

    def split_rows(n, offsets):
        def split_body(l, carry):
            for m in offsets:
                rows = pl.ds(pl.multiple_of(flip(low, m) * 16, 16), 16)
                for k, part in enumerate(split3(ls[n, l, rows])):
                    l3[k, n, l, rows] = part
            return carry

        lax.fori_loop(0, mpo, split_body, 0)

    def l_rest(n):
        for j in range(3):
            a, b, c = ORDERS[j]
            for m in (a + c, b + c, a + b + c):
                l_take(n, m, j, ())
        came(far_l, LF + 1, n)
        split_rows(n, FAR)

    def l_near(n):
        for j in range(3):
            a, b, c = ORDERS[j]
            l_take(n, a, j, (b, c))
            l_take(n, b, j, (c,))
            l_take(n, c, j, ())

    def l_first():
        for n in range(2):
            came(near_l, LF, n)
            split_rows(n, CLOSE)
        for n in range(2):
            for j in range(3):
                a, b, c = ORDERS[j]
                l_take(n, a + b, j, (c,))
        for m in SEVEN:
            p_copy(1, m).start()
        l_rest(0)

    def l_second():
        l_rest(1)
        for n in range(2):
            sent(seven_l, LS, n)
            sent(near_l, LF, n)
            sent(far_l, LF + 1, n)

    def psi_pass(t):
        came(seven_psi, PS, t)
        pf_copy(t).start()

    def ev_init(t):
        rinv = 1.0 / jnp.sqrt(total(t, NORM))
        put(t, BETA, jnp.zeros((1, 1), F32))
        for slot in range(2):
            put(t, FAC + slot, jnp.ones((1, 1), F32))

        def turn(first):
            def tr_body(b, carry):
                rows = pl.ds(pl.multiple_of(first + b * LN, LN), LN)
                for ij in range(PH):
                    vec[t, 0, rows, ij * LN:(ij + 1) * LN] = pg[t, ij, :, rows].T * rinv
                vec[t, 1, rows] = jnp.zeros((LN, WID), F32)
                return carry

            lax.fori_loop(0, half // LN, tr_body, 0)

        turn(core * half)
        pf_copy(t).wait_recv()
        turn(other * half)
        sent(seven_psi, PS, t)
        pf_copy(t).wait_send()

    def ev_sum(t, s, h, more):
        came(rsb.at[t, h], RS + h, t)
        hv = outb[t, 0, half_rows(h)] + sum(rsb[t, h, m - 1] for m in SEVEN)
        gat[t, gat_rows(0, h)] = hv
        if h:
            rows = pl.ds(pl.multiple_of(own, EC), EC)
            hv = gat[t, rows]
            g_send(t, ALPHA, fold(hv * vec[t, s % 2, rows]) * get(t, FAC + s % 2), fold_max(jnp.abs(hv)))

        @pl.when(more)
        def _():
            for m in SEVEN:
                g_copy(t, h, m).start()
            fw_copy(t, h, 0).start()

        sent(rsb.at[t, h], RS + h, t)

    def new_w(t, s, rows):
        cur, prev = s % 2, (s + 1) % 2
        return gat[t, rows] - get(t, ALPHA) * get(t, FAC + cur) * vec[t, cur, rows] - get(t, BETA) * get(t, FAC + prev) * vec[t, prev, rows]

    def ev_mid(t):
        r_send(t, ALPHA, g_sum(t, ALPHA))
        tile = functools.reduce(jnp.maximum, [gbuf[ALPHA, t, j, 1] for j in range(16)])
        put(t, SIZE, jnp.max(jnp.max(tile, axis=0, keepdims=True), axis=1, keepdims=True))

    def ev_alpha(t, s):
        alpha = total(t, ALPHA)
        put(t, ALPHA, alpha)
        put(t, SIZE, jnp.maximum(get(t, SIZE), jnp.maximum(jnp.abs(alpha), get(t, BETA))))
        record(0, t, s, alpha)
        res = new_w(t, s, pl.ds(pl.multiple_of(own, EC), EC))
        g_send(t, BETA, fold(res * res))

        @pl.when(s == STEPS - 1)
        def _():
            for q in range(2):
                pair = [res[:, j * LN:(j + 1) * LN] for j in (2 * q, 2 * q + 1)]
                fsend[t, q] = jnp.concatenate(pair, axis=0).T
            for m in SEVEN:
                f_copy(t, m).start()
            frecv[t, eset] = fsend[t, :, myrows]

    def ev_pass(t):
        r_send(t, BETA, g_sum(t, BETA))

    def ev_fwd(t, h):
        came(seven_halves, GA + h, t)
        for m in SEVEN:
            fw_copy(t, h, m).start()

    def ev_beta(t, s):
        beta = jnp.sqrt(total(t, BETA))
        put(t, BETA, beta)
        record(1, t, s, beta)
        put(t, FAC + (s + 1) % 2, get(t, SIZE) / beta)
        return beta

    def ev_scale(t, s):
        ev_beta(t, s - 1)
        fac = get(t, FAC + s % 2)
        for m in range(8):
            outb[t, m, half_rows(0)] = outb[t, m, half_rows(0)] * fac

    def ev_vec(t, s):
        size = get(t, SIZE)
        rinv = jnp.where(size > 0, 1.0 / size, 0.0)

        def rows_of(first):
            def body(j, carry):
                rows = pl.ds(pl.multiple_of(first + j * LN, LN), LN)
                vec[t, (s + 1) % 2, rows] = new_w(t, s, rows) * rinv
                return carry

            lax.fori_loop(0, half // LN, body, 0)

        rows_of(core * half)
        for h in range(2):
            came(eight_halves, FW + h, t)
        rows_of(other * half)
        for h in range(2):
            sent(eight_halves, FW + h, t)
            sent(seven_halves, GA + h, t)

    def r_phase(t, s, first, count):
        rows = rf[:, pl.ds(pl.multiple_of(first, 16), count), :].reshape(mpo * count, bond)
        xv = jnp.dot(rows, vec[t, s % 2], preferred_element_type=F32, precision=HI)
        base = first % EH
        for r in range(mpo):
            for ij in range(PH):
                xf[pl.ds(pl.multiple_of((ij * mpo + r) * NX + base, 8), count), :] = xv[r * count:(r + 1) * count, ij * LN:(ij + 1) * LN]

    def w_phase(h):
        for e in range(0, EH, 2):
            xs = jnp.concatenate([xf[pl.ds(e + q, PH * mpo, stride=NX), :] for q in range(2)], axis=1)
            x0, x1, x2 = split3(xs)
            yv = jnp.dot(wpk[...], jnp.concatenate([x0, x1, x2, x0, x1, x0], axis=0), preferred_element_type=F32)
            for q in range(2):
                yf[pl.ds(h * EH + e + q, PH * mpo, stride=NY), :] = yv[:, q * LN:(q + 1) * LN]

    def l_phase(t, s, h, n):
        lhs = [jnp.concatenate([yf[pl.ds(pl.multiple_of((l * PH + mn) * NY + h * EH, 8), EH), :] for mn in range(PH)], axis=0) for l in range(mpo)]
        y0, y1, y2 = split3(jnp.concatenate(lhs, axis=1))
        b0, b1, b2 = [l3[k, n].reshape(mpo * LN, PH * LN) for k in range(3)]
        p0 = jnp.dot(jnp.concatenate([y0, y1, y2], axis=0), b0, preferred_element_type=F32)
        p1 = jnp.dot(jnp.concatenate([y0, y1], axis=0), b1, preferred_element_type=F32)
        p2 = jnp.dot(y0, b2, preferred_element_type=F32)
        ov = (((p0[2 * LN:] + p1[LN:]) + p2) + (p0[LN:2 * LN] + p1[:LN]) + p0[:LN]) * jnp.where(h == 1, get(t, FAC + s % 2), 1.0)
        for j in range(PH):
            m = FAR[j] + n * (CLOSE[j] - FAR[j])
            for mn in range(PH):
                outb[t, m, half_rows(h), mn * LN:(mn + 1) * LN] = ov[mn * EH:(mn + 1) * EH, j * LN:(j + 1) * LN]

    def step_body(it, carry):
        t, s = it % 2, it // 2
        ot = 1 - t
        os = (it + 1) // 2 - 1
        first = 1 - (it + 2 * STEPS - 1) // (2 * STEPS)
        has = it >= 1
        more = jnp.logical_and(has, it < 2 * STEPS - 1)

        @pl.when(it < 2)
        def _():
            ev_init(t)

        @pl.when(it >= 2)
        def _():
            ev_vec(t, s - 1)

        @pl.when(it == 0)
        def _():
            r_ld.wait()

        def send_part(h, part):
            for m in part:
                rs_copy(t, h, m).start()

        def slot_body(q, c2):
            h = first * (q % 2) + (1 - first) * (q // 3)
            n = first * ((q - 2) // 2) + (1 - first) * (q % 3 - 1)
            is_rw = jnp.logical_or(jnp.logical_and(it == 0, q < 2), jnp.logical_and(has, q % 3 == 0))

            def at(cond, slot, event, *args):
                @pl.when(jnp.logical_and(cond, q == slot))
                def _():
                    event(*args)

            @pl.when(is_rw)
            def _():
                def part(k, c3):
                    r_phase(t, s, h * EH + k * (EH // 2), EH // 2)

                    @pl.when(k == 0)
                    def _():
                        at(it == 0, 1, l_near, 1)
                        at(it >= 2, 0, ev_pass, t)
                        at(has, 0, ev_sum, ot, os, 0, more)
                        at(has, 3, ev_mid, ot)
                        at(it >= 2, 3, ev_scale, t, s)
                        at(has, 3, send_part, 0, SEVEN)

                    return c3

                lax.fori_loop(0, 2, part, 0)
                w_phase(h)
                at(it == 0, 0, l_near, 0)
                at(more, 3, ev_fwd, ot, 0)

            @pl.when(jnp.logical_not(is_rw))
            def _():
                at(it == 0, 2, l_first)
                at(it == 0, 4, l_second)
                l_phase(t, s, h, n)
                at(it == 0, 4, psi_pass, 1)
                at(it == 0, 4, send_part, 0, SEVEN)
                at(has, 1, ev_sum, ot, os, 1, more)
                at(has, 4, ev_alpha, ot, os)
                at(more, 4, ev_fwd, ot, 1)
                at(has, 4, send_part, 1, FAR[::-1])
                at(it == 0, 5, send_part, 1, FAR[::-1])
                at(it >= 0, 5, send_part, 1, NEAR)

            return c2

        lax.fori_loop(0, 6, slot_body, 0)
        return carry

    psi_pass(0)
    lax.fori_loop(0, 2 * STEPS, step_body, 0)

    last = STEPS - 1

    def finish(t):
        rinv = 1.0 / ev_beta(t, last)
        came(seven_fin, FI, t)
        for i in range(2):
            for j in range(2):
                psi_out[t, :, i, j, :] = jnp.concatenate([frecv[t, g, i][:, j * EC:(j + 1) * EC] for g in range(8)], axis=1) * rinv
        sent(seven_fin, FI, t)

    ev_pass(0)
    ev_sum(1, last, 0, False)
    ev_sum(1, last, 1, False)
    finish(0)
    ev_mid(1)
    ev_alpha(1, last)
    ev_pass(1)
    finish(1)


def solution(mesh):
    psi_spec = P(None, "lb", None, None, "rb")

    def local_run(psi_loc, left_loc, right_loc, mpo_pair):
        rows = psi_loc.shape[1]
        mpo, bond = left_loc.shape[1:]
        left_t = jnp.transpose(left_loc, (1, 0, 2))
        right_t = jnp.transpose(right_loc, (1, 0, 2))
        wmat = jnp.transpose(mpo_pair.reshape(mpo, mpo, PH, PH), (0, 3, 2, 1)).reshape(PH * mpo, PH * mpo)
        dma = pltpu.SemaphoreType.DMA
        any_spec = pl.BlockSpec(memory_space=pl.ANY)
        vm = pl.BlockSpec(memory_space=pltpu.VMEM)
        f32_shapes = [
            (mpo, EC, bond),
            (2, mpo, LN, WID),
            (mpo, rows, bond),
            (2, bond, WID),
            (2, 2, bond, WID),
            (2, PH, LN, bond),
            psi_loc.shape,
            (PH * mpo * NX, LN),
            (PH * mpo * NY, LN),
            (2, 8, EC, WID),
            (2, 2, 7, EH, WID),
        ]
        small = [(3, 2, 16, 2, 8, LN), (3, 2, 8, 8, LN), (3, 2, 2, 2, 8, LN), (SIZE + 1, 2, 8, LN), (2, 2, LN, LN), (2, 8, 2, 16, LN)]
        call = pl.pallas_call(
            functools.partial(kernel, (bond, mpo, float(bond * bond * PH))),
            out_shape=[jax.ShapeDtypeStruct(shape, F32) for shape in (psi_loc.shape, (2, 2, STEPS))],
            in_specs=[any_spec, any_spec, any_spec, vm],
            out_specs=[vm] * 2,
            scratch_shapes=[pltpu.VMEM(shape, F32) for shape in f32_shapes]
            + [pltpu.VMEM((3, 2, mpo, LN, WID), BF16), pltpu.VMEM((PH * mpo, 6 * PH * mpo), BF16)]
            + [pltpu.VMEM(shape, F32) for shape in small]
            + [dma((KINDS, 2))] * 2
            + [dma((2, 3, 8)), dma((3,))],
            compiler_params=pltpu.CompilerParams(vmem_limit_bytes=63 << 20, has_side_effects=True, collective_id=0),
            name="lanczos",
        )
        psi_next, sums = call(psi_loc, left_t, right_t, wmat)
        return sums[0], sums[1], psi_next

    return jax.shard_map(local_run, mesh=mesh, in_specs=(psi_spec, P("lb", None, None), P("rb", None, None), P()), out_specs=(P(), P(), psi_spec), check_vma=False)
```

```python
import functools

import jax
import jax.numpy as jnp
from jax import lax
from jax.experimental import pallas as pl
from jax.experimental.pallas import tpu as pltpu
from jax.sharding import PartitionSpec as P

STEPS = 4
HI = lax.Precision.HIGHEST
F32 = jnp.float32
BF16 = jnp.bfloat16
MESH = pl.DeviceIdType.MESH
LN = 128
EC = 64
EH = EC // 2
PH = 4
WID = PH * LN
NX = 40
NY = 72
FAR = (3, 5, 6, 7)
CLOSE = (4, 2, 1, 0)
NEAR = CLOSE[:3]
SEVEN = FAR[::-1] + NEAR
ALPHA, BETA, NORM, FAC = range(4)
SIZE = FAC + 2
RS, GA, FW = 0, 2, 4
PS, PF, FI, AG = range(6, 10)
AR = AG + 3
LS, LF = AR + 3, AR + 4
KINDS = AR + 6
THIRDS = ((0, 4), (4, 3), (7, 3))
PLANES = ((0, 2), (2, 1), (3, 1))
ORDERS = ((4, 2, 1), (2, 1, 4), (1, 4, 2))


def split3(val):
    top = val.astype(BF16)
    rest = val - top.astype(F32)
    mid = rest.astype(BF16)
    low = (rest - mid.astype(F32)).astype(BF16)
    return top, mid, low


def fold(val, op=jnp.add):
    acc = functools.reduce(op, [val[:, j:j + LN] for j in range(0, val.shape[1], LN)])
    acc = functools.reduce(op, [acc[j:j + 8] for j in range(0, val.shape[0], 8)])
    return (jnp.max if op is jnp.maximum else jnp.sum)(acc, axis=0, keepdims=True)


def bits(m):
    return m // 4, (m // 2) % 2, m % 2


def number(trip, base=2):
    return (trip[0] * base + trip[1]) * base + trip[2]


def flip(trip, m):
    return number([q + b * (1 - 2 * q) for q, b in zip(trip, bits(m))])


def places(lb):
    place = (lb // 16, (lb // 4) % 4, lb % 4)
    return place, [q % 2 for q in place], [q // 2 for q in place], [((q + 1) // 2) % 2 for q in place]


def kernel(cfg, psi_ref, left_ref, right_ref, wmat_ref, psi_out, sums_out,
           rf, ls, lst, gat, vec, pg, praw, xf, yf, outb, rsb, l3, wpk, gbuf, rbuf, asend, scal, fsend, frecv, ssem, rsem, lsem, psem, ldsem):
    bond, mpo, elems = cfg
    core, lb = lax.axis_index("rb"), lax.axis_index("lb")
    place, low, high, side = places(lb)
    pos, aset, eset = number(low), number(high), number(side)
    half, lhalf = bond // 2, mpo // 2
    own = core * half + eset * EC
    other = 1 - core
    myrows = pl.ds(pl.multiple_of(pos * 16, 16), 16)
    mycols = pl.ds(pl.multiple_of(core * half, half), half)

    def gpeer(m):
        return number([q + b * (1 - 2 * p) for q, b, p in zip(place, bits(m), low)], 4)

    def rpeer(m):
        return number([q + b * (3 - 2 * q) for q, b in zip(place, bits(m))], 4)

    def remote(src, dst, ssm, rsm, c, chip):
        return pltpu.make_async_remote_copy(src_ref=src, dst_ref=dst, send_sem=ssm, recv_sem=rsm, device_id=(c, chip), device_id_type=MESH)

    def tagged(src, dst, kind, t, c, chip):
        return remote(src, dst, ssem.at[kind, t], rsem.at[kind, t], c, chip)

    def sent(region, kind, t):
        tagged(region, region, kind, t, other, lb).wait_send()

    def came(region, kind, t):
        tagged(region, region, kind, t, other, lb).wait_recv()

    def half_rows(h):
        return pl.ds(h * EH, EH)

    def rs_copy(t, h, m):
        return tagged(outb.at[t, m, half_rows(h)], rsb.at[t, h, m - 1], RS + h, t, core, rpeer(m))

    def gat_rows(m, h):
        return pl.ds(pl.multiple_of(core * half + flip(side, m) * EC + h * EH, EH), EH)

    def g_copy(t, h, m):
        reg = gat.at[t, gat_rows(0, h)]
        return tagged(reg, reg, GA + h, t, core, gpeer(m))

    def fw_copy(t, h, m):
        reg = gat.at[t, gat_rows(m, h)]
        return tagged(reg, reg, FW + h, t, other, lb)

    seven_halves = gat.at[0, pl.ds(0, 7 * EH)]
    eight_halves = gat.at[0, pl.ds(0, 8 * EH)]

    def p_region(t, m, j):
        return pg.at[t, pl.ds(*PLANES[j]), pl.ds(pl.multiple_of(flip(low, m) * 16, 16), 16), mycols]

    def p_copy(t, m, j, d):
        reg = p_region(t, m, j)
        return remote(reg, reg, ssem.at[PS, t], psem.at[t, j, m + d], core, gpeer(d))

    def p_take(t, m, j, links):
        reg = p_region(t, m, j)
        remote(reg, reg, ssem.at[PS, t], psem.at[t, j, m], core, lb).wait_recv()
        for d in links:
            p_copy(t, m, j, d).start()

    def p_send(t):
        for j in range(3):
            for d in NEAR:
                p_copy(t, 0, j, d).start()

    def p_near(t):
        for j in range(3):
            a, b, c = ORDERS[j]
            p_take(t, a, j, (b, c))
            p_take(t, b, j, (c,))

    def p_last(t):
        for j in range(3):
            a, b, c = ORDERS[j]
            p_take(t, a + b, j, (c,))

    def p_rest(t):
        for j in range(3):
            a, b, c = ORDERS[j]
            for m in (c, a + c, b + c, a + b + c):
                p_take(t, m, j, ())
        pf_copy(t).start()

    def pf_copy(t):
        reg = pg.at[t, :, :, mycols]
        return tagged(reg, reg, PF, t, other, lb)

    seven_psi = pg.at[0, :, pl.ds(0, 7 * 16), pl.ds(0, half)]

    def f_copy(t, m):
        src = fsend.at[t, :, pl.ds(pl.multiple_of(flip(low, m) * 16, 16), 16)]
        return tagged(src, frecv.at[t, eset], FI, t, core, gpeer(m))

    seven_fin = frecv.at[0, pl.ds(0, 7)]

    def l_region(n, m, j):
        first, count = THIRDS[j]
        return ls.at[n, pl.ds(core * lhalf + first, count), pl.ds(pl.multiple_of(flip(low, m) * 16, 16), 16)]

    def l_copy(n, m, j, d):
        reg = l_region(n, m, j)
        return remote(reg, reg, ssem.at[LS, n], lsem.at[n, j, m + d], core, gpeer(d))

    def l_send(shares):
        for n, j in shares:
            for d in NEAR:
                l_copy(n, 0, j, d).start()

    def lf_copy(n, m, j):
        reg = l_region(n, m, j)
        return tagged(reg, reg, LF + (m in FAR), n, other, lb)

    seven_l = ls.at[0, pl.ds(0, lhalf), pl.ds(0, 7 * 16)]
    near_l, far_l = [ls.at[0, pl.ds(0, lhalf), pl.ds(0, len(part) * 16)] for part in (NEAR, FAR)]

    group = [(c, m) for c in range(2) for m in range(8) if c or m]

    def flip_core(c):
        return core + c * (1 - 2 * core)

    def g_send(t, kind, *rows):
        for k, row in enumerate(rows):
            asend[kind, t, 0, pl.ds(k, 1)] = row
            gbuf[kind, t, core * 8 + eset, pl.ds(k, 1)] = row
        for c, m in group:
            tagged(asend.at[kind, t, 0], gbuf.at[kind, t, core * 8 + eset], AG + kind, t, flip_core(c), gpeer(m)).start()

    def g_sum(t, kind):
        came(gbuf.at[kind, t, pl.ds(0, 15)], AG + kind, t)
        both = [gbuf[kind, t, j] for j in range(16)]
        return sum(both)[0:1], functools.reduce(jnp.maximum, both)[1:2]

    def r_send(t, kind, row):
        asend[kind, t, 1, pl.ds(0, 1)] = row
        rbuf[kind, t, aset, pl.ds(0, 1)] = row
        for m in SEVEN:
            tagged(asend.at[kind, t, 1], rbuf.at[kind, t, aset], AR + kind, t, core, rpeer(m)).start()

    def r_sum(t, kind):
        came(rbuf.at[kind, t, pl.ds(0, 7)], AR + kind, t)
        return sum(rbuf[kind, t, j] for j in range(8))[0:1]

    def mean(row):
        return jnp.sum(row, axis=1, keepdims=True) / elems

    def total(t, kind):
        row = r_sum(t, kind)
        sent(gbuf.at[kind, t, pl.ds(0, 15)], AG + kind, t)
        sent(rbuf.at[kind, t, pl.ds(0, 7)], AR + kind, t)
        return mean(row)

    def put(t, kind, val):
        scal[kind, t] = jnp.broadcast_to(val, (8, LN))

    def get(t, kind):
        return scal[kind, t][0:1, 0:1]

    def wide(tile, rows):
        return jnp.concatenate([jnp.concatenate([tile] * PH, axis=1)] * (rows // 8), axis=0)

    def record(kind, t, s, val):
        rows = lax.broadcasted_iota(jnp.int32, (2, STEPS), 0)
        cols = lax.broadcasted_iota(jnp.int32, (2, STEPS), 1)
        sums_out[kind] = jnp.where(jnp.logical_and(rows == t, cols == s), val, sums_out[kind])

    psi_ld = pltpu.make_async_copy(psi_ref, praw, ldsem.at[0])
    psi_ld.start()
    l_ld = pltpu.make_async_copy(left_ref, lst, ldsem.at[1])
    l_ld.start()
    r_ld = pltpu.make_async_copy(right_ref.at[:, pl.ds(pl.multiple_of(eset * EC, EC), EC)], rf, ldsem.at[2])
    r_ld.start()
    barrier = pltpu.get_barrier_semaphore()
    for c, m in group:
        pl.semaphore_signal(barrier, inc=1, device_id=(flip_core(c), gpeer(m)), device_id_type=MESH)
    for m in SEVEN:
        pl.semaphore_signal(barrier, inc=1, device_id=(core, rpeer(m)), device_id_type=MESH)
    psi_ld.wait()
    parts = []
    for t in range(2):
        acc = 0
        for ij in range(PH):
            val = praw[t, :, ij // 2, ij % 2, :]
            pg[t, ij, myrows, mycols] = val
            acc = acc + val * val
        parts.append(fold(acc))
    sums_out[...] = jnp.zeros(sums_out.shape, F32)
    asend[...] = jnp.zeros(asend.shape, F32)
    pl.semaphore_wait(barrier, len(group) + len(SEVEN))
    for t in range(2):
        g_send(t, NORM, parts[t])
    p_send(0)
    l_ld.wait()

    def perm_body(l, carry):
        lane = lax.broadcasted_iota(jnp.int32, (16, LN), 1) // 32
        for hz in range(2):
            for hy in range(2):
                src = [lst[l, :, pl.ds((4 * hz + 2 * q + hy) * LN, LN)] for q in range(2)]
                for hx in range(2):
                    pick = None
                    for c in range(PH):
                        shift = (c - 2 * (c % 2) - hx) * 32 % LN
                        val = pltpu.roll(src[c // 2], shift, 1) if shift else src[c // 2]
                        pick = val if pick is None else jnp.where(lane == c, val, pick)
                    rel = [p + q * (1 - 2 * p) for p, q in zip((hz, hy, hx), high)]
                    far = sum(rel) // 2
                    rank = [p + far * (1 - 2 * p) for p in rel]
                    j = 3 - (3 * rank[0] + 2 * rank[1] + rank[2])
                    ls[1 - far, l, myrows, pl.ds(pl.multiple_of(j * LN, LN), LN)] = pick
        return carry

    lax.fori_loop(0, mpo, perm_body, 0)
    p_near(0)
    l_sends = [(n, j) for n in range(2) for j in range(3)]
    l_send(l_sends[:1])
    p_last(0)
    l_send(l_sends[1:])
    w0, w1, w2 = split3(wmat_ref[...])
    wpk[...] = jnp.concatenate([w0, w0, w0, w1, w1, w2], axis=1)
    for t in range(2):
        r_send(t, NORM, g_sum(t, NORM)[0])

    def l_take(n, m, j, links):
        reg = l_region(n, m, j)
        remote(reg, reg, ssem.at[LS, n], lsem.at[n, j, m], other, lb).wait_recv()
        for d in links:
            l_copy(n, m, j, d).start()
        lf_copy(n, m, j).start()

    def split_rows(n, offsets):
        def split_body(l, carry):
            for m in offsets:
                rows = pl.ds(pl.multiple_of(flip(low, m) * 16, 16), 16)
                for k, part in enumerate(split3(ls[n, l, rows])):
                    l3[k, n, l, rows] = part
            return carry

        lax.fori_loop(0, mpo, split_body, 0)

    def l_rest(n):
        for j in range(3):
            a, b, c = ORDERS[j]
            for m in (a + c, b + c, a + b + c):
                l_take(n, m, j, ())
        came(far_l, LF + 1, n)
        split_rows(n, FAR)

    def l_near(n):
        for j in range(3):
            a, b, c = ORDERS[j]
            l_take(n, a, j, (b, c))
            l_take(n, b, j, (c,))
            l_take(n, c, j, ())
        if n:
            p_send(1)

    def l_first():
        for n in range(2):
            came(near_l, LF, n)
            split_rows(n, CLOSE)
        for n in range(2):
            for j in range(3):
                a, b, c = ORDERS[j]
                l_take(n, a + b, j, (c,))
        p_near(1)
        l_rest(0)
        p_last(1)

    def l_second():
        l_rest(1)
        for n in range(2):
            sent(seven_l, LS, n)
            sent(near_l, LF, n)
            sent(far_l, LF + 1, n)

    def ev_init(t):
        rinv = 1.0 / jnp.sqrt(total(t, NORM))
        put(t, BETA, jnp.zeros((1, 1), F32))
        for slot in range(2):
            put(t, FAC + slot, jnp.ones((1, 1), F32))

        def turn(first):
            def tr_body(b, carry):
                rows = pl.ds(pl.multiple_of(first + b * LN, LN), LN)
                for ij in range(PH):
                    vec[t, 0, rows, ij * LN:(ij + 1) * LN] = pg[t, ij, :, rows].T * rinv
                vec[t, 1, rows] = jnp.zeros((LN, WID), F32)
                return carry

            lax.fori_loop(0, half // LN, tr_body, 0)

        turn(core * half)
        pf_copy(t).wait_recv()
        turn(other * half)
        sent(seven_psi, PS, t)
        pf_copy(t).wait_send()

    def ev_sum(t, s, h, more):
        came(rsb.at[t, h], RS + h, t)
        hv = outb[t, 0, half_rows(h)] + sum(rsb[t, h, m - 1] for m in SEVEN)
        gat[t, gat_rows(0, h)] = hv
        if h:
            rows = pl.ds(pl.multiple_of(own, EC), EC)
            hv = gat[t, rows]
            g_send(t, ALPHA, fold(hv * vec[t, s % 2, rows]) * get(t, FAC + s % 2), fold(jnp.abs(hv), jnp.maximum))

        @pl.when(more)
        def _():
            for k, m in ((0, NEAR), (1, FAR[::-1]), (1, NEAR)) if h else ((0, FAR[::-1]),):
                for q in m:
                    g_copy(t, k, q).start()
            fw_copy(t, h, 0).start()

        sent(rsb.at[t, h], RS + h, t)

    def new_w(t, s, first, count):
        cur, prev = s % 2, (s + 1) % 2
        rows = pl.ds(pl.multiple_of(first, EC), count)
        along, back = wide(scal[ALPHA, t] * scal[FAC + cur, t], count), wide(scal[BETA, t] * scal[FAC + prev, t], count)
        return gat[t, rows] - along * vec[t, cur, rows] - back * vec[t, prev, rows]

    def ev_mid(t):
        row, most = g_sum(t, ALPHA)
        r_send(t, ALPHA, row)
        put(t, SIZE, jnp.max(most, axis=1, keepdims=True))

    def ev_alpha(t, s):
        alpha = total(t, ALPHA)
        put(t, ALPHA, alpha)
        put(t, SIZE, jnp.maximum(get(t, SIZE), jnp.maximum(jnp.abs(alpha), get(t, BETA))))
        record(0, t, s, alpha)
        res = new_w(t, s, own, EC)
        g_send(t, BETA, fold(res * res))

        @pl.when(s == STEPS - 1)
        def _():
            for q in range(2):
                pair = [res[:, j * LN:(j + 1) * LN] for j in (2 * q, 2 * q + 1)]
                fsend[t, q] = jnp.concatenate(pair, axis=0).T
            for m in SEVEN:
                f_copy(t, m).start()
            frecv[t, eset] = fsend[t, :, myrows]

    def ev_pass(t):
        r_send(t, BETA, g_sum(t, BETA)[0])

    def ev_fwd(t, h):
        came(seven_halves, GA + h, t)
        for m in SEVEN:
            fw_copy(t, h, m).start()

    def ev_beta(t, s):
        beta = jnp.sqrt(total(t, BETA))
        put(t, BETA, beta)
        record(1, t, s, beta)
        put(t, FAC + (s + 1) % 2, get(t, SIZE) / beta)
        return beta

    def ev_scale(t, s):
        ev_beta(t, s - 1)
        fac = get(t, FAC + s % 2)
        for m in range(8):
            outb[t, m, half_rows(0)] = outb[t, m, half_rows(0)] * fac

    def ev_vec(t, s):
        size = scal[SIZE, t]
        rinv = wide(jnp.where(size > 0, 1.0 / size, 0.0), LN)

        def rows_of(first):
            def body(j, carry):
                start = first + j * LN
                vec[t, (s + 1) % 2, pl.ds(pl.multiple_of(start, LN), LN)] = new_w(t, s, start, LN) * rinv
                return carry

            lax.fori_loop(0, half // LN, body, 0)

        rows_of(core * half)
        for h in range(2):
            came(eight_halves, FW + h, t)
        rows_of(other * half)
        for h in range(2):
            sent(eight_halves, FW + h, t)
            sent(seven_halves, GA + h, t)

    def r_phase(t, s, first, count):
        xv = jnp.dot(rf[:, pl.ds(first, count), :].reshape(mpo * count, bond), vec[t, s % 2], preferred_element_type=F32, precision=HI)
        for r in range(mpo):
            for ij in range(PH):
                xf[pl.ds((ij * mpo + r) * NX + first % EH, count), :] = xv[r * count:(r + 1) * count, ij * LN:(ij + 1) * LN]

    def w_phase(h):
        for e in range(0, EH, 2):
            xs = jnp.concatenate([xf[pl.ds(e + q, PH * mpo, stride=NX), :] for q in range(2)], axis=1)
            x0, x1, x2 = split3(xs)
            yv = jnp.dot(wpk[...], jnp.concatenate([x0, x1, x2, x0, x1, x0], axis=0), preferred_element_type=F32)
            for q in range(2):
                yf[pl.ds(h * EH + e + q, PH * mpo, stride=NY), :] = yv[:, q * LN:(q + 1) * LN]

    def l_phase(t, h, n, fac):
        lhs = [jnp.concatenate([yf[pl.ds((l * PH + mn) * NY + h * EH, EH), :] for mn in range(PH)], axis=0) for l in range(mpo)]
        y0, y1, y2 = split3(jnp.concatenate(lhs, axis=1))
        b0, b1, b2 = [l3[k, n].reshape(mpo * LN, PH * LN) for k in range(3)]
        p0 = jnp.dot(jnp.concatenate([y0, y1, y2], axis=0), b0, preferred_element_type=F32)
        p1 = jnp.dot(jnp.concatenate([y0, y1], axis=0), b1, preferred_element_type=F32)
        p2 = jnp.dot(y0, b2, preferred_element_type=F32)
        ov = ((p0[2 * LN:] + p1[LN:]) + p2) + (p0[LN:2 * LN] + p1[:LN]) + p0[:LN]
        if fac is not None:
            ov = ov * fac
        for j, m in enumerate(CLOSE if n else FAR):
            for mn in range(PH):
                outb[t, m, half_rows(h), mn * LN:(mn + 1) * LN] = ov[mn * EH:(mn + 1) * EH, j * LN:(j + 1) * LN]

    def send_part(t, h, part):
        for m in part:
            rs_copy(t, h, m).start()

    quarter = EH // 2

    def step_body(it, carry):
        t, s = it % 2, it // 2
        ot = 1 - t
        os = (it + 1) // 2 - 1
        more = it < 2 * STEPS - 1
        later = it >= 2

        @pl.when(it == 1)
        def _():
            ev_init(t)

        @pl.when(later)
        def _():
            ev_vec(t, s - 1)

        r_phase(t, s, 0, quarter)

        @pl.when(later)
        def _():
            ev_pass(t)

        ev_sum(ot, os, 0, more)
        r_phase(t, s, quarter, quarter)
        w_phase(0)
        l_phase(t, 0, 0, None)
        ev_sum(ot, os, 1, more)
        l_phase(t, 0, 1, None)
        r_phase(t, s, EH, quarter)
        ev_mid(ot)

        @pl.when(later)
        def _():
            ev_scale(t, s)

        send_part(t, 0, SEVEN)

        r_phase(t, s, EH + quarter, quarter)
        w_phase(1)
        l_phase(t, 1, 0, get(t, FAC + s % 2))
        ev_alpha(ot, os)

        @pl.when(more)
        def _():
            ev_fwd(ot, 0)
            ev_fwd(ot, 1)

        send_part(t, 1, FAR[::-1])
        l_phase(t, 1, 1, get(t, FAC + s % 2))
        send_part(t, 1, NEAR)
        return carry

    p_rest(0)
    ev_init(0)
    r_ld.wait()
    for h in range(2):
        r_phase(0, 0, h * EH, quarter)
        if h:
            l_near(1)
        r_phase(0, 0, h * EH + quarter, quarter)
        w_phase(h)
        if h == 0:
            l_near(0)
    l_first()
    for n, part in enumerate((FAR[::-1], NEAR)):
        for h in range(2):
            l_phase(0, h, n, None)
            send_part(0, h, part)
            if n and not h:
                p_rest(1)
        if n == 0:
            l_second()
    lax.fori_loop(1, 2 * STEPS, step_body, 0)

    last = STEPS - 1

    def finish(t):
        rinv = 1.0 / ev_beta(t, last)
        came(seven_fin, FI, t)
        for i in range(2):
            for j in range(2):
                psi_out[t, :, i, j, :] = jnp.concatenate([frecv[t, g, i][:, j * EC:(j + 1) * EC] for g in range(8)], axis=1) * rinv
        sent(seven_fin, FI, t)

    ev_pass(0)
    ev_sum(1, last, 0, False)
    ev_sum(1, last, 1, False)
    ev_mid(1)
    finish(0)
    ev_alpha(1, last)
    ev_pass(1)
    finish(1)


def solution(mesh):
    psi_spec = P(None, "lb", None, None, "rb")

    def local_run(psi_loc, left_loc, right_loc, mpo_pair):
        rows = psi_loc.shape[1]
        mpo, bond = left_loc.shape[1:]
        left_t = jnp.transpose(left_loc, (1, 0, 2))
        right_t = jnp.transpose(right_loc, (1, 0, 2))
        wmat = jnp.transpose(mpo_pair.reshape(mpo, mpo, PH, PH), (0, 3, 2, 1)).reshape(PH * mpo, PH * mpo)
        dma = pltpu.SemaphoreType.DMA
        any_spec = pl.BlockSpec(memory_space=pl.ANY)
        vm = pl.BlockSpec(memory_space=pltpu.VMEM)
        f32_shapes = [
            (mpo, EC, bond),
            (2, mpo, LN, WID),
            (mpo, rows, bond),
            (2, bond, WID),
            (2, 2, bond, WID),
            (2, PH, LN, bond),
            psi_loc.shape,
            (PH * mpo * NX, LN),
            (PH * mpo * NY, LN),
            (2, 8, EC, WID),
            (2, 2, 7, EH, WID),
        ]
        small = [(3, 2, 16, 2, LN), (3, 2, 8, 2, LN), (3, 2, 2, 2, LN), (SIZE + 1, 2, 8, LN), (2, 2, LN, LN), (2, 8, 2, 16, LN)]
        call = pl.pallas_call(
            functools.partial(kernel, (bond, mpo, float(bond * bond * PH))),
            out_shape=[jax.ShapeDtypeStruct(shape, F32) for shape in (psi_loc.shape, (2, 2, STEPS))],
            in_specs=[any_spec, any_spec, any_spec, vm],
            out_specs=[vm] * 2,
            scratch_shapes=[pltpu.VMEM(shape, F32) for shape in f32_shapes]
            + [pltpu.VMEM((3, 2, mpo, LN, WID), BF16), pltpu.VMEM((PH * mpo, 6 * PH * mpo), BF16)]
            + [pltpu.VMEM(shape, F32) for shape in small]
            + [dma((KINDS, 2))] * 2
            + [dma((2, 3, 8)), dma((2, 3, 8)), dma((3,))],
            compiler_params=pltpu.CompilerParams(vmem_limit_bytes=63 << 20, has_side_effects=True, collective_id=0),
            name="lanczos",
        )
        psi_next, sums = call(psi_loc, left_t, right_t, wmat)
        return sums[0], sums[1], psi_next

    return jax.shard_map(local_run, mesh=mesh, in_specs=(psi_spec, P("lb", None, None), P("rb", None, None), P()), out_specs=(P(), P(), psi_spec), check_vma=False)
```

```python
import functools

import jax
import jax.numpy as jnp
from jax import lax
from jax.experimental import pallas as pl
from jax.experimental.pallas import tpu as pltpu
from jax.sharding import PartitionSpec as P

STEPS = 4
HI = lax.Precision.HIGHEST
F32 = jnp.float32
BF16 = jnp.bfloat16
MESH = pl.DeviceIdType.MESH
LN = 128
RB = 16
EC = 64
EH = EC // 2
PH = 4
WID = PH * LN
NX = 40
NY = 72
FAR = (3, 5, 6, 7)
CLOSE = (4, 2, 1, 0)
NEAR = CLOSE[:3]
SEVEN = FAR[::-1] + NEAR
ALPHA, BETA, NORM, FAC = range(4)
SIZE = FAC + 2
RS, GA, FW = 0, 2, 4
PS, PF, FI, AG = range(6, 10)
AR = AG + 3
LS, LF = AR + 3, AR + 4
LR, PR = AR + 6, AR + 15
KINDS = PR + 9
THIRDS = ((0, 4), (4, 3), (7, 3))
PLANES = ((0, 2), (2, 1), (3, 1))
ORDERS = ((4, 2, 1), (2, 1, 4), (1, 4, 2))


def split3(val):
    top = val.astype(BF16)
    rest = val - top.astype(F32)
    mid = rest.astype(BF16)
    low = (rest - mid.astype(F32)).astype(BF16)
    return top, mid, low


def fold(val, op=jnp.add):
    acc = functools.reduce(op, [val[:, j:j + LN] for j in range(0, val.shape[1], LN)])
    acc = functools.reduce(op, [acc[j:j + 8] for j in range(0, val.shape[0], 8)])
    return (jnp.max if op is jnp.maximum else jnp.sum)(acc, axis=0, keepdims=True)


def tree(j):
    a, b, c = ORDERS[j]
    return ((0, a), (0, b), (0, c)), ((a, b), (a, c), (b, c)), ((a + b, c),), ()


def members(j):
    a, b, c = ORDERS[j]
    return NEAR, (a + b,), (a + c, b + c, a + b + c)


def slot(m, j):
    return 3 * [m in part for part in members(j)].index(True) + j


def bits(m):
    return m // 4, (m // 2) % 2, m % 2


def number(trip, base=2):
    return (trip[0] * base + trip[1]) * base + trip[2]


def flip(trip, m):
    return number([q + b * (1 - 2 * q) for q, b in zip(trip, bits(m))])


def places(lb):
    place = (lb // RB, (lb // 4) % 4, lb % 4)
    return place, [q % 2 for q in place], [q // 2 for q in place], [(q + 1) // 2 % 2 for q in place]


def kernel(cfg, psi_ref, left_ref, right_ref, mpo_ref, rows_out, sums_out,
           rf, ls, lst, gat, vec, pg, praw, wraw, wst, xf, yf, outb, rsb, l3, wpk, gbuf, rbuf, asend, scal, fsend, ssem, rsem, ldsem):
    bond, mpo, elems = cfg
    core, lb = lax.axis_index("rb"), lax.axis_index("lb")
    place, low, high, side = places(lb)
    pos, aset, eset = number(low), number(high), number(side)
    half, lhalf = bond // 2, mpo // 2
    own = core * half + eset * EC
    other = 1 - core
    myrows = pl.ds(pl.multiple_of(pos * RB, RB), RB)
    mycols = pl.ds(pl.multiple_of(core * half, half), half)

    def gpeer(m):
        return number([q + b * (1 - 2 * p) for q, b, p in zip(place, bits(m), low)], 4)

    def rpeer(m):
        return number([q + b * (3 - 2 * q) for q, b in zip(place, bits(m))], 4)

    def remote(src, dst, ssm, rsm, c, chip):
        return pltpu.make_async_remote_copy(src_ref=src, dst_ref=dst, send_sem=ssm, recv_sem=rsm, device_id=(c, chip), device_id_type=MESH)

    def tagged(src, dst, kind, t, c, chip):
        return remote(src, dst, ssem.at[kind, t], rsem.at[kind, t], c, chip)

    def sent(region, kind, t):
        tagged(region, region, kind, t, other, lb).wait_send()

    def came(region, kind, t):
        tagged(region, region, kind, t, other, lb).wait_recv()

    def half_rows(h, base=0):
        return pl.ds(base + h * EH if isinstance(h, int) else pl.multiple_of(base + h * EH, 8), EH)

    def rs_copy(t, h, m):
        return tagged(outb.at[t, m, half_rows(h)], rsb.at[t, h, m - 1], RS + h, t, core, rpeer(m))

    def gat_rows(m, h):
        return pl.ds(pl.multiple_of(core * half + flip(side, m) * EC + h * EH, EH), EH)

    def g_copy(t, h, m):
        reg = gat.at[t, gat_rows(0, h)]
        return tagged(reg, reg, GA + h, t, core, gpeer(m))

    def fw_copy(t, h, m):
        reg = gat.at[t, gat_rows(m, h)]
        return tagged(reg, reg, FW + h, t, other, lb)

    seven_halves = gat.at[0, pl.ds(0, 7 * EH)]
    eight_halves = gat.at[0, pl.ds(0, 8 * EH)]

    def p_region(t, m, j):
        return pg.at[t, pl.ds(*PLANES[j]), pl.ds(pl.multiple_of(flip(low, m) * RB, RB), RB), mycols]

    def p_copy(t, m, j, d):
        reg = p_region(t, m, j)
        return remote(reg, reg, ssem.at[PS, t], rsem.at[PR + slot(m + d, j), t], core, gpeer(d))

    def p_over(t, m, j):
        reg = p_region(t, m, j)
        return tagged(reg, reg, PF, t, other, lb)

    def p_pass(t, level, j):
        for m, d in tree(j)[level]:
            p_copy(t, m, j, d).start()

    def p_send(t):
        for j in range(3):
            p_pass(t, 0, j)
            p_over(t, 0, j).start()

    def p_take(t, level):
        for j in range(3):
            part = members(j)[level]
            came(pg.at[t, pl.ds(0, PLANES[j][1]), pl.ds(0, RB * len(part)), pl.ds(0, half)], PR + 3 * level + j, t)
            p_pass(t, level + 1, j)
            for m in part:
                p_over(t, m, j).start()

    seven_psi = pg.at[0, :, pl.ds(0, 7 * RB), pl.ds(0, half)]
    half_psi = pg.at[0, :, :, pl.ds(0, half)]

    def f_copy(t, m):
        src = fsend.at[t, :, pl.ds(pl.multiple_of(flip(low, m) * RB, RB), RB)]
        if m == 0:
            return pltpu.make_async_copy(src, rows_out.at[t, eset], ldsem.at[t])
        return tagged(src, rows_out.at[t, eset], FI, t, core, gpeer(m))

    seven_fin = rows_out.at[0, pl.ds(0, 7)]

    def l_region(n, m, j):
        first, count = THIRDS[j]
        return ls.at[n, pl.ds(core * lhalf + first, count), pl.ds(pl.multiple_of(flip(low, m) * RB, RB), RB)]

    def l_copy(n, m, j, d):
        reg = l_region(n, m, j)
        return remote(reg, reg, ssem.at[LS, n], rsem.at[LR + slot(m + d, j), n], core, gpeer(d))

    def l_pass(n, level, j):
        for m, d in tree(j)[level]:
            l_copy(n, m, j, d).start()

    def lf_copy(n, m, j):
        reg = l_region(n, m, j)
        return tagged(reg, reg, LF + (m in FAR), n, other, lb)

    seven_l = ls.at[0, pl.ds(0, lhalf), pl.ds(0, 7 * RB)]
    near_l, far_l = [ls.at[0, pl.ds(0, lhalf), pl.ds(0, len(part) * RB)] for part in (NEAR, FAR)]

    group = [(c, m) for c in range(2) for m in range(8) if c or m]

    def flip_core(c):
        return core + c * (1 - 2 * core)

    def g_send(t, kind, *rows):
        for k, row in enumerate(rows):
            asend[kind, t, 0, pl.ds(k, 1)] = row
            gbuf[kind, t, core * 8 + eset, pl.ds(k, 1)] = row
        for c, m in group:
            tagged(asend.at[kind, t, 0], gbuf.at[kind, t, core * 8 + eset], AG + kind, t, flip_core(c), gpeer(m)).start()

    def g_sum(t, kind):
        came(gbuf.at[kind, t, pl.ds(0, 15)], AG + kind, t)
        both = [gbuf[kind, t, j] for j in range(RB)]
        return sum(both)[0:1], functools.reduce(jnp.maximum, both)[1:2]

    def r_send(t, kind, row):
        asend[kind, t, 1, pl.ds(0, 1)] = row
        rbuf[kind, t, aset, pl.ds(0, 1)] = row
        for m in SEVEN:
            tagged(asend.at[kind, t, 1], rbuf.at[kind, t, aset], AR + kind, t, core, rpeer(m)).start()

    def r_sum(t, kind):
        came(rbuf.at[kind, t, pl.ds(0, 7)], AR + kind, t)
        return sum(rbuf[kind, t, j] for j in range(8))[0:1]

    def mean(row):
        return jnp.sum(row, axis=1, keepdims=True) / elems

    def total(t, kind):
        row = r_sum(t, kind)
        sent(gbuf.at[kind, t, pl.ds(0, 15)], AG + kind, t)
        sent(rbuf.at[kind, t, pl.ds(0, 7)], AR + kind, t)
        return mean(row)

    def put(t, kind, val):
        scal[kind, t] = jnp.broadcast_to(val, (8, LN))

    def get(t, kind):
        return scal[kind, t][0:1, 0:1]

    def wide(tile, rows):
        return jnp.concatenate([jnp.concatenate([tile] * PH, axis=1)] * (rows // 8), axis=0)

    def record(kind, t, s, val):
        rows = lax.broadcasted_iota(jnp.int32, (2, STEPS), 0)
        cols = lax.broadcasted_iota(jnp.int32, (2, STEPS), 1)
        sums_out[kind] = jnp.where(jnp.logical_and(rows == t, cols == s), val, sums_out[kind])

    psi_ld = pltpu.make_async_copy(psi_ref, praw, ldsem.at[0])
    psi_ld.start()
    l_ld = pltpu.make_async_copy(left_ref, lst, ldsem.at[1])
    l_ld.start()
    r_ld = pltpu.make_async_copy(right_ref.at[:, pl.ds(pl.multiple_of(eset * EC, EC), EC)], rf, ldsem.at[2])
    r_ld.start()
    w_ld = pltpu.make_async_copy(mpo_ref, wraw, ldsem.at[3])
    w_ld.start()
    barrier = pltpu.get_barrier_semaphore()
    for c, m in group:
        pl.semaphore_signal(barrier, inc=1, device_id=(flip_core(c), gpeer(m)), device_id_type=MESH)
    for m in SEVEN:
        pl.semaphore_signal(barrier, inc=1, device_id=(core, rpeer(m)), device_id_type=MESH)
    psi_ld.wait()
    parts = []
    for t in range(2):
        acc = 0
        for ij in range(PH):
            val = praw[t, :, ij // 2, ij % 2, :]
            pg[t, ij, myrows, mycols] = val
            acc = acc + val * val
        parts.append(fold(acc))
    sums_out[...] = jnp.zeros(sums_out.shape, F32)
    asend[...] = jnp.zeros(asend.shape, F32)
    pl.semaphore_wait(barrier, len(group) + len(SEVEN))
    for t in range(2):
        g_send(t, NORM, parts[t])
    p_send(0)
    l_ld.wait()

    def perm_body(l, carry):
        lane = lax.broadcasted_iota(jnp.int32, (RB, LN), 1) // 32
        for hz in range(2):
            for hy in range(2):
                src = [lst[l, :, pl.ds((4 * hz + 2 * q + hy) * LN, LN)] for q in range(2)]
                for hx in range(2):
                    pick = None
                    for c in range(PH):
                        shift = (c - 2 * (c % 2) - hx) * 32 % LN
                        val = pltpu.roll(src[c // 2], shift, 1) if shift else src[c // 2]
                        pick = val if pick is None else jnp.where(lane == c, val, pick)
                    rel = [p + q * (1 - 2 * p) for p, q in zip((hz, hy, hx), high)]
                    far = sum(rel) // 2
                    rank = [p + far * (1 - 2 * p) for p in rel]
                    j = 3 - (3 * rank[0] + 2 * rank[1] + rank[2])
                    ls[1 - far, l, myrows, pl.ds(pl.multiple_of(j * LN, LN), LN)] = pick
        return carry

    lax.fori_loop(0, mpo, perm_body, 0)
    p_take(0, 0)
    shares = [(n, 0, j) for n in range(2) for j in range(3)]
    l_pass(*shares[0])
    for t in range(2):
        r_send(t, NORM, g_sum(t, NORM)[0])
    p_take(0, 1)
    for share in shares[1:]:
        l_pass(*share)
    w_ld.wait()
    for mn in range(PH):
        planes = [wraw[:, ij // 2, ij % 2, mn // 2, mn % 2, :] for ij in range(PH)]
        wst[pl.ds(mn, mpo, stride=PH), :] = jnp.concatenate(planes + [jnp.zeros((mpo, LN - PH * mpo), F32)], axis=1)
    w0, w1, w2 = split3(wst[:, :PH * mpo])
    wpk[...] = jnp.concatenate([w0, w0, w0, w1, w1, w2], axis=1)

    def l_take(n, level):
        for j in range(3):
            part = members(j)[level]
            came(ls.at[n, pl.ds(0, THIRDS[j][1]), pl.ds(0, RB * len(part))], LR + 3 * level + j, n)
            l_pass(n, level + 1, j)
            for m in part:
                lf_copy(n, m, j).start()

    def split_rows(n, offsets):
        def split_body(l, carry):
            for m in offsets:
                rows = pl.ds(pl.multiple_of(flip(low, m) * RB, RB), RB)
                for k, part in enumerate(split3(ls[n, l, rows])):
                    l3[k, n, l, rows] = part
            return carry

        lax.fori_loop(0, mpo, split_body, 0)

    def l_rest(n):
        came(far_l, LF + 1, n)
        split_rows(n, FAR)

    def l_first():
        for n in range(2):
            came(near_l, LF, n)
            split_rows(n, CLOSE)
        for n in range(2):
            l_take(n, 1)
        l_take(0, 2)
        p_take(1, 0)
        l_rest(0)

    def l_second():
        l_rest(1)
        for n in range(2):
            sent(seven_l, LS, n)
            sent(near_l, LF, n)
            sent(far_l, LF + 1, n)

    def ev_init(t):
        rinv = 1.0 / jnp.sqrt(total(t, NORM))
        put(t, BETA, jnp.zeros((1, 1), F32))
        for slot in range(2):
            put(t, FAC + slot, jnp.ones((1, 1), F32))

        def turn(first):
            def tr_body(b, carry):
                rows = pl.ds(pl.multiple_of(first + b * LN, LN), LN)
                for ij in range(PH):
                    vec[t, 0, rows, ij * LN:(ij + 1) * LN] = pg[t, ij, :, rows].T * rinv
                vec[t, 1, rows] = jnp.zeros((LN, WID), F32)
                return carry

            lax.fori_loop(0, half // LN, tr_body, 0)

        turn(core * half)
        came(half_psi, PF, t)
        turn(other * half)
        sent(seven_psi, PS, t)
        sent(half_psi, PF, t)

    def ev_sum(t, s, h, more):
        came(rsb.at[t, h], RS + h, t)
        hv = outb[t, 0, half_rows(h)] + sum(rsb[t, h, m - 1] for m in SEVEN)
        gat[t, gat_rows(0, h)] = hv
        if h:
            rows = pl.ds(pl.multiple_of(own, EC), EC)
            hv = gat[t, rows]
            g_send(t, ALPHA, fold(hv * vec[t, s % 2, rows]) * get(t, FAC + s % 2), fold(jnp.abs(hv), jnp.maximum))

        @pl.when(more)
        def _():
            for k, m in ((0, NEAR), (1, FAR[::-1]), (1, NEAR)) if h else ((0, FAR[::-1]),):
                for q in m:
                    g_copy(t, k, q).start()
            fw_copy(t, h, 0).start()

        sent(rsb.at[t, h], RS + h, t)

    def new_w(t, s, first, count):
        cur, prev = s % 2, (s + 1) % 2
        rows = pl.ds(pl.multiple_of(first, EC), count)
        along, back = wide(scal[ALPHA, t] * scal[FAC + cur, t], count), wide(scal[BETA, t] * scal[FAC + prev, t], count)
        return gat[t, rows] - along * vec[t, cur, rows] - back * vec[t, prev, rows]

    def ev_mid(t):
        row, most = g_sum(t, ALPHA)
        r_send(t, ALPHA, row)
        put(t, SIZE, jnp.max(most, axis=1, keepdims=True))

    def ev_alpha(t, s):
        alpha = total(t, ALPHA)
        put(t, ALPHA, alpha)
        put(t, SIZE, jnp.maximum(get(t, SIZE), jnp.maximum(jnp.abs(alpha), get(t, BETA))))
        record(0, t, s, alpha)
        res = new_w(t, s, own, EC)
        g_send(t, BETA, fold(res * res))

        @pl.when(s == STEPS - 1)
        def _():
            for q in range(2):
                pair = [res[:, j * LN:(j + 1) * LN] for j in (2 * q, 2 * q + 1)]
                fsend[t, q] = jnp.concatenate(pair, axis=0).T
            for m in SEVEN + (0,):
                f_copy(t, m).start()

    def ev_pass(t):
        r_send(t, BETA, g_sum(t, BETA)[0])

    def ev_fwd(t, h):
        came(seven_halves, GA + h, t)
        for m in SEVEN:
            fw_copy(t, h, m).start()

    def ev_beta(t, s):
        beta = jnp.sqrt(total(t, BETA))
        put(t, BETA, beta)
        record(1, t, s, beta)
        put(t, FAC + (s + 1) % 2, get(t, SIZE) / beta)
        return beta

    def ev_scale(t, s):
        ev_beta(t, s - 1)
        fac = get(t, FAC + s % 2)
        for m in range(8):
            outb[t, m, half_rows(0)] = outb[t, m, half_rows(0)] * fac

    def vec_rows(t, s, first):
        size = scal[SIZE, t]
        rinv = wide(jnp.where(size > 0, 1.0 / size, 0.0), LN)
        for j in range(0, half, LN):
            vec[t, (s + 1) % 2, pl.ds(pl.multiple_of(first + j, LN), LN)] = new_w(t, s, first + j, LN) * rinv

    def ev_vec(t, s):
        for h in range(2):
            came(eight_halves, FW + h, t)
        vec_rows(t, s, other * half)
        for h in range(2):
            sent(eight_halves, FW + h, t)
            sent(seven_halves, GA + h, t)

    def rel(n, j):
        return FAR[j] + n * (CLOSE[j] - FAR[j])

    def r_phase(t, s, start, count, shift=0):
        xv = jnp.dot(rf[:, pl.ds(start + shift, count), :].reshape(mpo * count, bond), vec[t, s % 2], preferred_element_type=F32, precision=HI)
        for r in range(mpo):
            for ij in range(PH):
                xf[pl.ds((ij * mpo + r) * NX + shift, count), :] = xv[r * count:(r + 1) * count, ij * LN:(ij + 1) * LN]

    def w_phase(start):
        for e in range(0, EH, 2):
            xs = jnp.concatenate([xf[pl.ds(e + q, PH * mpo, stride=NX), :] for q in range(2)], axis=1)
            x0, x1, x2 = split3(xs)
            yv = jnp.dot(wpk[...], jnp.concatenate([x0, x1, x2, x0, x1, x0], axis=0), preferred_element_type=F32)
            for q in range(2):
                yf[pl.ds(start + e + q, PH * mpo, stride=NY), :] = yv[:, q * LN:(q + 1) * LN]

    def l_phase(t, h, n, fac):
        rows = [half_rows(h, (l * PH + mn) * NY) for l in range(mpo) for mn in range(PH)]
        lhs = [jnp.concatenate([yf[r, :] for r in rows[l * PH:l * PH + PH]], axis=0) for l in range(mpo)]
        y0, y1, y2 = split3(jnp.concatenate(lhs, axis=1))
        b0, b1, b2 = [l3[k, n].reshape(mpo * LN, PH * LN) for k in range(3)]
        p0 = jnp.dot(jnp.concatenate([y0, y1, y2], axis=0), b0, preferred_element_type=F32)
        p1 = jnp.dot(jnp.concatenate([y0, y1], axis=0), b1, preferred_element_type=F32)
        p2 = jnp.dot(y0, b2, preferred_element_type=F32)
        ov = ((p0[2 * LN:] + p1[LN:]) + p2) + (p0[LN:2 * LN] + p1[:LN]) + p0[:LN]
        if fac is not None:
            ov = ov * fac
        for j in range(PH):
            for mn in range(PH):
                outb[t, rel(n, j), half_rows(h), mn * LN:(mn + 1) * LN] = ov[mn * EH:(mn + 1) * EH, j * LN:(j + 1) * LN]

    def send_part(t, h, part):
        for m in part:
            rs_copy(t, h, m).start()

    quarter = EH // 2

    def step_body(it, carry):
        t, s = it % 2, it // 2
        ot = 1 - t
        os = (it + 1) // 2 - 1
        more = it < 2 * STEPS - 1
        later = it >= 2

        @pl.when(it == 1)
        def _():
            ev_init(t)

        @pl.when(later)
        def _():
            ev_vec(t, s - 1)

        r_phase(t, s, 0, quarter)

        @pl.when(later)
        def _():
            ev_pass(t)

        ev_sum(ot, os, 0, more)
        r_phase(t, s, 0, quarter, quarter)
        w_phase(0)
        l_phase(t, 0, 0, None)
        ev_sum(ot, os, 1, more)
        l_phase(t, 0, 1, None)
        r_phase(t, s, EH, quarter)
        ev_mid(ot)

        @pl.when(later)
        def _():
            ev_scale(t, s)

        send_part(t, 0, SEVEN)

        r_phase(t, s, EH, quarter, quarter)
        w_phase(EH)
        l_phase(t, 1, 0, get(t, FAC + s % 2))
        ev_alpha(ot, os)

        @pl.when(more)
        def _():
            ev_fwd(ot, 0)
            ev_fwd(ot, 1)

        send_part(t, 1, FAR[::-1])
        vec_rows(ot, os, core * half)
        l_phase(t, 1, 1, get(t, FAC + s % 2))
        send_part(t, 1, NEAR)
        return carry

    p_take(0, 2)
    ev_init(0)
    r_ld.wait()

    def first_rw(h, carry):
        start = pl.multiple_of(h * EH, EH)
        r_phase(0, 0, start, quarter)

        @pl.when(h == 1)
        def _():
            l_take(1, 0)
            p_send(1)

        r_phase(0, 0, start, quarter, quarter)
        w_phase(start)

        @pl.when(h == 0)
        def _():
            l_take(0, 0)

        return carry

    lax.fori_loop(0, 2, first_rw, 0)
    l_first()

    def first_l(q, carry):
        n, h = q // 2, q % 2

        @pl.when(q == 2)
        def _():
            l_second()

        l_phase(0, h, n, None)
        for j in range(3):
            rs_copy(0, h, rel(n, j)).start()

        @pl.when(n == 0)
        def _():
            rs_copy(0, h, FAR[3]).start()

        @pl.when(q == 0)
        def _():
            p_take(1, 1)

        @pl.when(q == 1)
        def _():
            l_take(1, 2)

        @pl.when(q == 2)
        def _():
            p_take(1, 2)

        return carry

    lax.fori_loop(0, 4, first_l, 0)
    lax.fori_loop(1, 2 * STEPS, step_body, 0)

    last = STEPS - 1

    def finish(t):
        ev_beta(t, last)
        came(seven_fin, FI, t)
        sent(seven_fin, FI, t)
        f_copy(t, 0).wait()

    ev_pass(0)
    ev_sum(1, last, 0, False)
    ev_sum(1, last, 1, False)
    ev_mid(1)
    finish(0)
    ev_alpha(1, last)
    ev_pass(1)
    finish(1)


def output_kernel(rows_ref, sums_ref, alpha_out, beta_out, psi_out):
    alpha_out[...] = sums_ref[0]
    beta_out[...] = sums_ref[1]
    for t in range(2):
        rinv = 1.0 / sums_ref[1, t:t + 1, STEPS - 1:STEPS]
        for i in range(2):
            for j in range(2):
                psi_out[t, :, i, j, :] = jnp.concatenate([rows_ref[t, g, i][:, j * EC:(j + 1) * EC] for g in range(8)], axis=1) * rinv


def solution(mesh):
    psi_spec = P(None, "lb", None, None, "rb")

    def local_run(psi_loc, left_loc, right_loc, mpo_pair):
        rows = psi_loc.shape[1]
        mpo, bond = left_loc.shape[1:]
        left_t = jnp.transpose(left_loc, (1, 0, 2))
        right_t = jnp.transpose(right_loc, (1, 0, 2))
        mpo_t = jnp.transpose(mpo_pair, (0, 2, 3, 4, 5, 1))
        dma = pltpu.SemaphoreType.DMA
        any_spec = pl.BlockSpec(memory_space=pl.ANY)
        vm = pl.BlockSpec(memory_space=pltpu.VMEM)
        f32_shapes = [
            (mpo, EC, bond),
            (2, mpo, LN, WID),
            (mpo, rows, bond),
            (2, bond, WID),
            (2, 2, bond, WID),
            (2, PH, LN, bond),
            psi_loc.shape,
            mpo_t.shape,
            (PH * mpo, LN),
            (PH * mpo * NX, LN),
            (PH * mpo * NY, LN),
            (2, 8, EC, WID),
            (2, 2, 7, EH, WID),
        ]
        small = [(3, 2, RB, 2, LN), (3, 2, 8, 2, LN), (3, 2, 2, 2, LN), (SIZE + 1, 2, 8, LN), (2, 2, LN, LN)]
        call = pl.pallas_call(
            functools.partial(kernel, (bond, mpo, float(bond * bond * PH))),
            out_shape=[jax.ShapeDtypeStruct(shape, F32) for shape in ((2, 8, 2, rows, LN), (2, 2, STEPS))],
            in_specs=[any_spec] * 4,
            out_specs=[any_spec, vm],
            scratch_shapes=[pltpu.VMEM(shape, F32) for shape in f32_shapes]
            + [pltpu.VMEM((3, 2, mpo, LN, WID), BF16), pltpu.VMEM((PH * mpo, 6 * PH * mpo), BF16)]
            + [pltpu.VMEM(shape, F32) for shape in small]
            + [dma((KINDS, 2))] * 2
            + [dma((4,))],
            compiler_params=pltpu.CompilerParams(vmem_limit_bytes=63 << 20, has_side_effects=True, collective_id=0),
            name="lanczos",
        )
        last_rows, sums = call(psi_loc, left_t, right_t, mpo_t)
        shapes = [(2, STEPS), (2, STEPS), psi_loc.shape]
        put_out = pl.pallas_call(
            output_kernel,
            out_shape=[jax.ShapeDtypeStruct(shape, F32) for shape in shapes],
            in_specs=[vm] * 2,
            out_specs=[vm] * 3,
            name="outputs",
        )
        return put_out(last_rows, sums)

    return jax.shard_map(local_run, mesh=mesh, in_specs=(psi_spec, P("lb", None, None), P("rb", None, None), P()), out_specs=(P(), P(), psi_spec), check_vma=False)
```

```python
import functools

import jax
import jax.numpy as jnp
from jax import lax
from jax.experimental import pallas as pl
from jax.experimental.pallas import tpu as pltpu
from jax.sharding import PartitionSpec as P

STEPS = 4
HI = lax.Precision.HIGHEST
F32 = jnp.float32
BF16 = jnp.bfloat16
MESH = pl.DeviceIdType.MESH
BOTH, SHARES, EIGHT = range(2), range(3), range(8)
LN = 128
RB = 16
EC = 64
EH = EC // 2
PH = 4
WID = PH * LN
NX = 40
NY = 72
FAR = (3, 5, 6, 7)
CLOSE = (4, 2, 1, 0)
NEAR = CLOSE[:3]
SEVEN = FAR[::-1] + NEAR
ALPHA, BETA, NORM, FAC = range(4)
SIZE = FAC + 2
RS, GA, FW = 0, 2, 4
PS, PF, FI, AG = range(6, 10)
AR = AG + 3
LS, LF, EX = AR + 3, AR + 6, AR + 9
PR, LR = EX + 2, EX + 11
KINDS = LR + 12
SIDE, MAIN, DIAG = SHARES
THIRDS = ((0, 4), (4, 3), (7, 3))
PLANES = ((0, 2), (2, 1), (3, 1))
ORDERS = (NEAR, NEAR[1:] + NEAR[:1], NEAR[2:] + NEAR[:2])
PIECES = (SIDE,) * 3 + (MAIN,) * 3 + (DIAG,) * 2
SIDES, MAINS, DIAGS = [[u for u, ph in enumerate(PIECES) if ph == phase] for phase in SHARES]


def split3(val):
    top = val.astype(BF16)
    rest = val - top.astype(F32)
    mid = rest.astype(BF16)
    low = (rest - mid.astype(F32)).astype(BF16)
    return top, mid, low


def fold(val, op=jnp.add):
    acc = functools.reduce(op, [val[:, j:j + LN] for j in range(0, val.shape[1], LN)])
    acc = functools.reduce(op, [acc[j:j + 8] for j in range(0, val.shape[0], 8)])
    return (jnp.max if op is jnp.maximum else jnp.sum)(acc, axis=0, keepdims=True)


def tree(j):
    a, b, c = ORDERS[j]
    return ((0, a), (0, b), (0, c)), ((a, b), (a, c), (b, c)), ((a + b, c),), ()


def members(j):
    a, b, c = ORDERS[j]
    return NEAR, (a + b,), (a + c, b + c, a + b + c)


def slot(m, j, step=3):
    return step * [m in part for part in members(j)].index(True) + j


def bits(m):
    return [m // d % 2 for d in NEAR]


def number(trip, base=2):
    return (trip[0] * base + trip[1]) * base + trip[2]


def flip(trip, m):
    return number([q + b * (1 - 2 * q) for q, b in zip(trip, bits(m))])


def places(lb):
    place = (lb // RB, (lb // 4) % 4, lb % 4)
    return place, [q % 2 for q in place], [q // 2 for q in place], [(q + 1) // 2 % 2 for q in place]


def kernel(cfg, psi_ref, left_ref, right_ref, mpo_ref, rows_out, sums_out,
           rf, ls, lst, gat, vec, pg, praw, wraw, wst, xf, yf, outb, rsb, xst, l3, wpk, gbuf, rbuf, asend, scal, fsend, ssem, rsem, ldsem):
    bond, mpo, elems = cfg
    core, lb = lax.axis_index("rb"), lax.axis_index("lb")
    place, low, high, side = places(lb)
    pos, aset, eset = number(low), number(high), number(side)
    half, lhalf = bond // 2, mpo // 2
    own = core * half + eset * EC
    other = 1 - core
    myrows = pl.ds(pl.multiple_of(pos * RB, RB), RB)
    mycols = pl.ds(pl.multiple_of(core * half, half), half)

    def chip_rows(m):
        return pl.ds(pl.multiple_of(flip(low, m) * RB, RB), RB)

    def gpeer(m):
        return number([q + b * (1 - 2 * p) for q, b, p in zip(place, bits(m), low)], 4)

    def rpeer(m):
        return number([q + b * (3 - 2 * q) for q, b in zip(place, bits(m))], 4)

    def remote(src, dst, ssm, rsm, c, chip):
        return pltpu.make_async_remote_copy(src_ref=src, dst_ref=dst, send_sem=ssm, recv_sem=rsm, device_id=(c, chip), device_id_type=MESH)

    def tagged(src, dst, kind, t, c, chip):
        return remote(src, dst, ssem.at[kind, t], rsem.at[kind, t], c, chip)

    def sent(region, kind, t):
        tagged(region, region, kind, t, other, lb).wait_send()

    def came(region, kind, t):
        tagged(region, region, kind, t, other, lb).wait_recv()

    def came_at(region, arrival):
        remote(region, region, ssem.at[0, 0], arrival, other, lb).wait_recv()

    def half_rows(h, base=0):
        return pl.ds(base + h * EH if isinstance(h, int) else pl.multiple_of(base + h * EH, 8), EH)

    def rs_copy(t, h, m):
        return tagged(outb.at[t, m, half_rows(h)], rsb.at[t, h, m - 1], RS + h, t, core, rpeer(m))

    def gat_rows(m, h):
        return pl.ds(pl.multiple_of(core * half + flip(side, m) * EC + h * EH, EH), EH)

    def g_copy(t, h, m):
        reg = gat.at[t, gat_rows(0, h)]
        return tagged(reg, reg, GA + h, t, core, gpeer(m))

    def fw_copy(t, h, m):
        reg = gat.at[t, gat_rows(m, h)]
        return tagged(reg, reg, FW + h, t, other, lb)

    seven_halves = gat.at[0, pl.ds(0, 7 * EH)]
    eight_halves = gat.at[0, pl.ds(0, 8 * EH)]

    def p_region(t, m, j):
        return pg.at[t, pl.ds(*PLANES[j]), chip_rows(m), mycols]

    def p_copy(t, m, j, d):
        reg = p_region(t, m, j)
        return remote(reg, reg, ssem.at[PS, t], rsem.at[PR + slot(m + d, j), t], core, gpeer(d))

    def p_over(t, m, j):
        reg = p_region(t, m, j)
        return tagged(reg, reg, PF, t, other, lb)

    def p_pass(t, level, j):
        for m, d in tree(j)[level]:
            p_copy(t, m, j, d).start()

    def p_send(t):
        for j in SHARES:
            p_pass(t, 0, j)
            p_over(t, 0, j).start()

    def p_take(t, level):
        for j in SHARES:
            part = members(j)[level]
            came(pg.at[t, pl.ds(0, PLANES[j][1]), pl.ds(0, RB * len(part)), pl.ds(0, half)], PR + 3 * level + j, t)
            p_pass(t, level + 1, j)
            for m in part:
                p_over(t, m, j).start()

    seven_psi = pg.at[0, :, pl.ds(0, 7 * RB), pl.ds(0, half)]
    half_psi = pg.at[0, :, :, pl.ds(0, half)]

    def f_copy(t, m):
        src = fsend.at[t, :, chip_rows(m)]
        if m == 0:
            return pltpu.make_async_copy(src, rows_out.at[t, eset], ldsem.at[t])
        return tagged(src, rows_out.at[t, eset], FI, t, core, gpeer(m))

    seven_fin = rows_out.at[0, pl.ds(0, 7)]

    fifth = lhalf // 2
    pieces = [(1, core * lhalf + fifth * high[k], fifth, k * LN, LN, k) for k in SHARES]
    pieces += [(0, core * lhalf + first, count, 0, WID, k) for k, (first, count) in enumerate(THIRDS)]
    pieces += [(1, core * lhalf + fifth * k, fifth, 3 * LN, LN, 2 - k) for k in BOTH]

    def l_region(u, m):
        n, first, count, lane, lanes, _ = pieces[u]
        return ls.at[n, pl.ds(first, count), chip_rows(m), pl.ds(lane, lanes)]

    def l_arrival(u, level):
        return rsem.at[LR + (3 * u + level) // 2, (3 * u + level) % 2]

    def l_copy(u, m, d):
        reg = l_region(u, m)
        return remote(reg, reg, ssem.at[LS + PIECES[u], 0], l_arrival(u, slot(m + d, pieces[u][5], 1) - pieces[u][5]), core, gpeer(d))

    def l_pass(level, *which):
        for u in which:
            for m, d in tree(pieces[u][5])[level]:
                l_copy(u, m, d).start()

    def lf_copy(u, m):
        reg = l_region(u, m)
        return tagged(reg, reg, LF + PIECES[u], int(m in FAR), other, lb)

    def l_bytes(phase, rows):
        count, lanes = ((fifth, 3 * LN), (lhalf, WID), (lhalf, LN))[phase]
        return ls.at[0, pl.ds(0, count), pl.ds(0, rows), pl.ds(0, lanes)]

    def ex_region(k, mine):
        bit = high[k] if mine else 1 - high[k]
        return ls.at[1, pl.ds(core * lhalf + fifth * bit, fifth), :, pl.ds(k * LN, LN)]

    def ex_copy(k):
        return tagged(xst.at[k], ex_region(k, True), EX, 0, core, rpeer(NEAR[k]))

    def ex_over(k):
        return tagged(ex_region(k, False), ex_region(k, False), EX, 1, other, lb)

    group = [(c, m) for c in BOTH for m in EIGHT if c or m]

    def flip_core(c):
        return core + c * (1 - 2 * core)

    def g_send(t, kind, *rows):
        for k, row in enumerate(rows):
            asend[kind, t, 0, pl.ds(k, 1)] = row
            gbuf[kind, t, core * 8 + eset, pl.ds(k, 1)] = row
        for c, m in group:
            tagged(asend.at[kind, t, 0], gbuf.at[kind, t, core * 8 + eset], AG + kind, t, flip_core(c), gpeer(m)).start()

    def g_sum(t, kind):
        came(gbuf.at[kind, t, pl.ds(0, 15)], AG + kind, t)
        both = [gbuf[kind, t, j] for j in range(RB)]
        return sum(both)[0:1], functools.reduce(jnp.maximum, both)[1:2]

    def r_send(t, kind, row):
        asend[kind, t, 1, pl.ds(0, 1)] = row
        rbuf[kind, t, aset, pl.ds(0, 1)] = row
        for m in SEVEN:
            tagged(asend.at[kind, t, 1], rbuf.at[kind, t, aset], AR + kind, t, core, rpeer(m)).start()

    def r_sum(t, kind):
        came(rbuf.at[kind, t, pl.ds(0, 7)], AR + kind, t)
        return sum(rbuf[kind, t, j] for j in EIGHT)[0:1]

    def mean(row):
        return jnp.sum(row, axis=1, keepdims=True) / elems

    def total(t, kind):
        row = r_sum(t, kind)
        sent(gbuf.at[kind, t, pl.ds(0, 15)], AG + kind, t)
        sent(rbuf.at[kind, t, pl.ds(0, 7)], AR + kind, t)
        return mean(row)

    def put(t, kind, val):
        scal[kind, t] = jnp.broadcast_to(val, (8, LN))

    def get(t, kind):
        return scal[kind, t][0:1, 0:1]

    def wide(tile, rows):
        return jnp.concatenate([jnp.concatenate([tile] * PH, axis=1)] * (rows // 8), axis=0)

    def record(kind, t, s, val):
        rows = lax.broadcasted_iota(jnp.int32, (2, STEPS), 0)
        cols = lax.broadcasted_iota(jnp.int32, (2, STEPS), 1)
        sums_out[kind] = jnp.where(jnp.logical_and(rows == t, cols == s), val, sums_out[kind])

    psi_ld = pltpu.make_async_copy(psi_ref, praw, ldsem.at[0])
    psi_ld.start()
    l_ld = pltpu.make_async_copy(left_ref, lst, ldsem.at[1])
    l_ld.start()
    r_ld = pltpu.make_async_copy(right_ref.at[:, pl.ds(pl.multiple_of(eset * EC, EC), EC)], rf, ldsem.at[2])
    r_ld.start()
    w_ld = pltpu.make_async_copy(mpo_ref, wraw, ldsem.at[3])
    w_ld.start()
    barrier = pltpu.get_barrier_semaphore()
    for c, m in group:
        pl.semaphore_signal(barrier, inc=1, device_id=(flip_core(c), gpeer(m)), device_id_type=MESH)
    for m in SEVEN:
        pl.semaphore_signal(barrier, inc=1, device_id=(core, rpeer(m)), device_id_type=MESH)
    psi_ld.wait()
    parts = []
    for t in BOTH:
        acc = 0
        for ij in range(PH):
            val = praw[t, :, ij // 2, ij % 2, :]
            pg[t, ij, myrows, mycols] = val
            acc = acc + val * val
        parts.append(fold(acc))
    sums_out[...] = jnp.zeros(sums_out.shape, F32)
    asend[...] = jnp.zeros(asend.shape, F32)
    pl.semaphore_wait(barrier, len(group) + len(SEVEN))
    for t in BOTH:
        g_send(t, NORM, parts[t])
    p_send(0)
    l_ld.wait()

    def perm_body(l, carry):
        lane = lax.broadcasted_iota(jnp.int32, (RB, LN), 1) // 32
        for hz in BOTH:
            for hy in BOTH:
                src = [lst[l, :, pl.ds((4 * hz + 2 * q + hy) * LN, LN)] for q in BOTH]
                for hx in BOTH:
                    pick = None
                    for c in range(PH):
                        shift = (c - 2 * (c % 2) - hx) * 32 % LN
                        val = pltpu.roll(src[c // 2], shift, 1) if shift else src[c // 2]
                        pick = val if pick is None else jnp.where(lane == c, val, pick)
                    rel = [p + q * (1 - 2 * p) for p, q in zip((hz, hy, hx), high)]
                    far = sum(rel) // 2
                    rank = [p + far * (1 - 2 * p) for p in rel]
                    j = 3 - (3 * rank[0] + 2 * rank[1] + rank[2])
                    one = sum(rel) % 2 - sum(rel) // 3
                    here, there = l // fifth % 2, sum(p * q for p, q in zip(rel, high))
                    skip = one * (here + there - 2 * here * there)
                    ls[1 - far, l + skip * (mpo - l), myrows, pl.ds(pl.multiple_of(j * LN, LN), LN)] = pick
        return carry

    lax.fori_loop(0, mpo, perm_body, 0)
    p_take(0, 0)
    l_pass(0, *SIDES)
    for t in BOTH:
        r_send(t, NORM, g_sum(t, NORM)[0])
    p_take(0, 1)
    l_pass(0, *MAINS[:1])
    w_ld.wait()
    for mn in range(PH):
        planes = [wraw[:, ij // 2, ij % 2, mn // 2, mn % 2, :] for ij in range(PH)]
        wst[pl.ds(mn, mpo, stride=PH), :] = jnp.concatenate(planes + [jnp.zeros((mpo, LN - PH * mpo), F32)], axis=1)
    w0, w1, w2 = split3(wst[:, :PH * mpo])
    none = jnp.zeros_like(w0)
    groups = [jnp.concatenate(g, axis=1) for g in ([w0] * 3, [w1, w1, none], [w2, none, none])]
    wpk[...] = jnp.concatenate(groups, axis=0)

    def l_take(level, *which):
        for u in which:
            n, _, count, _, lanes, j = pieces[u]
            part = members(j)[level]
            came_at(ls.at[n, pl.ds(0, count), pl.ds(0, RB * len(part)), pl.ds(0, lanes)], l_arrival(u, level))
            l_pass(level + 1, u)
            for m in part:
                lf_copy(u, m).start()

    def split_rows(n, lane, lanes, offsets):
        cols = pl.ds(lane, lanes)

        def split_body(l, carry):
            for m in offsets:
                rows = chip_rows(m)
                for k, part in enumerate(split3(ls[n, l, rows, cols])):
                    l3[k, n, l, rows, cols] = part
            return carry

        lax.fori_loop(0, mpo, split_body, 0)

    def over(phase, part):
        came(l_bytes(phase, RB * len(part)), LF + phase, int(part is FAR))

    def ex_send():
        def turn_body(i, carry):
            for k in SHARES:
                xst[k, i] = ls[1, core * lhalf + fifth * high[k] + i, :, k * LN:(k + 1) * LN].T
            return carry

        lax.fori_loop(0, fifth, turn_body, 0)
        for k in SHARES:
            ex_copy(k).start()

    def ex_take():
        came(l_bytes(SIDE, LN), EX, 0)
        for k in SHARES:
            ex_over(k).start()

    def l_first():
        l_take(2, *SIDES)
        ex_send()
        over(MAIN, NEAR)
        split_rows(0, 0, WID, CLOSE)
        l_take(1, *(MAINS + DIAGS))
        p_send(1)
        ex_take()
        l_take(2, *MAINS)
        for part in (NEAR, FAR):
            over(SIDE, part)
        came(l_bytes(SIDE, LN), EX, 1)
        split_rows(1, 0, 3 * LN, CLOSE + FAR)
        over(MAIN, FAR)
        split_rows(0, 0, WID, FAR)
        p_take(1, 0)
        l_take(2, *DIAGS)

    def l_second():
        for part in (NEAR, FAR):
            over(DIAG, part)
        split_rows(1, 3 * LN, LN, CLOSE + FAR)
        for phase in SHARES:
            sent(l_bytes(phase, 7 * RB), LS + phase, 0)
            for k, part in enumerate((NEAR, FAR)):
                sent(l_bytes(phase, RB * len(part)), LF + phase, k)
        for k in BOTH:
            sent(l_bytes(SIDE, LN), EX, k)

    def ev_init(t):
        rinv = 1.0 / jnp.sqrt(total(t, NORM))
        put(t, BETA, jnp.zeros((1, 1), F32))
        for slot in BOTH:
            put(t, FAC + slot, jnp.ones((1, 1), F32))

        def turn(first):
            def tr_body(b, carry):
                rows = pl.ds(pl.multiple_of(first + b * LN, LN), LN)
                for ij in range(PH):
                    vec[t, 0, rows, ij * LN:(ij + 1) * LN] = pg[t, ij, :, rows].T * rinv
                vec[t, 1, rows] = jnp.zeros((LN, WID), F32)
                return carry

            lax.fori_loop(0, half // LN, tr_body, 0)

        turn(core * half)
        came(half_psi, PF, t)
        turn(other * half)
        sent(seven_psi, PS, t)
        sent(half_psi, PF, t)

    def ev_sum(t, s, h, more):
        came(rsb.at[t, h], RS + h, t)
        hv = outb[t, 0, half_rows(h)] + sum(rsb[t, h, m - 1] for m in SEVEN)
        gat[t, gat_rows(0, h)] = hv
        if h:
            rows = pl.ds(pl.multiple_of(own, EC), EC)
            hv = gat[t, rows]
            g_send(t, ALPHA, fold(hv * vec[t, s % 2, rows]) * get(t, FAC + s % 2), fold(jnp.abs(hv), jnp.maximum))

        @pl.when(more)
        def _():
            for k, m in ((0, NEAR), (1, FAR[::-1]), (1, NEAR)) if h else ((0, FAR[::-1]),):
                for q in m:
                    g_copy(t, k, q).start()
            fw_copy(t, h, 0).start()

        sent(rsb.at[t, h], RS + h, t)

    def new_w(t, s, first, count):
        cur, prev = s % 2, (s + 1) % 2
        rows = pl.ds(pl.multiple_of(first, EC), count)
        along, back = wide(scal[ALPHA, t] * scal[FAC + cur, t], count), wide(scal[BETA, t] * scal[FAC + prev, t], count)
        return gat[t, rows] - along * vec[t, cur, rows] - back * vec[t, prev, rows]

    def ev_mid(t):
        row, most = g_sum(t, ALPHA)
        r_send(t, ALPHA, row)
        put(t, SIZE, jnp.max(most, axis=1, keepdims=True))

    def ev_alpha(t, s):
        alpha = total(t, ALPHA)
        put(t, ALPHA, alpha)
        put(t, SIZE, jnp.maximum(get(t, SIZE), jnp.maximum(jnp.abs(alpha), get(t, BETA))))
        record(0, t, s, alpha)
        res = new_w(t, s, own, EC)
        g_send(t, BETA, fold(res * res))

        @pl.when(s == STEPS - 1)
        def _():
            for q in BOTH:
                pair = [res[:, j * LN:(j + 1) * LN] for j in (2 * q, 2 * q + 1)]
                fsend[t, q] = jnp.concatenate(pair, axis=0).T
            for m in SEVEN + (0,):
                f_copy(t, m).start()

    def ev_pass(t):
        r_send(t, BETA, g_sum(t, BETA)[0])

    def ev_fwd(t, h):
        came(seven_halves, GA + h, t)
        for m in SEVEN:
            fw_copy(t, h, m).start()

    def ev_beta(t, s):
        beta = jnp.sqrt(total(t, BETA))
        put(t, BETA, beta)
        record(1, t, s, beta)
        put(t, FAC + (s + 1) % 2, get(t, SIZE) / beta)
        return beta

    def ev_scale(t, s):
        ev_beta(t, s - 1)
        fac = get(t, FAC + s % 2)
        for m in EIGHT:
            outb[t, m, half_rows(0)] = outb[t, m, half_rows(0)] * fac

    def vec_rows(t, s, first):
        size = scal[SIZE, t]
        rinv = wide(jnp.where(size > 0, 1.0 / size, 0.0), LN)
        for j in range(0, half, LN):
            vec[t, (s + 1) % 2, pl.ds(pl.multiple_of(first + j, LN), LN)] = new_w(t, s, first + j, LN) * rinv

    def ev_vec(t, s):
        for h in BOTH:
            came(eight_halves, FW + h, t)
        vec_rows(t, s, other * half)
        for h in BOTH:
            sent(eight_halves, FW + h, t)
            sent(seven_halves, GA + h, t)

    def rel(n, j):
        return FAR[j] + n * (CLOSE[j] - FAR[j])

    def r_phase(t, s, start, count, shift=0):
        xv = jnp.dot(rf[:, pl.ds(start + shift, count), :].reshape(mpo * count, bond), vec[t, s % 2], preferred_element_type=F32, precision=HI)
        for r in range(mpo):
            for ij in range(PH):
                xf[pl.ds((ij * mpo + r) * NX + shift, count), :] = xv[r * count:(r + 1) * count, ij * LN:(ij + 1) * LN]

    def w_phase(start):
        for e in range(0, EH, 2):
            xs = jnp.concatenate([xf[pl.ds(e + q, PH * mpo, stride=NX), :] for q in BOTH], axis=1)
            x0, x1, x2 = split3(xs)
            y0, y1, y2 = jnp.split(jnp.dot(wpk[...], jnp.concatenate([x0, x1, x2], axis=0), preferred_element_type=F32), 3)
            yv = (y2 + y1) + y0
            for q in BOTH:
                yf[pl.ds(start + e + q, PH * mpo, stride=NY), :] = yv[:, q * LN:(q + 1) * LN]

    def l_phase(t, h, n, fac):
        rows = [half_rows(h, (l * PH + mn) * NY) for l in range(mpo) for mn in range(PH)]
        lhs = [jnp.concatenate([yf[r, :] for r in rows[l * PH:l * PH + PH]], axis=0) for l in range(mpo)]
        y0, y1, y2 = split3(jnp.concatenate(lhs, axis=1))
        b0, b1, b2 = [l3[k, n].reshape(mpo * LN, PH * LN) for k in SHARES]
        p0 = jnp.dot(jnp.concatenate([y0, y1, y2], axis=0), b0, preferred_element_type=F32)
        p1 = jnp.dot(jnp.concatenate([y0, y1], axis=0), b1, preferred_element_type=F32)
        p2 = jnp.dot(y0, b2, preferred_element_type=F32)
        ov = ((p0[2 * LN:] + p1[LN:]) + p2) + (p0[LN:2 * LN] + p1[:LN]) + p0[:LN]
        if fac is not None:
            ov = ov * fac
        for j in range(PH):
            for mn in range(PH):
                outb[t, rel(n, j), half_rows(h), mn * LN:(mn + 1) * LN] = ov[mn * EH:(mn + 1) * EH, j * LN:(j + 1) * LN]

    def send_part(t, h, part):
        for m in part:
            rs_copy(t, h, m).start()

    quarter = EH // 2

    def step_body(it, carry):
        t, s = it % 2, it // 2
        ot = 1 - t
        os = (it + 1) // 2 - 1
        more = it < 2 * STEPS - 1
        later = it >= 2

        @pl.when(it == 1)
        def _():
            ev_init(t)

        @pl.when(later)
        def _():
            ev_vec(t, s - 1)

        r_phase(t, s, 0, quarter)

        @pl.when(later)
        def _():
            ev_pass(t)

        ev_sum(ot, os, 0, more)
        r_phase(t, s, 0, quarter, quarter)
        w_phase(0)
        l_phase(t, 0, 0, None)
        ev_sum(ot, os, 1, more)
        l_phase(t, 0, 1, None)
        r_phase(t, s, EH, quarter)
        ev_mid(ot)

        @pl.when(later)
        def _():
            ev_scale(t, s)

        send_part(t, 0, SEVEN)

        r_phase(t, s, EH, quarter, quarter)
        w_phase(EH)
        l_phase(t, 1, 0, get(t, FAC + s % 2))
        ev_alpha(ot, os)

        @pl.when(more)
        def _():
            ev_fwd(ot, 0)
            ev_fwd(ot, 1)

        send_part(t, 1, FAR[::-1])
        vec_rows(ot, os, core * half)
        l_phase(t, 1, 1, get(t, FAC + s % 2))
        send_part(t, 1, NEAR)
        return carry

    p_take(0, 2)
    l_take(0, *SIDES)
    l_pass(0, *(MAINS[1:] + DIAGS))
    ev_init(0)
    r_ld.wait()

    def first_rw(h, carry):
        start = pl.multiple_of(h * EH, EH)
        r_phase(0, 0, start, quarter)

        @pl.when(h == 1)
        def _():
            l_take(0, *(MAINS + DIAGS))

        r_phase(0, 0, start, quarter, quarter)
        w_phase(start)

        @pl.when(h == 0)
        def _():
            l_take(1, *SIDES)

        return carry

    lax.fori_loop(0, 2, first_rw, 0)
    l_first()

    def first_l(q, carry):
        n, h = q // 2, q % 2

        @pl.when(q == 2)
        def _():
            l_second()

        l_phase(0, h, n, None)
        for j in SHARES:
            rs_copy(0, h, rel(n, j)).start()

        @pl.when(n == 0)
        def _():
            rs_copy(0, h, FAR[3]).start()

        @pl.when(q == 1)
        def _():
            p_take(1, 1)

        @pl.when(q == 2)
        def _():
            p_take(1, 2)

        return carry

    lax.fori_loop(0, 4, first_l, 0)
    lax.fori_loop(1, 2 * STEPS, step_body, 0)

    last = STEPS - 1

    def finish(t):
        ev_beta(t, last)
        came(seven_fin, FI, t)
        sent(seven_fin, FI, t)
        f_copy(t, 0).wait()

    ev_pass(0)
    ev_sum(1, last, 0, False)
    ev_sum(1, last, 1, False)
    ev_mid(1)
    finish(0)
    ev_alpha(1, last)
    ev_pass(1)
    finish(1)


def output_kernel(rows_ref, sums_ref, alpha_out, beta_out, psi_out):
    alpha_out[...] = sums_ref[0]
    beta_out[...] = sums_ref[1]
    for t in BOTH:
        rinv = 1.0 / sums_ref[1, t:t + 1, STEPS - 1:STEPS]
        for i in BOTH:
            for j in BOTH:
                psi_out[t, :, i, j, :] = jnp.concatenate([rows_ref[t, g, i][:, j * EC:(j + 1) * EC] for g in EIGHT], axis=1) * rinv


def solution(mesh):
    psi_spec = P(None, "lb", None, None, "rb")

    def local_run(psi_loc, left_loc, right_loc, mpo_pair):
        rows = psi_loc.shape[1]
        mpo, bond = left_loc.shape[1:]
        left_t = jnp.transpose(left_loc, (1, 0, 2))
        right_t = jnp.transpose(right_loc, (1, 0, 2))
        mpo_t = jnp.transpose(mpo_pair, (0, 2, 3, 4, 5, 1))
        dma = pltpu.SemaphoreType.DMA
        any_spec = pl.BlockSpec(memory_space=pl.ANY)
        vm = pl.BlockSpec(memory_space=pltpu.VMEM)
        f32_shapes = [
            (mpo, EC, bond),
            (2, mpo + 1, LN, WID),
            (mpo, rows, bond),
            (2, bond, WID),
            (2, 2, bond, WID),
            (2, PH, LN, bond),
            psi_loc.shape,
            mpo_t.shape,
            (PH * mpo, LN),
            (PH * mpo * NX, LN),
            (PH * mpo * NY, LN),
            (2, 8, EC, WID),
            (2, 2, 7, EH, WID),
            (3, mpo // 4, LN, LN),
        ]
        small = [(3, 2, k, 2, LN) for k in (RB, 8, 2)] + [(SIZE + 1, 2, 8, LN), (2, 2, LN, LN)]
        call = pl.pallas_call(
            functools.partial(kernel, (bond, mpo, float(bond * bond * PH))),
            out_shape=[jax.ShapeDtypeStruct(shape, F32) for shape in ((2, len(EIGHT), 2, rows, LN), (2, 2, STEPS))],
            in_specs=[any_spec] * 4,
            out_specs=[any_spec, vm],
            scratch_shapes=[pltpu.VMEM(shape, F32) for shape in f32_shapes]
            + [pltpu.VMEM((3, 2, mpo, LN, WID), BF16), pltpu.VMEM((3 * PH * mpo, 3 * PH * mpo), BF16)]
            + [pltpu.VMEM(shape, F32) for shape in small]
            + [dma((KINDS, 2))] * 2
            + [dma((4,))],
            compiler_params=pltpu.CompilerParams(vmem_limit_bytes=63 << 20, has_side_effects=True, collective_id=0),
            name="lanczos",
        )
        last_rows, sums = call(psi_loc, left_t, right_t, mpo_t)
        shapes = [(2, STEPS), (2, STEPS), psi_loc.shape]
        put_out = pl.pallas_call(
            output_kernel,
            out_shape=[jax.ShapeDtypeStruct(shape, F32) for shape in shapes],
            in_specs=[vm] * 2,
            out_specs=[vm] * 3,
            name="outputs",
        )
        return put_out(last_rows, sums)

    return jax.shard_map(local_run, mesh=mesh, in_specs=(psi_spec, P("lb", None, None), P("rb", None, None), P()), out_specs=(P(), P(), psi_spec), check_vma=False)
```

```python
import functools

import jax
import jax.numpy as jnp
from jax import lax
from jax.experimental import pallas as pl
from jax.experimental.pallas import tpu as pltpu
from jax.sharding import PartitionSpec as P

STEPS = 4
HI = lax.Precision.HIGHEST
F32 = jnp.float32
BF16 = jnp.bfloat16
MESH = pl.DeviceIdType.MESH
BOTH, SHARES, EIGHT = range(2), range(3), range(8)
LN = 128
RB = 16
EC = 64
EH = EC // 2
PH = 4
WID = PH * LN
NX = 40
NY = 72
FAR = (3, 5, 6, 7)
CLOSE = (4, 2, 1, 0)
NEAR = CLOSE[:3]
SEVEN = FAR[::-1] + NEAR
ALPHA, BETA, NORM, FAC = range(4)
SIZE = FAC + 2
RS, GA, FW = 0, 2, 4
PS, PF, FI, AG = range(6, 10)
AR = AG + 3
LS, LF, EX = AR + 3, AR + 6, AR + 9
PR, LR = EX + 2, EX + 11
KINDS = LR + 12
SIDE, MAIN, DIAG = SHARES
THIRDS = ((0, 4), (4, 3), (7, 3))
PLANES = ((0, 2), (2, 1), (3, 1)), ((0, 1), (1, 2), (3, 1))
ORDERS = (NEAR, NEAR[1:] + NEAR[:1], NEAR[2:] + NEAR[:2])
PIECES = (SIDE,) * 3 + (MAIN,) * 3 + (DIAG,) * 2
SIDES, MAINS, DIAGS = [[u for u, ph in enumerate(PIECES) if ph == phase] for phase in SHARES]


def split3(val):
    top = val.astype(BF16)
    rest = val - top.astype(F32)
    mid = rest.astype(BF16)
    low = (rest - mid.astype(F32)).astype(BF16)
    return top, mid, low


def fold(val, op=jnp.add):
    acc = functools.reduce(op, [val[:, j:j + LN] for j in range(0, val.shape[1], LN)])
    acc = functools.reduce(op, [acc[j:j + 8] for j in range(0, val.shape[0], 8)])
    return (jnp.max if op is jnp.maximum else jnp.sum)(acc, axis=0, keepdims=True)


def tree(j):
    a, b, c = ORDERS[j]
    return ((0, a), (0, b), (0, c)), ((a, b), (a, c), (b, c)), ((a + b, c),), ()


def members(j):
    a, b, c = ORDERS[j]
    return NEAR, (a + b,), (a + c, b + c, a + b + c)


def slot(m, j, step=3):
    return step * [m in part for part in members(j)].index(True) + j


def bits(m):
    return [m // d % 2 for d in NEAR]


def number(trip, base=2):
    return (trip[0] * base + trip[1]) * base + trip[2]


def flip(trip, m):
    return number([q + b * (1 - 2 * q) for q, b in zip(trip, bits(m))])


def places(lb):
    place = (lb // RB, (lb // 4) % 4, lb % 4)
    return place, [q % 2 for q in place], [q // 2 for q in place], [(q + 1) // 2 % 2 for q in place]


def kernel(cfg, psi_ref, left_ref, right_ref, mpo_ref, rows_out, sums_out,
           rf, ls, lst, gat, vec, pg, praw, wraw, wst, xf, yf, outb, rsb, xst, l3, wpk, gbuf, rbuf, asend, scal, fsend, ssem, rsem, ldsem):
    bond, mpo, elems = cfg
    core, lb = lax.axis_index("rb"), lax.axis_index("lb")
    place, low, high, side = places(lb)
    pos, aset, eset = number(low), number(high), number(side)
    half, lhalf = bond // 2, mpo // 2
    own = core * half + eset * EC
    other = 1 - core
    myrows = pl.ds(pl.multiple_of(pos * RB, RB), RB)
    mycols = pl.ds(pl.multiple_of(core * half, half), half)

    def chip_rows(m):
        return pl.ds(pl.multiple_of(flip(low, m) * RB, RB), RB)

    def gpeer(m):
        return number([q + b * (1 - 2 * p) for q, b, p in zip(place, bits(m), low)], 4)

    def rpeer(m):
        return number([q + b * (3 - 2 * q) for q, b in zip(place, bits(m))], 4)

    def remote(src, dst, ssm, rsm, c, chip):
        return pltpu.make_async_remote_copy(src_ref=src, dst_ref=dst, send_sem=ssm, recv_sem=rsm, device_id=(c, chip), device_id_type=MESH)

    def tagged(src, dst, kind, t, c, chip):
        return remote(src, dst, ssem.at[kind, t], rsem.at[kind, t], c, chip)

    def sent(region, kind, t):
        tagged(region, region, kind, t, other, lb).wait_send()

    def came(region, kind, t):
        tagged(region, region, kind, t, other, lb).wait_recv()

    def came_at(region, arrival):
        remote(region, region, ssem.at[0, 0], arrival, other, lb).wait_recv()

    def half_rows(h, base=0):
        return pl.ds(base + h * EH if isinstance(h, int) else pl.multiple_of(base + h * EH, 8), EH)

    def rs_copy(t, h, m):
        return tagged(outb.at[t, m, half_rows(h)], rsb.at[t, h, m - 1], RS + h, t, core, rpeer(m))

    def gat_rows(m, h):
        return pl.ds(pl.multiple_of(core * half + flip(side, m) * EC + h * EH, EH), EH)

    def g_copy(t, h, m):
        reg = gat.at[t, gat_rows(0, h)]
        return tagged(reg, reg, GA + h, t, core, gpeer(m))

    def fw_copy(t):
        reg = gat.at[t, mycols]
        return tagged(reg, reg, FW, t, other, lb)

    seven_halves = gat.at[0, pl.ds(0, 7 * EH)]

    def p_region(t, m, j):
        return pg.at[t, pl.ds(*PLANES[t][j]), chip_rows(m), mycols]

    def p_copy(t, m, j, d):
        reg = p_region(t, m, j)
        return remote(reg, reg, ssem.at[PS, t], rsem.at[PR + slot(m + d, j), t], core, gpeer(d))

    def p_over(t, m, j):
        reg = p_region(t, m, j)
        return tagged(reg, reg, PF, t, other, lb)

    def p_pass(t, level, j):
        for m, d in tree(j)[level]:
            p_copy(t, m, j, d).start()

    def p_send(t):
        for j in SHARES:
            p_pass(t, 0, j)
            p_over(t, 0, j).start()

    def p_take(t, level):
        for j in SHARES:
            part = members(j)[level]
            came(pg.at[t, pl.ds(0, PLANES[t][j][1]), pl.ds(0, RB * len(part)), pl.ds(0, half)], PR + 3 * level + j, t)
            p_pass(t, level + 1, j)
            for m in part:
                p_over(t, m, j).start()

    seven_psi = pg.at[0, :, pl.ds(0, 7 * RB), pl.ds(0, half)]
    half_psi = pg.at[0, :, :, pl.ds(0, half)]

    def f_copy(t, m):
        src = fsend.at[t, :, chip_rows(m)]
        if m == 0:
            return pltpu.make_async_copy(src, rows_out.at[t, eset], ldsem.at[t])
        return tagged(src, rows_out.at[t, eset], FI, t, core, gpeer(m))

    seven_fin = rows_out.at[0, pl.ds(0, 7)]

    fifth = lhalf // 2
    pieces = [(1, core * lhalf + fifth * high[k], fifth, k * LN, LN, k) for k in SHARES]
    pieces += [(0, core * lhalf + first, count, 0, WID, k) for k, (first, count) in enumerate(THIRDS)]
    pieces += [(1, core * lhalf + fifth * k, fifth, 3 * LN, LN, 2 - k) for k in BOTH]

    def l_region(u, m):
        n, first, count, lane, lanes, _ = pieces[u]
        return ls.at[n, pl.ds(first, count), chip_rows(m), pl.ds(lane, lanes)]

    def l_arrival(u, level):
        return rsem.at[LR + (3 * u + level) // 2, (3 * u + level) % 2]

    def l_copy(u, m, d):
        reg = l_region(u, m)
        return remote(reg, reg, ssem.at[LS + PIECES[u], 0], l_arrival(u, slot(m + d, pieces[u][5], 1) - pieces[u][5]), core, gpeer(d))

    def l_pass(level, *which):
        for u in which:
            for m, d in tree(pieces[u][5])[level]:
                l_copy(u, m, d).start()

    def lf_copy(u, m):
        reg = l_region(u, m)
        return tagged(reg, reg, LF + PIECES[u], int(m in FAR), other, lb)

    def l_bytes(phase, rows):
        count, lanes = ((fifth, 3 * LN), (lhalf, WID), (lhalf, LN))[phase]
        return ls.at[0, pl.ds(0, count), pl.ds(0, rows), pl.ds(0, lanes)]

    def ex_region(k, mine):
        bit = high[k] if mine else 1 - high[k]
        return ls.at[1, pl.ds(core * lhalf + fifth * bit, fifth), :, pl.ds(k * LN, LN)]

    def ex_copy(k):
        return tagged(xst.at[k], ex_region(k, True), EX, 0, core, rpeer(NEAR[k]))

    def ex_over(k):
        return tagged(ex_region(k, False), ex_region(k, False), EX, 1, other, lb)

    group = [(c, m) for c in BOTH for m in EIGHT if c or m]

    def flip_core(c):
        return core + c * (1 - 2 * core)

    def g_send(t, kind, *rows):
        for k, row in enumerate(rows):
            asend[kind, t, 0, pl.ds(k, 1)] = row
            gbuf[kind, t, core * 8 + eset, pl.ds(k, 1)] = row
        for c, m in group:
            tagged(asend.at[kind, t, 0], gbuf.at[kind, t, core * 8 + eset], AG + kind, t, flip_core(c), gpeer(m)).start()

    def g_sum(t, kind):
        came(gbuf.at[kind, t, pl.ds(0, 15)], AG + kind, t)
        both = [gbuf[kind, t, j] for j in range(RB)]
        return sum(both)[0:1], functools.reduce(jnp.maximum, both)[1:2]

    def r_send(t, kind, row):
        asend[kind, t, 1, pl.ds(0, 1)] = row
        rbuf[kind, t, aset, pl.ds(0, 1)] = row
        for m in SEVEN:
            tagged(asend.at[kind, t, 1], rbuf.at[kind, t, aset], AR + kind, t, core, rpeer(m)).start()

    def r_sum(t, kind):
        came(rbuf.at[kind, t, pl.ds(0, 7)], AR + kind, t)
        return sum(rbuf[kind, t, j] for j in EIGHT)[0:1]

    def mean(row):
        return jnp.sum(row, axis=1, keepdims=True) / elems

    def total(t, kind):
        row = r_sum(t, kind)
        sent(gbuf.at[kind, t, pl.ds(0, 15)], AG + kind, t)
        sent(rbuf.at[kind, t, pl.ds(0, 7)], AR + kind, t)
        return mean(row)

    def put(t, kind, val):
        scal[kind, t] = jnp.broadcast_to(val, (8, LN))

    def get(t, kind):
        return scal[kind, t][0:1, 0:1]

    def wide(tile, rows):
        return jnp.concatenate([jnp.concatenate([tile] * PH, axis=1)] * (rows // 8), axis=0)

    def record(kind, t, s, val):
        rows = lax.broadcasted_iota(jnp.int32, (2, STEPS), 0)
        cols = lax.broadcasted_iota(jnp.int32, (2, STEPS), 1)
        sums_out[kind] = jnp.where(jnp.logical_and(rows == t, cols == s), val, sums_out[kind])

    psi_ld = pltpu.make_async_copy(psi_ref, praw, ldsem.at[0])
    psi_ld.start()
    l_ld = pltpu.make_async_copy(left_ref, lst, ldsem.at[1])
    l_ld.start()
    r_ld = pltpu.make_async_copy(right_ref.at[:, pl.ds(pl.multiple_of(eset * EC, EC), EC)], rf, ldsem.at[2])
    r_ld.start()
    w_ld = pltpu.make_async_copy(mpo_ref, wraw, ldsem.at[3])
    w_ld.start()
    barrier = pltpu.get_barrier_semaphore()
    for c, m in group:
        pl.semaphore_signal(barrier, inc=1, device_id=(flip_core(c), gpeer(m)), device_id_type=MESH)
    for m in SEVEN:
        pl.semaphore_signal(barrier, inc=1, device_id=(core, rpeer(m)), device_id_type=MESH)
    psi_ld.wait()
    parts = []
    for t in BOTH:
        acc = 0
        for ij in range(PH):
            val = praw[t, :, ij // 2, ij % 2, :]
            pg[t, ij, myrows, mycols] = val
            acc = acc + val * val
        parts.append(fold(acc))
    sums_out[...] = jnp.zeros(sums_out.shape, F32)
    asend[...] = jnp.zeros(asend.shape, F32)
    pl.semaphore_wait(barrier, len(group) + len(SEVEN))
    for t in BOTH:
        g_send(t, NORM, parts[t])
    p_send(0)
    l_ld.wait()

    def perm_body(l, carry):
        lane = lax.broadcasted_iota(jnp.int32, (RB, LN), 1) // 32
        for hz in BOTH:
            for hy in BOTH:
                src = [lst[l, :, pl.ds((4 * hz + 2 * q + hy) * LN, LN)] for q in BOTH]
                for hx in BOTH:
                    pick = None
                    for c in range(PH):
                        shift = (c - 2 * (c % 2) - hx) * 32 % LN
                        val = pltpu.roll(src[c // 2], shift, 1) if shift else src[c // 2]
                        pick = val if pick is None else jnp.where(lane == c, val, pick)
                    rel = [p + q * (1 - 2 * p) for p, q in zip((hz, hy, hx), high)]
                    far = sum(rel) // 2
                    rank = [p + far * (1 - 2 * p) for p in rel]
                    j = 3 - (3 * rank[0] + 2 * rank[1] + rank[2])
                    one = sum(rel) % 2 - sum(rel) // 3
                    here, there = l // fifth % 2, sum(p * q for p, q in zip(rel, high))
                    skip = one * (here + there - 2 * here * there)
                    ls[1 - far, l + skip * (mpo - l), myrows, pl.ds(pl.multiple_of(j * LN, LN), LN)] = pick
        return carry

    lax.fori_loop(0, mpo, perm_body, 0)
    p_take(0, 0)
    l_pass(0, *SIDES)
    for t in BOTH:
        r_send(t, NORM, g_sum(t, NORM)[0])
    p_take(0, 1)
    l_pass(0, *MAINS[:1])
    w_ld.wait()
    for mn in range(PH):
        planes = [wraw[:, ij // 2, ij % 2, mn // 2, mn % 2, :] for ij in range(PH)]
        wst[pl.ds(mn, mpo, stride=PH), :] = jnp.concatenate(planes + [jnp.zeros((mpo, LN - PH * mpo), F32)], axis=1)
    w0, w1, w2 = split3(wst[:, :PH * mpo])
    none = jnp.zeros_like(w0)
    groups = [jnp.concatenate(g, axis=1) for g in ([w0] * 3, [w1, w1, none], [w2, none, none])]
    wpk[...] = jnp.concatenate(groups, axis=0)

    def l_take(level, *which):
        for u in which:
            n, _, count, _, lanes, j = pieces[u]
            part = members(j)[level]
            came_at(ls.at[n, pl.ds(0, count), pl.ds(0, RB * len(part)), pl.ds(0, lanes)], l_arrival(u, level))
            l_pass(level + 1, u)
            for m in part:
                lf_copy(u, m).start()

    def split_rows(n, lane, lanes, offsets):
        cols = pl.ds(lane, lanes)

        def split_body(l, carry):
            for m in offsets:
                rows = chip_rows(m)
                for k, part in enumerate(split3(ls[n, l, rows, cols])):
                    l3[k, n, l, rows, cols] = part
            return carry

        lax.fori_loop(0, mpo, split_body, 0)

    def over(phase, part):
        came(l_bytes(phase, RB * len(part)), LF + phase, int(part is FAR))

    def ex_send():
        def turn_body(i, carry):
            for k in SHARES:
                xst[k, i] = ls[1, core * lhalf + fifth * high[k] + i, :, k * LN:(k + 1) * LN].T
            return carry

        lax.fori_loop(0, fifth, turn_body, 0)
        for k in SHARES:
            ex_copy(k).start()

    def ex_take():
        came(l_bytes(SIDE, LN), EX, 0)
        for k in SHARES:
            ex_over(k).start()

    def l_first():
        l_take(2, *SIDES)
        ex_send()
        over(MAIN, NEAR)
        split_rows(0, 0, WID, CLOSE)
        l_take(1, *(MAINS + DIAGS))
        p_send(1)
        ex_take()
        l_take(2, *MAINS)
        for part in (NEAR, FAR):
            over(SIDE, part)
        came(l_bytes(SIDE, LN), EX, 1)
        split_rows(1, 0, 3 * LN, CLOSE + FAR)
        over(MAIN, FAR)
        split_rows(0, 0, WID, FAR)
        p_take(1, 0)
        l_take(2, *DIAGS)

    def l_second():
        for part in (NEAR, FAR):
            over(DIAG, part)
        split_rows(1, 3 * LN, LN, CLOSE + FAR)
        for phase in SHARES:
            sent(l_bytes(phase, 7 * RB), LS + phase, 0)
            for k, part in enumerate((NEAR, FAR)):
                sent(l_bytes(phase, RB * len(part)), LF + phase, k)
        for k in BOTH:
            sent(l_bytes(SIDE, LN), EX, k)

    def ev_init(t):
        rinv = 1.0 / jnp.sqrt(total(t, NORM))
        put(t, BETA, jnp.zeros((1, 1), F32))
        for slot in BOTH:
            put(t, FAC + slot, jnp.ones((1, 1), F32))

        def turn(first):
            def tr_body(b, carry):
                rows = pl.ds(pl.multiple_of(first + b * LN, LN), LN)
                for ij in range(PH):
                    vec[t, 0, rows, ij * LN:(ij + 1) * LN] = pg[t, ij, :, rows].T * rinv
                vec[t, 1, rows] = jnp.zeros((LN, WID), F32)
                return carry

            lax.fori_loop(0, half // LN, tr_body, 0)

        turn(core * half)
        came(half_psi, PF, t)
        turn(other * half)
        sent(seven_psi, PS, t)
        sent(half_psi, PF, t)

    def ev_sum(t, s, h, more):
        came(rsb.at[t, h], RS + h, t)
        hv = outb[t, 0, half_rows(h)] + sum(rsb[t, h, m - 1] for m in SEVEN)
        gat[t, gat_rows(0, h)] = hv
        if h:
            rows = pl.ds(pl.multiple_of(own, EC), EC)
            hv = gat[t, rows]
            g_send(t, ALPHA, fold(hv * vec[t, s % 2, rows]) * get(t, FAC + s % 2), fold(jnp.abs(hv), jnp.maximum))

        @pl.when(more)
        def _():
            for k, m in ((0, NEAR), (1, FAR[::-1]), (1, NEAR)) if h else ((0, FAR[::-1]),):
                for q in m:
                    g_copy(t, k, q).start()

        sent(rsb.at[t, h], RS + h, t)

    def new_w(t, s, first, count):
        cur, prev = s % 2, (s + 1) % 2
        rows = pl.ds(pl.multiple_of(first, EC), count)
        along, back = wide(scal[ALPHA, t] * scal[FAC + cur, t], count), wide(scal[BETA, t] * scal[FAC + prev, t], count)
        return gat[t, rows] - along * vec[t, cur, rows] - back * vec[t, prev, rows]

    def ev_mid(t):
        row, most = g_sum(t, ALPHA)
        r_send(t, ALPHA, row)
        put(t, SIZE, jnp.max(most, axis=1, keepdims=True))

    def ev_alpha(t, s):
        alpha = total(t, ALPHA)
        put(t, ALPHA, alpha)
        put(t, SIZE, jnp.maximum(get(t, SIZE), jnp.maximum(jnp.abs(alpha), get(t, BETA))))
        record(0, t, s, alpha)
        res = new_w(t, s, own, EC)
        g_send(t, BETA, fold(res * res))

        @pl.when(s == STEPS - 1)
        def _():
            for q in BOTH:
                pair = [res[:, j * LN:(j + 1) * LN] for j in (2 * q, 2 * q + 1)]
                fsend[t, q] = jnp.concatenate(pair, axis=0).T
            for m in SEVEN + (0,):
                f_copy(t, m).start()

    def ev_pass(t):
        r_send(t, BETA, g_sum(t, BETA)[0])

    def ev_fwd(t):
        for h in BOTH:
            came(seven_halves, GA + h, t)
        fw_copy(t).start()

    def ev_beta(t, s):
        beta = jnp.sqrt(total(t, BETA))
        put(t, BETA, beta)
        record(1, t, s, beta)
        put(t, FAC + (s + 1) % 2, get(t, SIZE) / beta)
        return beta

    def ev_scale(t, s):
        ev_beta(t, s - 1)
        fac = get(t, FAC + s % 2)
        for m in EIGHT:
            outb[t, m, half_rows(0)] = outb[t, m, half_rows(0)] * fac

    def vec_rows(t, s, first):
        size = scal[SIZE, t]
        rinv = wide(jnp.where(size > 0, 1.0 / size, 0.0), LN)
        for j in range(0, half, LN):
            vec[t, (s + 1) % 2, pl.ds(pl.multiple_of(first + j, LN), LN)] = new_w(t, s, first + j, LN) * rinv

    def ev_vec(t, s):
        fw_copy(t).wait_recv()
        vec_rows(t, s, other * half)
        fw_copy(t).wait_send()
        for h in BOTH:
            sent(seven_halves, GA + h, t)

    def rel(n, j):
        return FAR[j] + n * (CLOSE[j] - FAR[j])

    def r_phase(t, s, start, count, shift=0):
        xv = jnp.dot(rf[:, pl.ds(start + shift, count), :].reshape(mpo * count, bond), vec[t, s % 2], preferred_element_type=F32, precision=HI)
        for r in range(mpo):
            for ij in range(PH):
                xf[pl.ds((ij * mpo + r) * NX + shift, count), :] = xv[r * count:(r + 1) * count, ij * LN:(ij + 1) * LN]

    def w_phase(start):
        for e in range(0, EH, 2):
            xs = jnp.concatenate([xf[pl.ds(e + q, PH * mpo, stride=NX), :] for q in BOTH], axis=1)
            x0, x1, x2 = split3(xs)
            y0, y1, y2 = jnp.split(jnp.dot(wpk[...], jnp.concatenate([x0, x1, x2], axis=0), preferred_element_type=F32), 3)
            yv = (y2 + y1) + y0
            for q in BOTH:
                yf[pl.ds(start + e + q, PH * mpo, stride=NY), :] = yv[:, q * LN:(q + 1) * LN]

    def l_phase(t, h, n, fac):
        rows = [half_rows(h, (l * PH + mn) * NY) for l in range(mpo) for mn in range(PH)]
        lhs = [jnp.concatenate([yf[r, :] for r in rows[l * PH:l * PH + PH]], axis=0) for l in range(mpo)]
        y0, y1, y2 = split3(jnp.concatenate(lhs, axis=1))
        b0, b1, b2 = [l3[k, n].reshape(mpo * LN, PH * LN) for k in SHARES]
        p0 = jnp.dot(jnp.concatenate([y0, y1, y2], axis=0), b0, preferred_element_type=F32)
        p1 = jnp.dot(jnp.concatenate([y0, y1], axis=0), b1, preferred_element_type=F32)
        p2 = jnp.dot(y0, b2, preferred_element_type=F32)
        ov = ((p0[2 * LN:] + p1[LN:]) + p2) + (p0[LN:2 * LN] + p1[:LN]) + p0[:LN]
        if fac is not None:
            ov = ov * fac
        for j in range(PH):
            for mn in range(PH):
                outb[t, rel(n, j), half_rows(h), mn * LN:(mn + 1) * LN] = ov[mn * EH:(mn + 1) * EH, j * LN:(j + 1) * LN]

    def send_part(t, h, part):
        for m in part:
            rs_copy(t, h, m).start()

    quarter = EH // 2

    def step_body(it, carry):
        t, s = it % 2, it // 2
        ot = 1 - t
        os = (it + 1) // 2 - 1
        more = it < 2 * STEPS - 1
        later = it >= 2

        @pl.when(it == 1)
        def _():
            ev_init(t)

        @pl.when(later)
        def _():
            ev_vec(t, s - 1)

        r_phase(t, s, 0, quarter)

        @pl.when(later)
        def _():
            ev_pass(t)

        ev_sum(ot, os, 0, more)
        r_phase(t, s, 0, quarter, quarter)
        w_phase(0)
        l_phase(t, 0, 0, None)
        ev_sum(ot, os, 1, more)
        l_phase(t, 0, 1, None)
        r_phase(t, s, EH, quarter)
        ev_mid(ot)

        @pl.when(later)
        def _():
            ev_scale(t, s)

        send_part(t, 0, SEVEN)

        r_phase(t, s, EH, quarter, quarter)
        w_phase(EH)
        l_phase(t, 1, 0, get(t, FAC + s % 2))
        ev_alpha(ot, os)

        @pl.when(more)
        def _():
            ev_fwd(ot)

        send_part(t, 1, FAR[::-1])
        vec_rows(ot, os, core * half)
        l_phase(t, 1, 1, get(t, FAC + s % 2))
        send_part(t, 1, NEAR)
        return carry

    p_take(0, 2)
    l_take(0, *SIDES)
    l_pass(0, *(MAINS[1:] + DIAGS))
    ev_init(0)
    r_ld.wait()

    def first_rw(h, carry):
        start = pl.multiple_of(h * EH, EH)
        r_phase(0, 0, start, quarter)

        @pl.when(h == 1)
        def _():
            l_take(0, *(MAINS + DIAGS))

        r_phase(0, 0, start, quarter, quarter)
        w_phase(start)

        @pl.when(h == 0)
        def _():
            l_take(1, *SIDES)

        return carry

    lax.fori_loop(0, 2, first_rw, 0)
    l_first()

    def first_l(q, carry):
        n, h = q // 2, q % 2

        @pl.when(q == 2)
        def _():
            l_second()

        l_phase(0, h, n, None)
        for j in SHARES:
            rs_copy(0, h, rel(n, j)).start()

        @pl.when(n == 0)
        def _():
            rs_copy(0, h, FAR[3]).start()

        @pl.when(q == 1)
        def _():
            p_take(1, 1)

        @pl.when(q == 2)
        def _():
            p_take(1, 2)

        return carry

    lax.fori_loop(0, 4, first_l, 0)
    lax.fori_loop(1, 2 * STEPS, step_body, 0)

    last = STEPS - 1

    def finish(t):
        ev_beta(t, last)
        came(seven_fin, FI, t)
        sent(seven_fin, FI, t)
        f_copy(t, 0).wait()

    ev_pass(0)
    ev_sum(1, last, 0, False)
    ev_sum(1, last, 1, False)
    ev_mid(1)
    finish(0)
    ev_alpha(1, last)
    ev_pass(1)
    finish(1)


def output_kernel(rows_ref, sums_ref, alpha_out, beta_out, psi_out):
    alpha_out[...] = sums_ref[0]
    beta_out[...] = sums_ref[1]
    for t in BOTH:
        rinv = 1.0 / sums_ref[1, t:t + 1, STEPS - 1:STEPS]
        for i in BOTH:
            for j in BOTH:
                psi_out[t, :, i, j, :] = jnp.concatenate([rows_ref[t, g, i][:, j * EC:(j + 1) * EC] for g in EIGHT], axis=1) * rinv


def solution(mesh):
    psi_spec = P(None, "lb", None, None, "rb")

    def local_run(psi_loc, left_loc, right_loc, mpo_pair):
        rows = psi_loc.shape[1]
        mpo, bond = left_loc.shape[1:]
        left_t = jnp.transpose(left_loc, (1, 0, 2))
        right_t = jnp.transpose(right_loc, (1, 0, 2))
        mpo_t = jnp.transpose(mpo_pair, (0, 2, 3, 4, 5, 1))
        dma = pltpu.SemaphoreType.DMA
        any_spec = pl.BlockSpec(memory_space=pl.ANY)
        vm = pl.BlockSpec(memory_space=pltpu.VMEM)
        f32_shapes = [
            (mpo, EC, bond),
            (2, mpo + 1, LN, WID),
            (mpo, rows, bond),
            (2, bond, WID),
            (2, 2, bond, WID),
            (2, PH, LN, bond),
            psi_loc.shape,
            mpo_t.shape,
            (PH * mpo, LN),
            (PH * mpo * NX, LN),
            (PH * mpo * NY, LN),
            (2, 8, EC, WID),
            (2, 2, 7, EH, WID),
            (3, mpo // 4, LN, LN),
        ]
        small = [(3, 2, k, 2, LN) for k in (RB, 8, 2)] + [(SIZE + 1, 2, 8, LN), (2, 2, LN, LN)]
        call = pl.pallas_call(
            functools.partial(kernel, (bond, mpo, float(bond * bond * PH))),
            out_shape=[jax.ShapeDtypeStruct(shape, F32) for shape in ((2, len(EIGHT), 2, rows, LN), (2, 2, STEPS))],
            in_specs=[any_spec] * 4,
            out_specs=[any_spec, vm],
            scratch_shapes=[pltpu.VMEM(shape, F32) for shape in f32_shapes]
            + [pltpu.VMEM((3, 2, mpo, LN, WID), BF16), pltpu.VMEM((3 * PH * mpo, 3 * PH * mpo), BF16)]
            + [pltpu.VMEM(shape, F32) for shape in small]
            + [dma((PR, 2)), dma((KINDS, 2))]
            + [dma((4,))],
            compiler_params=pltpu.CompilerParams(vmem_limit_bytes=63 << 20, has_side_effects=True, collective_id=0),
            name="lanczos",
        )
        last_rows, sums = call(psi_loc, left_t, right_t, mpo_t)
        shapes = [(2, STEPS), (2, STEPS), psi_loc.shape]
        put_out = pl.pallas_call(
            output_kernel,
            out_shape=[jax.ShapeDtypeStruct(shape, F32) for shape in shapes],
            in_specs=[vm] * 2,
            out_specs=[vm] * 3,
            name="outputs",
        )
        return put_out(last_rows, sums)

    return jax.shard_map(local_run, mesh=mesh, in_specs=(psi_spec, P("lb", None, None), P("rb", None, None), P()), out_specs=(P(), P(), psi_spec), check_vma=False)
```

```python
import functools

import jax
import jax.numpy as jnp
from jax import lax
from jax.experimental import pallas as pl
from jax.experimental.pallas import tpu as pltpu
from jax.sharding import PartitionSpec as P

STEPS = 4
HI = lax.Precision.HIGHEST
F32 = jnp.float32
BF16 = jnp.bfloat16
MESH = pl.DeviceIdType.MESH
BOTH, SHARES, EIGHT = range(2), range(3), range(8)
LN = 128
RB = 16
EC = 64
EH = EC // 2
PH = 4
WID = PH * LN
NX = 40
NY = 72
FAR = (3, 5, 6, 7)
CLOSE = (4, 2, 1, 0)
NEAR = CLOSE[:3]
SEVEN = FAR[::-1] + NEAR
ALPHA, BETA, NORM, FAC = range(4)
SIZE = FAC + 2
RS, GA, FW = 0, 2, 4
PF, FI, AG = range(FW + 1, FW + 4)
AR = AG + 3
LF, EX = AR + 3, AR + 6
PS, LS = EX + 1, EX + 2
PR, LR = PS, PS + 9
KINDS = LR + 12
SIDE, MAIN, DIAG = SHARES
THIRDS = ((0, 4), (4, 3), (7, 3))
PLANES = ((0, 2), (2, 1), (3, 1)), ((0, 1), (1, 2), (3, 1))
ORDERS = (NEAR, NEAR[1:] + NEAR[:1], NEAR[2:] + NEAR[:2])
PIECES = (SIDE,) * 3 + (MAIN,) * 3 + (DIAG,) * 2
SIDES, MAINS, DIAGS = [[u for u, ph in enumerate(PIECES) if ph == phase] for phase in SHARES]


def split3(val):
    top = val.astype(BF16)
    rest = val - top.astype(F32)
    mid = rest.astype(BF16)
    low = (rest - mid.astype(F32)).astype(BF16)
    return top, mid, low


def fold(val, op=jnp.add):
    acc = functools.reduce(op, [val[:, j:j + LN] for j in range(0, val.shape[1], LN)])
    acc = functools.reduce(op, [acc[j:j + 8] for j in range(0, val.shape[0], 8)])
    return (jnp.max if op is jnp.maximum else jnp.sum)(acc, axis=0, keepdims=True)


def tree(j):
    a, b, c = ORDERS[j]
    return ((0, a), (0, b), (0, c)), ((a, b), (a, c), (b, c)), ((a + b, c),), ()


def members(j):
    a, b, c = ORDERS[j]
    return NEAR, (a + b,), (a + c, b + c, a + b + c)


def slot(m, j, step=3):
    return step * [m in part for part in members(j)].index(True) + j


def bits(m):
    return [m // d % 2 for d in NEAR]


def number(trip, base=2):
    return (trip[0] * base + trip[1]) * base + trip[2]


def flip(trip, m):
    return number([q + b * (1 - 2 * q) for q, b in zip(trip, bits(m))])


def places(lb):
    place = (lb // RB, (lb // 4) % 4, lb % 4)
    return place, [q % 2 for q in place], [q // 2 for q in place], [(q + 1) // 2 % 2 for q in place]


def kernel(cfg, psi_ref, left_ref, right_ref, mpo_ref, rows_out, sums_out,
           rf, ls, lst, gat, vec, pg, praw, wraw, wst, xf, yf, outb, rsb, xst, l3, wpk, gbuf, rbuf, asend, scal, fsend, ssem, rsem, ldsem):
    bond, mpo, elems = cfg
    core, lb = lax.axis_index("rb"), lax.axis_index("lb")
    place, low, high, side = places(lb)
    pos, aset, eset = number(low), number(high), number(side)
    half, lhalf = bond // 2, mpo // 2
    own = core * half + eset * EC
    other = 1 - core
    myrows = pl.ds(pl.multiple_of(pos * RB, RB), RB)
    mycols = pl.ds(pl.multiple_of(core * half, half), half)

    def chip_rows(m):
        return pl.ds(pl.multiple_of(flip(low, m) * RB, RB), RB)

    def gpeer(m):
        return number([q + b * (1 - 2 * p) for q, b, p in zip(place, bits(m), low)], 4)

    def rpeer(m):
        return number([q + b * (3 - 2 * q) for q, b in zip(place, bits(m))], 4)

    def remote(src, dst, ssm, rsm, c, chip):
        return pltpu.make_async_remote_copy(src_ref=src, dst_ref=dst, send_sem=ssm, recv_sem=rsm, device_id=(c, chip), device_id_type=MESH)

    def tagged(src, dst, kind, t, c, chip):
        return remote(src, dst, ssem.at[kind, t], rsem.at[kind, t], c, chip)

    def sent(region, kind, t):
        tagged(region, region, kind, t, other, lb).wait_send()

    def came(region, kind, t):
        tagged(region, region, kind, t, other, lb).wait_recv()

    def came_at(region, arrival):
        remote(region, region, ssem.at[0, 0], arrival, other, lb).wait_recv()

    def half_rows(h, base=0):
        return pl.ds(base + h * EH if isinstance(h, int) else pl.multiple_of(base + h * EH, 8), EH)

    def rs_copy(t, h, m):
        return tagged(outb.at[t, m, half_rows(h)], rsb.at[t, h, m - 1], RS + h, t, core, rpeer(m))

    def gat_rows(m, h):
        return pl.ds(pl.multiple_of(core * half + flip(side, m) * EC + h * EH, EH), EH)

    def g_copy(t, h, m):
        reg = gat.at[t, gat_rows(0, h)]
        return tagged(reg, reg, GA + h, t, core, gpeer(m))

    def fw_copy(t):
        reg = gat.at[t, mycols]
        return tagged(reg, reg, FW, t, other, lb)

    seven_halves = gat.at[0, pl.ds(0, 7 * EH)]

    def p_region(t, m, j):
        return pg.at[t, pl.ds(*PLANES[t][j]), chip_rows(m), mycols]

    def p_copy(t, m, j, d):
        reg = p_region(t, m, j)
        return remote(reg, reg, ssem.at[PS, t], rsem.at[PR + slot(m + d, j), t], core, gpeer(d))

    def p_over(t, m, j):
        reg = p_region(t, m, j)
        return tagged(reg, reg, PF, t, other, lb)

    def p_pass(t, level, j):
        for m, d in tree(j)[level]:
            p_copy(t, m, j, d).start()

    def p_send(t):
        for j in SHARES:
            p_pass(t, 0, j)
            p_over(t, 0, j).start()

    def p_take(t, level):
        for j in SHARES:
            part = members(j)[level]
            came(pg.at[t, pl.ds(0, PLANES[t][j][1]), pl.ds(0, RB * len(part)), pl.ds(0, half)], PR + 3 * level + j, t)
            p_pass(t, level + 1, j)
            for m in part:
                p_over(t, m, j).start()

    seven_psi = pg.at[0, :, pl.ds(0, 7 * RB), pl.ds(0, half)]
    half_psi = pg.at[0, :, :, pl.ds(0, half)]

    def f_copy(t, m):
        src = fsend.at[t, :, chip_rows(m)]
        if m == 0:
            return pltpu.make_async_copy(src, rows_out.at[t, eset], ldsem.at[t])
        return tagged(src, rows_out.at[t, eset], FI, t, core, gpeer(m))

    seven_fin = rows_out.at[0, pl.ds(0, 7)]

    fifth = lhalf // 2
    pieces = [(1, core * lhalf + fifth * high[k], fifth, k * LN, LN, k) for k in SHARES]
    pieces += [(0, core * lhalf + first, count, 0, WID, k) for k, (first, count) in enumerate(THIRDS)]
    pieces += [(1, core * lhalf + fifth * k, fifth, 3 * LN, LN, 2 - k) for k in BOTH]

    def l_region(u, m):
        n, first, count, lane, lanes, _ = pieces[u]
        return ls.at[n, pl.ds(first, count), chip_rows(m), pl.ds(lane, lanes)]

    def l_arrival(u, level):
        return rsem.at[LR + (3 * u + level) // 2, (3 * u + level) % 2]

    def l_copy(u, m, d):
        reg = l_region(u, m)
        return remote(reg, reg, ssem.at[LS + PIECES[u], 0], l_arrival(u, slot(m + d, pieces[u][5], 1) - pieces[u][5]), core, gpeer(d))

    def l_pass(level, *which):
        for u in which:
            for m, d in tree(pieces[u][5])[level]:
                l_copy(u, m, d).start()

    def lf_copy(u, m):
        reg = l_region(u, m)
        return tagged(reg, reg, LF + PIECES[u], int(m in FAR), other, lb)

    def l_bytes(phase, rows):
        count, lanes = ((fifth, 3 * LN), (lhalf, WID), (lhalf, LN))[phase]
        return ls.at[0, pl.ds(0, count), pl.ds(0, rows), pl.ds(0, lanes)]

    def ex_region(k, mine):
        bit = high[k] if mine else 1 - high[k]
        return ls.at[1, pl.ds(core * lhalf + fifth * bit, fifth), :, pl.ds(k * LN, LN)]

    def ex_copy(k):
        return tagged(xst.at[k], ex_region(k, True), EX, 0, core, rpeer(NEAR[k]))

    def ex_over(k):
        return tagged(ex_region(k, False), ex_region(k, False), EX, 1, other, lb)

    others = pl.ds(0, 15)
    group = [(c, m) for c in BOTH for m in EIGHT if c or m]

    def flip_core(c):
        return core + c * (1 - 2 * core)

    def g_send(t, kind, *rows):
        for k, row in enumerate(rows):
            asend[kind, t, 0, pl.ds(k, 1)] = row
            gbuf[kind, t, core * 8 + eset, pl.ds(k, 1)] = row
        for c, m in group:
            tagged(asend.at[kind, t, 0], gbuf.at[kind, t, core * 8 + eset], AG + kind, t, flip_core(c), gpeer(m)).start()

    def g_sum(t, kind):
        came(gbuf.at[kind, t, others], AG + kind, t)
        both = [gbuf[kind, t, j] for j in range(RB)]
        return sum(both)[0:1], functools.reduce(jnp.maximum, both)[1:2]

    def r_send(t, kind, row):
        asend[kind, t, 1, pl.ds(0, 1)] = row
        rbuf[kind, t, aset, pl.ds(0, 1)] = row
        for m in SEVEN:
            tagged(asend.at[kind, t, 1], rbuf.at[kind, t, aset], AR + kind, t, core, rpeer(m)).start()

    def r_sum(t, kind):
        came(rbuf.at[kind, t, pl.ds(0, 7)], AR + kind, t)
        return sum(rbuf[kind, t, j] for j in EIGHT)[0:1]

    def mean(row):
        return jnp.sum(row, axis=1, keepdims=True) / elems

    def total(t, kind):
        row = r_sum(t, kind)
        sent(gbuf.at[kind, t, others], AG + kind, t)
        sent(rbuf.at[kind, t, pl.ds(0, 7)], AR + kind, t)
        return mean(row)

    def put(t, kind, val):
        scal[kind, t] = jnp.broadcast_to(val, (8, LN))

    def get(t, kind):
        return scal[kind, t][0:1, 0:1]

    def wide(tile, rows):
        return jnp.concatenate([jnp.concatenate([tile] * PH, axis=1)] * (rows // 8), axis=0)

    def record(kind, t, s, val):
        rows = lax.broadcasted_iota(jnp.int32, (2, STEPS), 0)
        cols = lax.broadcasted_iota(jnp.int32, (2, STEPS), 1)
        sums_out[kind] = jnp.where(jnp.logical_and(rows == t, cols == s), val, sums_out[kind])

    psi_ld = pltpu.make_async_copy(psi_ref, praw, ldsem.at[0])
    psi_ld.start()
    l_ld = pltpu.make_async_copy(left_ref, lst, ldsem.at[1])
    l_ld.start()
    r_ld = pltpu.make_async_copy(right_ref.at[:, pl.ds(pl.multiple_of(eset * EC, EC), EC)], rf, ldsem.at[2])
    r_ld.start()
    w_ld = pltpu.make_async_copy(mpo_ref, wraw, ldsem.at[3])
    w_ld.start()
    barrier = pltpu.get_barrier_semaphore()
    for c, m in group:
        pl.semaphore_signal(barrier, inc=1, device_id=(flip_core(c), gpeer(m)), device_id_type=MESH)
    for m in SEVEN:
        pl.semaphore_signal(barrier, inc=1, device_id=(core, rpeer(m)), device_id_type=MESH)
    psi_ld.wait()
    parts = []
    for t in BOTH:
        acc = 0
        for ij in range(PH):
            val = praw[t, :, ij // 2, ij % 2, :]
            pg[t, ij, myrows, mycols] = val
            acc = acc + val * val
        parts.append(fold(acc))
    sums_out[...] = jnp.zeros(sums_out.shape, F32)
    asend[...] = jnp.zeros(asend.shape, F32)
    pl.semaphore_wait(barrier, len(group) + len(SEVEN))
    for t in BOTH:
        g_send(t, NORM, parts[t])
    p_send(0)
    l_ld.wait()

    def perm_body(l, carry):
        lane = lax.broadcasted_iota(jnp.int32, (RB, LN), 1) // 32
        for hz in BOTH:
            for hy in BOTH:
                src = [lst[l, :, pl.ds((4 * hz + 2 * q + hy) * LN, LN)] for q in BOTH]
                for hx in BOTH:
                    pick = None
                    for c in range(PH):
                        shift = (c - 2 * (c % 2) - hx) * 32 % LN
                        val = pltpu.roll(src[c // 2], shift, 1) if shift else src[c // 2]
                        pick = val if pick is None else jnp.where(lane == c, val, pick)
                    rel = [p + q * (1 - 2 * p) for p, q in zip((hz, hy, hx), high)]
                    far = sum(rel) // 2
                    rank = [p + far * (1 - 2 * p) for p in rel]
                    j = 3 - (3 * rank[0] + 2 * rank[1] + rank[2])
                    one = sum(rel) % 2 - sum(rel) // 3
                    here, there = l // fifth % 2, sum(p * q for p, q in zip(rel, high))
                    skip = one * (here + there - 2 * here * there)
                    ls[1 - far, l + skip * (mpo - l), myrows, pl.ds(pl.multiple_of(j * LN, LN), LN)] = pick
        return carry

    lax.fori_loop(0, mpo, perm_body, 0)
    p_take(0, 0)
    l_pass(0, *SIDES)
    for t in BOTH:
        r_send(t, NORM, g_sum(t, NORM)[0])
    p_take(0, 1)
    l_pass(0, *MAINS[:1])
    w_ld.wait()
    for mn in range(PH):
        planes = [wraw[:, ij // 2, ij % 2, mn // 2, mn % 2, :] for ij in range(PH)]
        wst[pl.ds(mn, mpo, stride=PH), :] = jnp.concatenate(planes + [jnp.zeros((mpo, LN - PH * mpo), F32)], axis=1)
    w0, w1, w2 = split3(wst[:PH * mpo, :PH * mpo])
    none = jnp.zeros_like(w0)
    groups = [jnp.concatenate(g, axis=1) for g in ([w0] * 3, [w1, w1, none], [w2, none, none])]
    wpk[...] = jnp.concatenate(groups, axis=0)

    def l_take(level, *which):
        for u in which:
            n, _, count, _, lanes, j = pieces[u]
            part = members(j)[level]
            came_at(ls.at[n, pl.ds(0, count), pl.ds(0, RB * len(part)), pl.ds(0, lanes)], l_arrival(u, level))
            l_pass(level + 1, u)
            for m in part:
                lf_copy(u, m).start()

    def split_rows(n, lane, lanes, offsets):
        cols = pl.ds(lane, lanes)

        def split_body(l, carry):
            for m in offsets:
                rows = chip_rows(m)
                for k, part in enumerate(split3(ls[n, l, rows, cols])):
                    l3[k, n, l, rows, cols] = part
            return carry

        lax.fori_loop(0, mpo, split_body, 0)

    def over(phase, part):
        came(l_bytes(phase, RB * len(part)), LF + phase, int(part is FAR))

    def ex_send():
        def turn_body(i, carry):
            for k in SHARES:
                xst[k, i] = ls[1, core * lhalf + fifth * high[k] + i, :, k * LN:(k + 1) * LN].T
            return carry

        lax.fori_loop(0, fifth, turn_body, 0)
        for k in SHARES:
            ex_copy(k).start()

    def ex_take():
        came(l_bytes(SIDE, LN), EX, 0)
        for k in SHARES:
            ex_over(k).start()

    def l_first():
        l_take(2, *SIDES)
        ex_send()
        over(MAIN, NEAR)
        split_rows(0, 0, WID, CLOSE)
        l_take(1, *(MAINS + DIAGS))
        p_send(1)
        ex_take()
        l_take(2, *MAINS)
        for part in (NEAR, FAR):
            over(SIDE, part)
        came(l_bytes(SIDE, LN), EX, 1)
        split_rows(1, 0, 3 * LN, CLOSE + FAR)
        over(MAIN, FAR)
        split_rows(0, 0, WID, FAR)
        p_take(1, 0)
        l_take(2, *DIAGS)

    def l_second():
        for part in (NEAR, FAR):
            over(DIAG, part)
        split_rows(1, 3 * LN, LN, CLOSE + FAR)
        for phase in SHARES:
            sent(l_bytes(phase, 7 * RB), LS + phase, 0)
            for k, part in enumerate((NEAR, FAR)):
                sent(l_bytes(phase, RB * len(part)), LF + phase, k)
        for k in BOTH:
            sent(l_bytes(SIDE, LN), EX, k)

    def ev_init(t):
        rinv = 1.0 / jnp.sqrt(total(t, NORM))
        put(t, BETA, jnp.zeros((1, 1), F32))
        for slot in BOTH:
            put(t, FAC + slot, jnp.ones((1, 1), F32))

        def turn(first):
            def tr_body(b, carry):
                rows = pl.ds(pl.multiple_of(first + b * LN, LN), LN)
                for ij in range(PH):
                    vec[t, 0, rows, ij * LN:(ij + 1) * LN] = pg[t, ij, :, rows].T * rinv
                vec[t, 1, rows] = jnp.zeros((LN, WID), F32)
                return carry

            lax.fori_loop(0, half // LN, tr_body, 0)

        turn(core * half)
        came(half_psi, PF, t)
        turn(other * half)
        sent(seven_psi, PS, t)
        sent(half_psi, PF, t)

    def ev_sum(t, s, h, more):
        came(rsb.at[t, h], RS + h, t)
        hv = outb[t, 0, half_rows(h)] + sum(rsb[t, h, m - 1] for m in SEVEN)
        gat[t, gat_rows(0, h)] = hv
        if h:
            rows = pl.ds(pl.multiple_of(own, EC), EC)
            hv = gat[t, rows]
            g_send(t, ALPHA, fold(hv * vec[t, s % 2, rows]) * get(t, FAC + s % 2), fold(jnp.abs(hv), jnp.maximum))

        @pl.when(more)
        def _():
            for k, m in ((0, NEAR), (1, FAR[::-1]), (1, NEAR)) if h else ((0, FAR[::-1]),):
                for q in m:
                    g_copy(t, k, q).start()

        sent(rsb.at[t, h], RS + h, t)

    def new_w(t, s, first, count):
        cur, prev = s % 2, (s + 1) % 2
        rows = pl.ds(pl.multiple_of(first, EC), count)
        along, back = wide(scal[ALPHA, t] * scal[FAC + cur, t], count), wide(scal[BETA, t] * scal[FAC + prev, t], count)
        return gat[t, rows] - along * vec[t, cur, rows] - back * vec[t, prev, rows]

    def ev_mid(t):
        row, most = g_sum(t, ALPHA)
        r_send(t, ALPHA, row)
        put(t, SIZE, jnp.max(most, axis=1, keepdims=True))

    def ev_alpha(t, s):
        alpha = total(t, ALPHA)
        put(t, ALPHA, alpha)
        put(t, SIZE, jnp.maximum(get(t, SIZE), jnp.maximum(jnp.abs(alpha), get(t, BETA))))
        record(0, t, s, alpha)
        res = new_w(t, s, own, EC)
        g_send(t, BETA, fold(res * res))

        @pl.when(s == STEPS - 1)
        def _():
            for q in BOTH:
                pair = [res[:, j * LN:(j + 1) * LN] for j in (2 * q, 2 * q + 1)]
                fsend[t, q] = jnp.concatenate(pair, axis=0).T
            for m in SEVEN + (0,):
                f_copy(t, m).start()

    def ev_pass(t):
        r_send(t, BETA, g_sum(t, BETA)[0])

    def ev_fwd(t):
        for h in BOTH:
            came(seven_halves, GA + h, t)
        fw_copy(t).start()

    def ev_beta(t, s):
        beta = jnp.sqrt(total(t, BETA))
        put(t, BETA, beta)
        record(1, t, s, beta)
        put(t, FAC + (s + 1) % 2, get(t, SIZE) / beta)
        return beta

    def ev_scale(t, s):
        ev_beta(t, s - 1)
        fac = get(t, FAC + s % 2)
        for m in EIGHT:
            outb[t, m, half_rows(0)] = outb[t, m, half_rows(0)] * fac

    def vec_rows(t, s, first):
        size = scal[SIZE, t]
        rinv = wide(jnp.where(size > 0, 1.0 / size, 0.0), LN)
        for j in range(0, half, LN):
            vec[t, (s + 1) % 2, pl.ds(pl.multiple_of(first + j, LN), LN)] = new_w(t, s, first + j, LN) * rinv

    def ev_vec(t, s):
        fw_copy(t).wait_recv()
        vec_rows(t, s, other * half)
        fw_copy(t).wait_send()
        for h in BOTH:
            sent(seven_halves, GA + h, t)

    def rel(n, j):
        return FAR[j] + n * (CLOSE[j] - FAR[j])

    def r_phase(t, s, start, count, shift=0):
        xv = jnp.dot(rf[:, pl.ds(start + shift, count), :].reshape(mpo * count, bond), vec[t, s % 2], preferred_element_type=F32, precision=HI)
        for r in range(mpo):
            for ij in range(PH):
                xf[pl.ds((ij * mpo + r) * NX + shift, count), :] = xv[r * count:(r + 1) * count, ij * LN:(ij + 1) * LN]

    def w_phase(start):
        for e in range(0, EH, 2):
            xs = jnp.concatenate([xf[pl.ds(e + q, PH * mpo, stride=NX), :] for q in BOTH], axis=1)
            x0, x1, x2 = split3(xs)
            y0, y1, y2 = jnp.split(jnp.dot(wpk[...], jnp.concatenate([x0, x1, x2], axis=0), preferred_element_type=F32), 3)
            yv = (y2 + y1) + y0
            for q in BOTH:
                yf[pl.ds(start + e + q, PH * mpo, stride=NY), :] = yv[:, q * LN:(q + 1) * LN]

    def l_phase(t, h, n, fac):
        rows = [half_rows(h, (l * PH + mn) * NY) for l in range(mpo) for mn in range(PH)]
        lhs = [jnp.concatenate([yf[r, :] for r in rows[l * PH:l * PH + PH]], axis=0) for l in range(mpo)]
        y0, y1, y2 = split3(jnp.concatenate(lhs, axis=1))
        b0, b1, b2 = [l3[k, n].reshape(mpo * LN, PH * LN) for k in SHARES]
        p0 = jnp.dot(jnp.concatenate([y0, y1, y2], axis=0), b0, preferred_element_type=F32)
        p1 = jnp.dot(jnp.concatenate([y0, y1], axis=0), b1, preferred_element_type=F32)
        p2 = jnp.dot(y0, b2, preferred_element_type=F32)
        ov = ((p0[2 * LN:] + p1[LN:]) + p2) + (p0[LN:2 * LN] + p1[:LN]) + p0[:LN]
        if fac is not None:
            ov = ov * fac
        for j in range(PH):
            for mn in range(PH):
                outb[t, rel(n, j), half_rows(h), mn * LN:(mn + 1) * LN] = ov[mn * EH:(mn + 1) * EH, j * LN:(j + 1) * LN]

    def send_part(t, h, part):
        for m in part:
            rs_copy(t, h, m).start()

    quarter = EH // 2

    def step_body(it, carry):
        t, s = it % 2, it // 2
        ot = 1 - t
        os = (it + 1) // 2 - 1
        more = it < 2 * STEPS - 1
        later = it >= 2

        @pl.when(it == 1)
        def _():
            ev_init(t)

        @pl.when(later)
        def _():
            ev_vec(t, s - 1)

        r_phase(t, s, 0, quarter)

        @pl.when(later)
        def _():
            ev_pass(t)

        ev_sum(ot, os, 0, more)
        r_phase(t, s, 0, quarter, quarter)
        w_phase(0)
        l_phase(t, 0, 0, None)
        ev_sum(ot, os, 1, more)
        l_phase(t, 0, 1, None)
        r_phase(t, s, EH, quarter)
        ev_mid(ot)

        @pl.when(later)
        def _():
            ev_scale(t, s)

        send_part(t, 0, SEVEN)

        r_phase(t, s, EH, quarter, quarter)
        w_phase(EH)
        l_phase(t, 1, 0, get(t, FAC + s % 2))
        ev_alpha(ot, os)

        @pl.when(more)
        def _():
            ev_fwd(ot)

        send_part(t, 1, FAR[::-1])
        vec_rows(ot, os, core * half)
        l_phase(t, 1, 1, get(t, FAC + s % 2))
        send_part(t, 1, NEAR)
        return carry

    p_take(0, 2)
    l_take(0, *SIDES)
    l_pass(0, *(MAINS[1:] + DIAGS))
    ev_init(0)
    r_ld.wait()

    def first_rw(h, carry):
        start = pl.multiple_of(h * EH, EH)
        r_phase(0, 0, start, quarter)

        @pl.when(h == 1)
        def _():
            l_take(0, *(MAINS + DIAGS))

        r_phase(0, 0, start, quarter, quarter)
        w_phase(start)

        @pl.when(h == 0)
        def _():
            l_take(1, *SIDES)

        return carry

    lax.fori_loop(0, 2, first_rw, 0)
    l_first()

    def first_l(q, carry):
        n, h = q // 2, q % 2

        @pl.when(q == 2)
        def _():
            l_second()

        l_phase(0, h, n, None)
        for j in SHARES:
            rs_copy(0, h, rel(n, j)).start()

        @pl.when(n == 0)
        def _():
            rs_copy(0, h, FAR[3]).start()

        @pl.when(q == 1)
        def _():
            p_take(1, 1)

        @pl.when(q == 2)
        def _():
            p_take(1, 2)

        return carry

    lax.fori_loop(0, 4, first_l, 0)
    lax.fori_loop(1, 2 * STEPS, step_body, 0)

    last = STEPS - 1

    def finish(t):
        ev_beta(t, last)
        came(seven_fin, FI, t)
        sent(seven_fin, FI, t)
        f_copy(t, 0).wait()

    ev_pass(0)
    ev_sum(1, last, 0, False)
    ev_sum(1, last, 1, False)
    ev_mid(1)
    finish(0)
    ev_alpha(1, last)
    ev_pass(1)
    finish(1)


def output_kernel(rows_ref, sums_ref, alpha_out, beta_out, psi_out):
    alpha_out[...] = sums_ref[0]
    beta_out[...] = sums_ref[1]
    for t in BOTH:
        rinv = 1.0 / sums_ref[1, t:t + 1, STEPS - 1:STEPS]
        for i in BOTH:
            for j in BOTH:
                psi_out[t, :, i, j, :] = jnp.concatenate([rows_ref[t, g, i][:, j * EC:(j + 1) * EC] for g in EIGHT], axis=1) * rinv


def solution(mesh):
    psi_spec = P(None, "lb", None, None, "rb")

    def local_run(psi_loc, left_loc, right_loc, mpo_pair):
        rows = psi_loc.shape[1]
        mpo, bond = left_loc.shape[1:]
        left_t = jnp.transpose(left_loc, (1, 0, 2))
        right_t = jnp.transpose(right_loc, (1, 0, 2))
        mpo_t = jnp.transpose(mpo_pair, (0, 2, 3, 4, 5, 1))
        dma = pltpu.SemaphoreType.DMA
        any_spec = pl.BlockSpec(memory_space=pl.ANY)
        vm = pl.BlockSpec(memory_space=pltpu.VMEM)
        f32_shapes = [
            (mpo, EC, bond),
            (2, mpo + 1, LN, WID),
            (mpo, rows, bond),
            (2, bond, WID),
            (2, 2, bond, WID),
            (2, PH, LN, bond),
            psi_loc.shape,
            mpo_t.shape,
            (PH * mpo + EC, LN),
            (PH * mpo * NX + EC, LN),
            (PH * mpo * NY + EC, LN),
            (2, 8, EC, WID),
            (2, 2, 7, EH, WID),
            (3, mpo // 4, LN, LN),
        ]
        small = [(3, 2, k, 2, LN) for k in (RB, 8, 2)] + [(SIZE + 1, 2, 8, LN), (2, 2, LN, LN)]
        call = pl.pallas_call(
            functools.partial(kernel, (bond, mpo, float(bond * bond * PH))),
            out_shape=[jax.ShapeDtypeStruct(shape, F32) for shape in ((2, len(EIGHT), 2, rows, LN), (2, 2, STEPS))],
            in_specs=[any_spec] * 4,
            out_specs=[any_spec, vm],
            scratch_shapes=[pltpu.VMEM(shape, F32) for shape in f32_shapes]
            + [pltpu.VMEM((3, 2, mpo, LN, WID), BF16), pltpu.VMEM((3 * PH * mpo, 3 * PH * mpo), BF16)]
            + [pltpu.VMEM(shape, F32) for shape in small]
            + [dma((LS + 3, 2)), dma((KINDS, 2))]
            + [dma((4,))],
            compiler_params=pltpu.CompilerParams(vmem_limit_bytes=63 << 20, has_side_effects=True, collective_id=0),
            name="lanczos",
        )
        last_rows, sums = call(psi_loc, left_t, right_t, mpo_t)
        shapes = [(2, STEPS), (2, STEPS), psi_loc.shape]
        put_out = pl.pallas_call(
            output_kernel,
            out_shape=[jax.ShapeDtypeStruct(shape, F32) for shape in shapes],
            in_specs=[vm] * 2,
            out_specs=[vm] * 3,
            name="outputs",
        )
        return put_out(last_rows, sums)

    return jax.shard_map(local_run, mesh=mesh, in_specs=(psi_spec, P("lb", None, None), P("rb", None, None), P()), out_specs=(P(), P(), psi_spec), check_vma=False)
```

```python
import functools

import jax
import jax.numpy as jnp
from jax import lax
from jax.experimental import pallas as pl
from jax.experimental.pallas import tpu as pltpu
from jax.sharding import PartitionSpec as P

STEPS = 4
HI = lax.Precision.HIGHEST
F32 = jnp.float32
BF16 = jnp.bfloat16
MESH = pl.DeviceIdType.MESH
BOTH, SHARES, EIGHT = range(2), range(3), range(8)
LN = 128
RB = 16
EC = 64
EH = EC // 2
PH = 4
WID = PH * LN
NX = 40
NY = 72
FAR = (3, 5, 6, 7)
CLOSE = (4, 2, 1, 0)
NEAR = CLOSE[:3]
SEVEN = FAR[::-1] + NEAR
ALPHA, BETA, NORM, FAC = range(4)
SIZE = FAC + 2
RS, GA, FW = 0, 2, 4
PF, FI, AG = range(FW + 1, FW + 4)
AR = AG + 3
LF, EX = AR + 3, AR + 6
PS, LS = EX + 1, EX + 2
PR, LR = PS, PS + 9
KINDS = LR + 12
SIDE, MAIN, DIAG = SHARES
THIRDS = ((0, 4), (4, 3), (7, 3))
PLANES = ((0, 2), (2, 1), (3, 1)), ((0, 1), (1, 2), (3, 1))
ORDERS = (NEAR, NEAR[1:] + NEAR[:1], NEAR[2:] + NEAR[:2])
PIECES = (SIDE,) * 3 + (MAIN,) * 3 + (DIAG,) * 2
SIDES, MAINS, DIAGS = [[u for u, ph in enumerate(PIECES) if ph == phase] for phase in SHARES]


def split3(val):
    top = val.astype(BF16)
    rest = val - top.astype(F32)
    mid = rest.astype(BF16)
    low = (rest - mid.astype(F32)).astype(BF16)
    return top, mid, low


def fold(val, op=jnp.add):
    acc = functools.reduce(op, [val[:, j:j + LN] for j in range(0, val.shape[1], LN)])
    acc = functools.reduce(op, [acc[j:j + 8] for j in range(0, val.shape[0], 8)])
    return (jnp.max if op is jnp.maximum else jnp.sum)(acc, axis=0, keepdims=True)


def tree(j):
    a, b, c = ORDERS[j]
    return ((0, a), (0, b), (0, c)), ((a, b), (a, c), (b, c)), ((a + b, c),), ()


def members(j):
    a, b, c = ORDERS[j]
    return NEAR, (a + b,), (a + c, b + c, a + b + c)


def slot(m, j, step=3):
    return step * [m in part for part in members(j)].index(True) + j


def bits(m):
    return [m // d % 2 for d in NEAR]


def number(trip, base=2):
    return (trip[0] * base + trip[1]) * base + trip[2]


def flip(trip, m):
    return number([q + b * (1 - 2 * q) for q, b in zip(trip, bits(m))])


def places(lb):
    place = (lb // RB, (lb // 4) % 4, lb % 4)
    return place, [q % 2 for q in place], [q // 2 for q in place], [(q + 1) // 2 % 2 for q in place]


def kernel(cfg, psi_ref, left_ref, right_ref, mpo_ref, rows_out, sums_out,
           rf, ls, lst, gat, vec, pg, praw, wraw, wst, xf, yf, outb, rsb, xst, l3, wpk, gbuf, rbuf, asend, scal, fsend, ssem, rsem, ldsem):
    bond, mpo, elems = cfg
    core, lb = lax.axis_index("rb"), lax.axis_index("lb")
    place, low, high, side = places(lb)
    pos, aset, eset = number(low), number(high), number(side)
    half, lhalf = bond // 2, mpo // 2
    own = core * half + eset * EC
    other = 1 - core
    myrows = pl.ds(pl.multiple_of(pos * RB, RB), RB)
    mycols = pl.ds(pl.multiple_of(core * half, half), half)

    def chip_rows(m):
        return pl.ds(pl.multiple_of(flip(low, m) * RB, RB), RB)

    def gpeer(m):
        return number([q + b * (1 - 2 * p) for q, b, p in zip(place, bits(m), low)], 4)

    def rpeer(m):
        return number([q + b * (3 - 2 * q) for q, b in zip(place, bits(m))], 4)

    def remote(src, dst, ssm, rsm, c, chip):
        return pltpu.make_async_remote_copy(src_ref=src, dst_ref=dst, send_sem=ssm, recv_sem=rsm, device_id=(c, chip), device_id_type=MESH)

    def tagged(src, dst, kind, t, c, chip):
        return remote(src, dst, ssem.at[kind, t], rsem.at[kind, t], c, chip)

    def sent(region, kind, t):
        tagged(region, region, kind, t, other, lb).wait_send()

    def came(region, kind, t):
        tagged(region, region, kind, t, other, lb).wait_recv()

    def came_at(region, arrival):
        remote(region, region, ssem.at[0, 0], arrival, other, lb).wait_recv()

    def half_rows(h, base=0):
        return pl.ds(base + h * EH if isinstance(h, int) else pl.multiple_of(base + h * EH, 8), EH)

    def rs_copy(t, h, m):
        return tagged(outb.at[t, m, half_rows(h)], rsb.at[t, h, m - 1], RS + h, t, core, rpeer(m))

    def gat_rows(m, h):
        return pl.ds(pl.multiple_of(core * half + flip(side, m) * EC + h * EH, EH), EH)

    def g_copy(t, h, m):
        reg = gat.at[t, gat_rows(0, h)]
        return tagged(reg, reg, GA + h, t, core, gpeer(m))

    def fw_copy(t):
        reg = gat.at[t, mycols]
        return tagged(reg, reg, FW, t, other, lb)

    seven_halves = gat.at[0, pl.ds(0, 7 * EH)]

    def p_region(t, m, j):
        return pg.at[t, pl.ds(*PLANES[t][j]), chip_rows(m), mycols]

    def p_copy(t, m, j, d):
        reg = p_region(t, m, j)
        return remote(reg, reg, ssem.at[PS, t], rsem.at[PR + slot(m + d, j), t], core, gpeer(d))

    def p_over(t, m, j):
        reg = p_region(t, m, j)
        return tagged(reg, reg, PF, t, other, lb)

    def p_pass(t, level, j):
        for m, d in tree(j)[level]:
            p_copy(t, m, j, d).start()

    def p_send(t):
        for j in SHARES:
            p_pass(t, 0, j)
            p_over(t, 0, j).start()

    def p_take(t, level):
        for j in SHARES:
            part = members(j)[level]
            came(pg.at[t, pl.ds(0, PLANES[t][j][1]), pl.ds(0, RB * len(part)), pl.ds(0, half)], PR + 3 * level + j, t)
            p_pass(t, level + 1, j)
            for m in part:
                p_over(t, m, j).start()

    seven_psi = pg.at[0, :, pl.ds(0, 7 * RB), pl.ds(0, half)]
    half_psi = pg.at[0, :, :, pl.ds(0, half)]

    def f_copy(t, m):
        src = fsend.at[t, :, chip_rows(m)]
        if m == 0:
            return pltpu.make_async_copy(src, rows_out.at[t, eset], ldsem.at[t])
        return tagged(src, rows_out.at[t, eset], FI, t, core, gpeer(m))

    seven_fin = rows_out.at[0, pl.ds(0, 7)]

    fifth = lhalf // 2
    pieces = [(1, core * lhalf + fifth * high[k], fifth, k * LN, LN, k) for k in SHARES]
    pieces += [(0, core * lhalf + first, count, 0, WID, k) for k, (first, count) in enumerate(THIRDS)]
    pieces += [(1, core * lhalf + fifth * k, fifth, 3 * LN, LN, 2 - k) for k in BOTH]

    def l_region(u, m):
        n, first, count, lane, lanes, _ = pieces[u]
        return ls.at[n, pl.ds(first, count), chip_rows(m), pl.ds(lane, lanes)]

    def l_arrival(u, level):
        return rsem.at[LR + (3 * u + level) // 2, (3 * u + level) % 2]

    def l_copy(u, m, d):
        reg = l_region(u, m)
        return remote(reg, reg, ssem.at[LS + PIECES[u], 0], l_arrival(u, slot(m + d, pieces[u][5], 1) - pieces[u][5]), core, gpeer(d))

    def l_pass(level, *which):
        for u in which:
            for m, d in tree(pieces[u][5])[level]:
                l_copy(u, m, d).start()

    def lf_copy(u, m):
        reg = l_region(u, m)
        return tagged(reg, reg, LF + PIECES[u], int(m in FAR), other, lb)

    def l_bytes(phase, rows):
        count, lanes = ((fifth, 3 * LN), (lhalf, WID), (lhalf, LN))[phase]
        return ls.at[0, pl.ds(0, count), pl.ds(0, rows), pl.ds(0, lanes)]

    def ex_region(k, mine):
        bit = high[k] if mine else 1 - high[k]
        return ls.at[1, pl.ds(core * lhalf + fifth * bit, fifth), :, pl.ds(k * LN, LN)]

    def ex_copy(k):
        return tagged(xst.at[k], ex_region(k, True), EX, 0, core, rpeer(NEAR[k]))

    def ex_over(k):
        return tagged(ex_region(k, False), ex_region(k, False), EX, 1, other, lb)

    others = pl.ds(0, 15)
    group = [(c, m) for c in BOTH for m in EIGHT if c or m]

    def flip_core(c):
        return core + c * (1 - 2 * core)

    def g_send(t, kind, *rows):
        for k, row in enumerate(rows):
            asend[kind, t, 0, pl.ds(k, 1)] = row
            gbuf[kind, t, core * 8 + eset, pl.ds(k, 1)] = row
        for c, m in group:
            tagged(asend.at[kind, t, 0], gbuf.at[kind, t, core * 8 + eset], AG + kind, t, flip_core(c), gpeer(m)).start()

    def g_sum(t, kind):
        came(gbuf.at[kind, t, others], AG + kind, t)
        both = [gbuf[kind, t, j] for j in range(RB)]
        return sum(both)[0:1], functools.reduce(jnp.maximum, both)[1:2]

    def r_send(t, kind, row):
        asend[kind, t, 1, pl.ds(0, 1)] = row
        rbuf[kind, t, aset, pl.ds(0, 1)] = row
        for m in SEVEN:
            tagged(asend.at[kind, t, 1], rbuf.at[kind, t, aset], AR + kind, t, core, rpeer(m)).start()

    def r_sum(t, kind):
        came(rbuf.at[kind, t, pl.ds(0, 7)], AR + kind, t)
        return sum(rbuf[kind, t, j] for j in EIGHT)[0:1]

    def mean(row):
        return jnp.sum(row, axis=1, keepdims=True) / elems

    def total(t, kind):
        row = r_sum(t, kind)
        sent(gbuf.at[kind, t, others], AG + kind, t)
        sent(rbuf.at[kind, t, pl.ds(0, 7)], AR + kind, t)
        return mean(row)

    def put(t, kind, val):
        scal[kind, t] = jnp.broadcast_to(val, (8, LN))

    def get(t, kind):
        return scal[kind, t][0:1, 0:1]

    def wide(tile, rows):
        return jnp.concatenate([jnp.concatenate([tile] * PH, axis=1)] * (rows // 8), axis=0)

    def record(kind, t, s, val):
        rows = lax.broadcasted_iota(jnp.int32, (2, STEPS), 0)
        cols = lax.broadcasted_iota(jnp.int32, (2, STEPS), 1)
        sums_out[kind] = jnp.where(jnp.logical_and(rows == t, cols == s), val, sums_out[kind])

    psi_ld = pltpu.make_async_copy(psi_ref, praw, ldsem.at[0])
    psi_ld.start()
    l_ld = pltpu.make_async_copy(left_ref, lst, ldsem.at[1])
    l_ld.start()
    r_ld = pltpu.make_async_copy(right_ref.at[:, pl.ds(pl.multiple_of(eset * EC, EC), EC)], rf, ldsem.at[2])
    r_ld.start()
    w_ld = pltpu.make_async_copy(mpo_ref, wraw, ldsem.at[3])
    w_ld.start()
    barrier = pltpu.get_barrier_semaphore()
    for c, m in group:
        pl.semaphore_signal(barrier, inc=1, device_id=(flip_core(c), gpeer(m)), device_id_type=MESH)
    for m in SEVEN:
        pl.semaphore_signal(barrier, inc=1, device_id=(core, rpeer(m)), device_id_type=MESH)
    psi_ld.wait()
    parts = []
    for t in BOTH:
        acc = 0
        for ij in range(PH):
            val = praw[t, :, ij // 2, ij % 2, :]
            pg[t, ij, myrows, mycols] = val
            acc = acc + val * val
        parts.append(fold(acc))
    sums_out[...] = jnp.zeros(sums_out.shape, F32)
    asend[...] = jnp.zeros(asend.shape, F32)
    pl.semaphore_wait(barrier, len(group) + len(SEVEN))
    for t in BOTH:
        g_send(t, NORM, parts[t])
    p_send(0)
    l_ld.wait()

    def perm_body(l, carry):
        lane = lax.broadcasted_iota(jnp.int32, (RB, LN), 1) // 32
        for hz in BOTH:
            for hy in BOTH:
                src = [lst[l, :, pl.ds((4 * hz + 2 * q + hy) * LN, LN)] for q in BOTH]
                for hx in BOTH:
                    pick = None
                    for c in range(PH):
                        shift = (c - 2 * (c % 2) - hx) * 32 % LN
                        val = pltpu.roll(src[c // 2], shift, 1) if shift else src[c // 2]
                        pick = val if pick is None else jnp.where(lane == c, val, pick)
                    rel = [p + q * (1 - 2 * p) for p, q in zip((hz, hy, hx), high)]
                    far = sum(rel) // 2
                    rank = [p + far * (1 - 2 * p) for p in rel]
                    j = 3 - (3 * rank[0] + 2 * rank[1] + rank[2])
                    one = sum(rel) % 2 - sum(rel) // 3
                    here, there = l // fifth % 2, sum(p * q for p, q in zip(rel, high))
                    skip = one * (here + there - 2 * here * there)
                    ls[1 - far, l + skip * (mpo - l), myrows, pl.ds(pl.multiple_of(j * LN, LN), LN)] = pick
        return carry

    lax.fori_loop(0, mpo, perm_body, 0)
    p_take(0, 0)
    l_pass(0, *SIDES)
    for t in BOTH:
        r_send(t, NORM, g_sum(t, NORM)[0])
    p_take(0, 1)
    l_pass(0, *MAINS[:1])
    w_ld.wait()
    for mn in range(PH):
        planes = [wraw[:, ij // 2, ij % 2, mn // 2, mn % 2, :] for ij in range(PH)]
        wst[pl.ds(mn, mpo, stride=PH), :] = jnp.concatenate(planes + [jnp.zeros((mpo, LN - PH * mpo), F32)], axis=1)
    w0, w1, w2 = split3(wst[:PH * mpo, :PH * mpo])
    none = jnp.zeros_like(w0)
    groups = [jnp.concatenate(g, axis=1) for g in ([w0] * 3, [w1, w1, none], [w2, none, none])]
    wpk[...] = jnp.concatenate(groups, axis=0)

    def l_take(level, *which):
        for u in which:
            n, _, count, _, lanes, j = pieces[u]
            part = members(j)[level]
            came_at(ls.at[n, pl.ds(0, count), pl.ds(0, RB * len(part)), pl.ds(0, lanes)], l_arrival(u, level))
            l_pass(level + 1, u)
            for m in part:
                lf_copy(u, m).start()

    def split_rows(n, lane, lanes, offsets):
        cols = pl.ds(lane, lanes)

        def split_body(l, carry):
            for m in offsets:
                rows = chip_rows(m)
                for k, part in enumerate(split3(ls[n, l, rows, cols])):
                    l3[k, n, l, rows, cols] = part
            return carry

        lax.fori_loop(0, mpo, split_body, 0, unroll=4)

    def over(phase, part):
        came(l_bytes(phase, RB * len(part)), LF + phase, int(part is FAR))

    def ex_send():
        def turn_body(i, carry):
            for k in SHARES:
                xst[k, i] = ls[1, core * lhalf + fifth * high[k] + i, :, k * LN:(k + 1) * LN].T
            return carry

        lax.fori_loop(0, fifth, turn_body, 0)
        for k in SHARES:
            ex_copy(k).start()

    def ex_take():
        came(l_bytes(SIDE, LN), EX, 0)
        for k in SHARES:
            ex_over(k).start()

    def l_first():
        l_take(2, *SIDES)
        ex_send()
        over(MAIN, NEAR)
        split_rows(0, 0, WID, CLOSE)
        l_take(1, *(MAINS + DIAGS))
        p_send(1)
        ex_take()
        l_take(2, *MAINS)
        for part in (NEAR, FAR):
            over(SIDE, part)
        came(l_bytes(SIDE, LN), EX, 1)
        split_rows(1, 0, 3 * LN, CLOSE + FAR)
        over(MAIN, FAR)
        split_rows(0, 0, WID, FAR)
        p_take(1, 0)
        l_take(2, *DIAGS)

    def l_second():
        for part in (NEAR, FAR):
            over(DIAG, part)
        split_rows(1, 3 * LN, LN, CLOSE + FAR)
        for phase in SHARES:
            sent(l_bytes(phase, 7 * RB), LS + phase, 0)
            for k, part in enumerate((NEAR, FAR)):
                sent(l_bytes(phase, RB * len(part)), LF + phase, k)
        for k in BOTH:
            sent(l_bytes(SIDE, LN), EX, k)

    def ev_init(t):
        rinv = 1.0 / jnp.sqrt(total(t, NORM))
        put(t, BETA, jnp.zeros((1, 1), F32))
        for slot in BOTH:
            put(t, FAC + slot, jnp.ones((1, 1), F32))

        def turn(first):
            def tr_body(b, carry):
                rows = pl.ds(pl.multiple_of(first + b * LN, LN), LN)
                for ij in range(PH):
                    vec[t, 0, rows, ij * LN:(ij + 1) * LN] = pg[t, ij, :, rows].T * rinv
                vec[t, 1, rows] = jnp.zeros((LN, WID), F32)
                return carry

            lax.fori_loop(0, half // LN, tr_body, 0)

        turn(core * half)
        came(half_psi, PF, t)
        turn(other * half)
        sent(seven_psi, PS, t)
        sent(half_psi, PF, t)

    def ev_sum(t, s, h, more):
        came(rsb.at[t, h], RS + h, t)
        hv = outb[t, 0, half_rows(h)] + sum(rsb[t, h, m - 1] for m in SEVEN)
        gat[t, gat_rows(0, h)] = hv
        if h:
            rows = pl.ds(pl.multiple_of(own, EC), EC)
            hv = gat[t, rows]
            g_send(t, ALPHA, fold(hv * vec[t, s % 2, rows]) * get(t, FAC + s % 2), fold(jnp.abs(hv), jnp.maximum))

        @pl.when(more)
        def _():
            for k, m in ((0, NEAR), (1, FAR[::-1]), (1, NEAR)) if h else ((0, FAR[::-1]),):
                for q in m:
                    g_copy(t, k, q).start()

        sent(rsb.at[t, h], RS + h, t)

    def new_w(t, s, first, count):
        cur, prev = s % 2, (s + 1) % 2
        rows = pl.ds(pl.multiple_of(first, EC), count)
        along, back = wide(scal[ALPHA, t] * scal[FAC + cur, t], count), wide(scal[BETA, t] * scal[FAC + prev, t], count)
        return gat[t, rows] - along * vec[t, cur, rows] - back * vec[t, prev, rows]

    def ev_mid(t):
        row, most = g_sum(t, ALPHA)
        r_send(t, ALPHA, row)
        put(t, SIZE, jnp.max(most, axis=1, keepdims=True))

    def ev_alpha(t, s):
        alpha = total(t, ALPHA)
        put(t, ALPHA, alpha)
        put(t, SIZE, jnp.maximum(get(t, SIZE), jnp.maximum(jnp.abs(alpha), get(t, BETA))))
        record(0, t, s, alpha)
        res = new_w(t, s, own, EC)
        g_send(t, BETA, fold(res * res))

        @pl.when(s == STEPS - 1)
        def _():
            for q in BOTH:
                pair = [res[:, j * LN:(j + 1) * LN] for j in (2 * q, 2 * q + 1)]
                fsend[t, q] = jnp.concatenate(pair, axis=0).T
            for m in SEVEN + (0,):
                f_copy(t, m).start()

    def ev_pass(t):
        r_send(t, BETA, g_sum(t, BETA)[0])

    def ev_fwd(t):
        for h in BOTH:
            came(seven_halves, GA + h, t)
        fw_copy(t).start()

    def ev_beta(t, s):
        beta = jnp.sqrt(total(t, BETA))
        put(t, BETA, beta)
        record(1, t, s, beta)
        put(t, FAC + (s + 1) % 2, get(t, SIZE) / beta)
        return beta

    def ev_scale(t, s):
        ev_beta(t, s - 1)
        fac = get(t, FAC + s % 2)
        for m in EIGHT:
            outb[t, m, half_rows(0)] = outb[t, m, half_rows(0)] * fac

    def vec_rows(t, s, first):
        size = scal[SIZE, t]
        rinv = wide(jnp.where(size > 0, 1.0 / size, 0.0), LN)
        for j in range(0, half, LN):
            vec[t, (s + 1) % 2, pl.ds(pl.multiple_of(first + j, LN), LN)] = new_w(t, s, first + j, LN) * rinv

    def ev_vec(t, s):
        fw_copy(t).wait_recv()
        vec_rows(t, s, other * half)
        fw_copy(t).wait_send()
        for h in BOTH:
            sent(seven_halves, GA + h, t)

    def rel(n, j):
        return FAR[j] + n * (CLOSE[j] - FAR[j])

    def r_phase(t, s, start, count, shift=0):
        xv = jnp.dot(rf[:, pl.ds(start + shift, count), :].reshape(mpo * count, bond), vec[t, s % 2], preferred_element_type=F32, precision=HI)
        for r in range(mpo):
            for ij in range(PH):
                xf[pl.ds((ij * mpo + r) * NX + shift, count), :] = xv[r * count:(r + 1) * count, ij * LN:(ij + 1) * LN]

    def w_phase(start):
        for e in range(0, EH, 2):
            xs = jnp.concatenate([xf[pl.ds(e + q, PH * mpo, stride=NX), :] for q in BOTH], axis=1)
            x0, x1, x2 = split3(xs)
            y0, y1, y2 = jnp.split(jnp.dot(wpk[...], jnp.concatenate([x0, x1, x2], axis=0), preferred_element_type=F32), 3)
            yv = (y2 + y1) + y0
            for q in BOTH:
                yf[pl.ds(start + e + q, PH * mpo, stride=NY), :] = yv[:, q * LN:(q + 1) * LN]

    def l_phase(t, h, n, fac):
        rows = [half_rows(h, (l * PH + mn) * NY) for l in range(mpo) for mn in range(PH)]
        lhs = [jnp.concatenate([yf[r, :] for r in rows[l * PH:l * PH + PH]], axis=0) for l in range(mpo)]
        y0, y1, y2 = split3(jnp.concatenate(lhs, axis=1))
        b0, b1, b2 = [l3[k, n].reshape(mpo * LN, PH * LN) for k in SHARES]
        p0 = jnp.dot(jnp.concatenate([y0, y1, y2], axis=0), b0, preferred_element_type=F32)
        p1 = jnp.dot(jnp.concatenate([y0, y1], axis=0), b1, preferred_element_type=F32)
        p2 = jnp.dot(y0, b2, preferred_element_type=F32)
        ov = ((p0[2 * LN:] + p1[LN:]) + p2) + (p0[LN:2 * LN] + p1[:LN]) + p0[:LN]
        if fac is not None:
            ov = ov * fac
        for j in range(PH):
            for mn in range(PH):
                outb[t, rel(n, j), half_rows(h), mn * LN:(mn + 1) * LN] = ov[mn * EH:(mn + 1) * EH, j * LN:(j + 1) * LN]

    def send_part(t, h, part):
        for m in part:
            rs_copy(t, h, m).start()

    quarter = EH // 2

    def step_body(it, carry):
        t, s = it % 2, it // 2
        ot = 1 - t
        os = (it + 1) // 2 - 1
        more = it < 2 * STEPS - 1
        later = it >= 2

        @pl.when(it == 1)
        def _():
            ev_init(t)

        @pl.when(later)
        def _():
            ev_vec(t, s - 1)

        r_phase(t, s, 0, quarter)

        @pl.when(later)
        def _():
            ev_pass(t)

        ev_sum(ot, os, 0, more)
        r_phase(t, s, 0, quarter, quarter)
        w_phase(0)
        l_phase(t, 0, 0, None)
        ev_sum(ot, os, 1, more)
        l_phase(t, 0, 1, None)
        r_phase(t, s, EH, quarter)
        ev_mid(ot)

        @pl.when(later)
        def _():
            ev_scale(t, s)

        send_part(t, 0, SEVEN)

        r_phase(t, s, EH, quarter, quarter)
        w_phase(EH)
        l_phase(t, 1, 0, get(t, FAC + s % 2))
        ev_alpha(ot, os)

        @pl.when(more)
        def _():
            ev_fwd(ot)

        send_part(t, 1, FAR[::-1])
        vec_rows(ot, os, core * half)
        l_phase(t, 1, 1, get(t, FAC + s % 2))
        send_part(t, 1, NEAR)
        return carry

    p_take(0, 2)
    l_take(0, *SIDES)
    l_pass(0, *(MAINS[1:] + DIAGS))
    ev_init(0)
    r_ld.wait()

    def first_rw(h, carry):
        start = pl.multiple_of(h * EH, EH)
        r_phase(0, 0, start, quarter)

        @pl.when(h == 1)
        def _():
            l_take(0, *(MAINS + DIAGS))

        r_phase(0, 0, start, quarter, quarter)
        w_phase(start)

        @pl.when(h == 0)
        def _():
            l_take(1, *SIDES)

        return carry

    lax.fori_loop(0, 2, first_rw, 0)
    l_first()

    def first_l(q, carry):
        n, h = q // 2, q % 2

        @pl.when(q == 2)
        def _():
            l_second()

        l_phase(0, h, n, None)
        for j in SHARES:
            rs_copy(0, h, rel(n, j)).start()

        @pl.when(n == 0)
        def _():
            rs_copy(0, h, FAR[3]).start()

        @pl.when(q == 1)
        def _():
            p_take(1, 1)

        @pl.when(q == 2)
        def _():
            p_take(1, 2)

        return carry

    lax.fori_loop(0, 4, first_l, 0)
    lax.fori_loop(1, 2 * STEPS, step_body, 0)

    last = STEPS - 1

    def finish(t):
        ev_beta(t, last)
        came(seven_fin, FI, t)
        sent(seven_fin, FI, t)
        f_copy(t, 0).wait()

    ev_pass(0)
    ev_sum(1, last, 0, False)
    ev_sum(1, last, 1, False)
    ev_mid(1)
    finish(0)
    ev_alpha(1, last)
    ev_pass(1)
    finish(1)


def output_kernel(rows_ref, sums_ref, alpha_out, beta_out, psi_out):
    alpha_out[...] = sums_ref[0]
    beta_out[...] = sums_ref[1]
    for t in BOTH:
        rinv = 1.0 / sums_ref[1, t:t + 1, STEPS - 1:STEPS]
        for i in BOTH:
            for j in BOTH:
                psi_out[t, :, i, j, :] = jnp.concatenate([rows_ref[t, g, i][:, j * EC:(j + 1) * EC] for g in EIGHT], axis=1) * rinv


def solution(mesh):
    psi_spec = P(None, "lb", None, None, "rb")

    def local_run(psi_loc, left_loc, right_loc, mpo_pair):
        rows = psi_loc.shape[1]
        mpo, bond = left_loc.shape[1:]
        left_t = jnp.transpose(left_loc, (1, 0, 2))
        right_t = jnp.transpose(right_loc, (1, 0, 2))
        mpo_t = jnp.transpose(mpo_pair, (0, 2, 3, 4, 5, 1))
        dma = pltpu.SemaphoreType.DMA
        any_spec = pl.BlockSpec(memory_space=pl.ANY)
        vm = pl.BlockSpec(memory_space=pltpu.VMEM)
        f32_shapes = [
            (mpo, EC, bond),
            (2, mpo + 1, LN, WID),
            (mpo, rows, bond),
            (2, bond, WID),
            (2, 2, bond, WID),
            (2, PH, LN, bond),
            psi_loc.shape,
            mpo_t.shape,
            (PH * mpo + EC, LN),
            (PH * mpo * NX + EC, LN),
            (PH * mpo * NY + EC, LN),
            (2, 8, EC, WID),
            (2, 2, 7, EH, WID),
            (3, mpo // 4, LN, LN),
        ]
        small = [(3, 2, k, 2, LN) for k in (RB, 8, 2)] + [(SIZE + 1, 2, 8, LN), (2, 2, LN, LN)]
        call = pl.pallas_call(
            functools.partial(kernel, (bond, mpo, float(bond * bond * PH))),
            out_shape=[jax.ShapeDtypeStruct(shape, F32) for shape in ((2, len(EIGHT), 2, rows, LN), (2, 2, STEPS))],
            in_specs=[any_spec] * 4,
            out_specs=[any_spec, vm],
            scratch_shapes=[pltpu.VMEM(shape, F32) for shape in f32_shapes]
            + [pltpu.VMEM((3, 2, mpo, LN, WID), BF16), pltpu.VMEM((3 * PH * mpo, 3 * PH * mpo), BF16)]
            + [pltpu.VMEM(shape, F32) for shape in small]
            + [dma((LS + 3, 2)), dma((KINDS, 2))]
            + [dma((4,))],
            compiler_params=pltpu.CompilerParams(vmem_limit_bytes=63 << 20, has_side_effects=True, collective_id=0),
            name="lanczos",
        )
        last_rows, sums = call(psi_loc, left_t, right_t, mpo_t)
        shapes = [(2, STEPS), (2, STEPS), psi_loc.shape]
        put_out = pl.pallas_call(
            output_kernel,
            out_shape=[jax.ShapeDtypeStruct(shape, F32) for shape in shapes],
            in_specs=[vm] * 2,
            out_specs=[vm] * 3,
            name="outputs",
        )
        return put_out(last_rows, sums)

    return jax.shard_map(local_run, mesh=mesh, in_specs=(psi_spec, P("lb", None, None), P("rb", None, None), P()), out_specs=(P(), P(), psi_spec), check_vma=False)
```

```python
import functools

import jax
import jax.numpy as jnp
from jax import lax
from jax.experimental import pallas as pl
from jax.experimental.pallas import tpu as pltpu
from jax.sharding import PartitionSpec as P

STEPS = 4
HI = lax.Precision.HIGHEST
F32 = jnp.float32
BF16 = jnp.bfloat16
MESH = pl.DeviceIdType.MESH
BOTH, SHARES, EIGHT = range(2), range(3), range(8)
LN = 128
RB = 16
EC = 64
EH = EC // 2
PH = 4
WID = PH * LN
NX = 40
NY = 72
FAR = (3, 5, 6, 7)
CLOSE = (4, 2, 1, 0)
NEAR = CLOSE[:3]
SEVEN = FAR[::-1] + NEAR
ALPHA, BETA, NORM, FAC = range(4)
SIZE = FAC + 2
RS, GA, FW = 0, 2, 4
PF, FI, AG = range(FW + 1, FW + 4)
AR = AG + 3
LF, EX = AR + 3, AR + 6
PS, LS = EX + 1, EX + 2
PR, LR = PS, PS + 9
KINDS = LR + 12
SIDE, MAIN, DIAG = SHARES
THIRDS = ((0, 4), (4, 3), (7, 3))
PLANES = ((0, 2), (2, 1), (3, 1)), ((0, 1), (1, 2), (3, 1))
ORDERS = (NEAR, NEAR[1:] + NEAR[:1], NEAR[2:] + NEAR[:2])
PIECES = (SIDE,) * 3 + (MAIN,) * 3 + (DIAG,) * 2
SIDES, MAINS, DIAGS = [[u for u, ph in enumerate(PIECES) if ph == phase] for phase in SHARES]


def split3(val):
    top = val.astype(BF16)
    rest = val - top.astype(F32)
    mid = rest.astype(BF16)
    low = (rest - mid.astype(F32)).astype(BF16)
    return top, mid, low


def fold(val, op=jnp.add):
    acc = functools.reduce(op, [val[:, j:j + LN] for j in range(0, val.shape[1], LN)])
    acc = functools.reduce(op, [acc[j:j + 8] for j in range(0, val.shape[0], 8)])
    return (jnp.max if op is jnp.maximum else jnp.sum)(acc, axis=0, keepdims=True)


def tree(j):
    a, b, c = ORDERS[j]
    return ((0, a), (0, b), (0, c)), ((a, b), (a, c), (b, c)), ((a + b, c),), ()


def members(j):
    a, b, c = ORDERS[j]
    return NEAR, (a + b,), (a + c, b + c, a + b + c)


def slot(m, j, step=3):
    return step * [m in part for part in members(j)].index(True) + j


def bits(m):
    return [m // d % 2 for d in NEAR]


def number(trip, base=2):
    return (trip[0] * base + trip[1]) * base + trip[2]


def flip(trip, m):
    return number([q + b * (1 - 2 * q) for q, b in zip(trip, bits(m))])


def places(lb):
    place = (lb // RB, (lb // 4) % 4, lb % 4)
    return place, [q % 2 for q in place], [q // 2 for q in place], [(q + 1) // 2 % 2 for q in place]


def kernel(cfg, psi_ref, left_ref, right_ref, mpo_ref, rows_out, sums_out,
           rf, ls, lst, gat, vec, pg, praw, wraw, wst, xf, yf, outb, rsb, xst, l3, wpk, gbuf, rbuf, asend, scal, fsend, ssem, rsem, ldsem):
    bond, mpo, elems = cfg
    core, lb = lax.axis_index("rb"), lax.axis_index("lb")
    place, low, high, side = places(lb)
    pos, aset, eset = number(low), number(high), number(side)
    half, lhalf = bond // 2, mpo // 2
    own = core * half + eset * EC
    other = 1 - core
    myrows = pl.ds(pl.multiple_of(pos * RB, RB), RB)
    mycols = pl.ds(pl.multiple_of(core * half, half), half)

    def chip_rows(m):
        return pl.ds(pl.multiple_of(flip(low, m) * RB, RB), RB)

    def gpeer(m):
        return number([q + b * (1 - 2 * p) for q, b, p in zip(place, bits(m), low)], 4)

    def rpeer(m):
        return number([q + b * (3 - 2 * q) for q, b in zip(place, bits(m))], 4)

    def remote(src, dst, ssm, rsm, c, chip):
        return pltpu.make_async_remote_copy(src_ref=src, dst_ref=dst, send_sem=ssm, recv_sem=rsm, device_id=(c, chip), device_id_type=MESH)

    def tagged(src, dst, kind, t, c, chip):
        return remote(src, dst, ssem.at[kind, t], rsem.at[kind, t], c, chip)

    def sent(region, kind, t):
        tagged(region, region, kind, t, other, lb).wait_send()

    def came(region, kind, t):
        tagged(region, region, kind, t, other, lb).wait_recv()

    def came_at(region, arrival):
        remote(region, region, ssem.at[0, 0], arrival, other, lb).wait_recv()

    def half_rows(h, base=0):
        return pl.ds(base + h * EH if isinstance(h, int) else pl.multiple_of(base + h * EH, 8), EH)

    def rs_copy(t, h, m):
        return tagged(outb.at[t, m, half_rows(h)], rsb.at[t, h, m - 1], RS + h, t, core, rpeer(m))

    def gat_rows(m, h):
        return pl.ds(pl.multiple_of(core * half + flip(side, m) * EC + h * EH, EH), EH)

    def g_copy(t, h, m):
        reg = gat.at[t, gat_rows(0, h)]
        return tagged(reg, reg, GA + h, t, core, gpeer(m))

    def fw_copy(t):
        reg = gat.at[t, mycols]
        return tagged(reg, reg, FW, t, other, lb)

    seven_halves = gat.at[0, pl.ds(0, 7 * EH)]

    def p_region(t, m, j):
        return pg.at[t, pl.ds(*PLANES[t][j]), chip_rows(m), mycols]

    def p_copy(t, m, j, d):
        reg = p_region(t, m, j)
        return remote(reg, reg, ssem.at[PS, t], rsem.at[PR + slot(m + d, j), t], core, gpeer(d))

    def p_over(t, m, j):
        reg = p_region(t, m, j)
        return tagged(reg, reg, PF, t, other, lb)

    def p_pass(t, level, j):
        for m, d in tree(j)[level]:
            p_copy(t, m, j, d).start()

    def p_send(t):
        for j in SHARES:
            p_pass(t, 0, j)
            p_over(t, 0, j).start()

    def p_take(t, level):
        for j in SHARES:
            part = members(j)[level]
            came(pg.at[t, pl.ds(0, PLANES[t][j][1]), pl.ds(0, RB * len(part)), pl.ds(0, half)], PR + 3 * level + j, t)
            p_pass(t, level + 1, j)
            for m in part:
                p_over(t, m, j).start()

    seven_psi = pg.at[0, :, pl.ds(0, 7 * RB), pl.ds(0, half)]
    half_psi = pg.at[0, :, :, pl.ds(0, half)]

    def f_copy(t, m):
        src = fsend.at[t, :, chip_rows(m)]
        if m == 0:
            return pltpu.make_async_copy(src, rows_out.at[t, eset], ldsem.at[t])
        return tagged(src, rows_out.at[t, eset], FI, t, core, gpeer(m))

    seven_fin = rows_out.at[0, pl.ds(0, 7)]

    fifth = lhalf // 2
    pieces = [(1, core * lhalf + fifth * high[k], fifth, k * LN, LN, k) for k in SHARES]
    pieces += [(0, core * lhalf + first, count, 0, WID, k) for k, (first, count) in enumerate(THIRDS)]
    pieces += [(1, core * lhalf + fifth * k, fifth, 3 * LN, LN, 2 - k) for k in BOTH]

    def l_region(u, m):
        n, first, count, lane, lanes, _ = pieces[u]
        return ls.at[n, pl.ds(first, count), chip_rows(m), pl.ds(lane, lanes)]

    def l_arrival(u, level):
        return rsem.at[LR + (3 * u + level) // 2, (3 * u + level) % 2]

    def l_copy(u, m, d):
        reg = l_region(u, m)
        return remote(reg, reg, ssem.at[LS + PIECES[u], 0], l_arrival(u, slot(m + d, pieces[u][5], 1) - pieces[u][5]), core, gpeer(d))

    def l_pass(level, *which):
        for u in which:
            for m, d in tree(pieces[u][5])[level]:
                l_copy(u, m, d).start()

    def lf_copy(u, m):
        reg = l_region(u, m)
        return tagged(reg, reg, LF + PIECES[u], int(m in FAR), other, lb)

    def l_bytes(phase, rows):
        count, lanes = ((fifth, 3 * LN), (lhalf, WID), (lhalf, LN))[phase]
        return ls.at[0, pl.ds(0, count), pl.ds(0, rows), pl.ds(0, lanes)]

    def ex_region(k, mine):
        bit = high[k] if mine else 1 - high[k]
        return ls.at[1, pl.ds(core * lhalf + fifth * bit, fifth), :, pl.ds(k * LN, LN)]

    def ex_copy(k):
        return tagged(xst.at[k], ex_region(k, True), EX, 0, core, rpeer(NEAR[k]))

    def ex_over(k):
        return tagged(ex_region(k, False), ex_region(k, False), EX, 1, other, lb)

    others = pl.ds(0, 15)
    group = [(c, m) for c in BOTH for m in EIGHT if c or m]

    def flip_core(c):
        return core + c * (1 - 2 * core)

    def g_send(t, kind, *rows):
        for k, row in enumerate(rows):
            asend[kind, t, 0, pl.ds(k, 1)] = row
            gbuf[kind, t, core * 8 + eset, pl.ds(k, 1)] = row
        for c, m in group:
            tagged(asend.at[kind, t, 0], gbuf.at[kind, t, core * 8 + eset], AG + kind, t, flip_core(c), gpeer(m)).start()

    def g_sum(t, kind):
        came(gbuf.at[kind, t, others], AG + kind, t)
        both = [gbuf[kind, t, j] for j in range(RB)]
        return sum(both)[0:1], functools.reduce(jnp.maximum, both)[1:2]

    def r_send(t, kind, row):
        asend[kind, t, 1, pl.ds(0, 1)] = row
        rbuf[kind, t, aset, pl.ds(0, 1)] = row
        for m in SEVEN:
            tagged(asend.at[kind, t, 1], rbuf.at[kind, t, aset], AR + kind, t, core, rpeer(m)).start()

    def r_sum(t, kind):
        came(rbuf.at[kind, t, pl.ds(0, 7)], AR + kind, t)
        return sum(rbuf[kind, t, j] for j in EIGHT)[0:1]

    def mean(row):
        return jnp.sum(row, axis=1, keepdims=True) / elems

    def total(t, kind):
        row = r_sum(t, kind)
        sent(gbuf.at[kind, t, others], AG + kind, t)
        sent(rbuf.at[kind, t, pl.ds(0, 7)], AR + kind, t)
        return mean(row)

    def put(t, kind, val):
        scal[kind, t] = jnp.broadcast_to(val, (8, LN))

    def get(t, kind):
        return scal[kind, t][0:1, 0:1]

    def wide(tile, rows):
        return jnp.concatenate([jnp.concatenate([tile] * PH, axis=1)] * (rows // 8), axis=0)

    def record(kind, t, s, val):
        rows = lax.broadcasted_iota(jnp.int32, (2, STEPS), 0)
        cols = lax.broadcasted_iota(jnp.int32, (2, STEPS), 1)
        sums_out[kind] = jnp.where(jnp.logical_and(rows == t, cols == s), val, sums_out[kind])

    psi_ld = pltpu.make_async_copy(psi_ref, praw, ldsem.at[0])
    psi_ld.start()
    l_ld = pltpu.make_async_copy(left_ref, lst, ldsem.at[1])
    l_ld.start()
    r_ld = pltpu.make_async_copy(right_ref.at[:, pl.ds(pl.multiple_of(eset * EC, EC), EC)], rf, ldsem.at[2])
    r_ld.start()
    w_ld = pltpu.make_async_copy(mpo_ref, wraw, ldsem.at[3])
    w_ld.start()
    barrier = pltpu.get_barrier_semaphore()
    for c, m in group:
        pl.semaphore_signal(barrier, inc=1, device_id=(flip_core(c), gpeer(m)), device_id_type=MESH)
    for m in SEVEN:
        pl.semaphore_signal(barrier, inc=1, device_id=(core, rpeer(m)), device_id_type=MESH)
    psi_ld.wait()
    parts = []
    for t in BOTH:
        acc = 0
        for ij in range(PH):
            val = praw[t, :, ij // 2, ij % 2, :]
            pg[t, ij, myrows, mycols] = val
            acc = acc + val * val
        parts.append(fold(acc))
    sums_out[...] = jnp.zeros(sums_out.shape, F32)
    asend[...] = jnp.zeros(asend.shape, F32)
    pl.semaphore_wait(barrier, len(group) + len(SEVEN))
    for t in BOTH:
        g_send(t, NORM, parts[t])
    p_send(0)
    l_ld.wait()

    def perm_body(l, carry):
        lane = lax.broadcasted_iota(jnp.int32, (RB, LN), 1) // 32
        for hz in BOTH:
            for hy in BOTH:
                src = [lst[l, :, pl.ds((4 * hz + 2 * q + hy) * LN, LN)] for q in BOTH]
                for hx in BOTH:
                    pick = None
                    for c in range(PH):
                        shift = (c - 2 * (c % 2) - hx) * 32 % LN
                        val = pltpu.roll(src[c // 2], shift, 1) if shift else src[c // 2]
                        pick = val if pick is None else jnp.where(lane == c, val, pick)
                    rel = [p + q * (1 - 2 * p) for p, q in zip((hz, hy, hx), high)]
                    far = sum(rel) // 2
                    rank = [p + far * (1 - 2 * p) for p in rel]
                    j = 3 - (3 * rank[0] + 2 * rank[1] + rank[2])
                    one = sum(rel) % 2 - sum(rel) // 3
                    here, there = l // fifth % 2, sum(p * q for p, q in zip(rel, high))
                    skip = one * (here + there - 2 * here * there)
                    ls[1 - far, l + skip * (mpo - l), myrows, pl.ds(pl.multiple_of(j * LN, LN), LN)] = pick
        return carry

    lax.fori_loop(0, mpo, perm_body, 0)
    p_take(0, 0)
    l_pass(0, *SIDES)
    for t in BOTH:
        r_send(t, NORM, g_sum(t, NORM)[0])
    p_take(0, 1)
    l_pass(0, *MAINS[:1])
    w_ld.wait()
    for mn in range(PH):
        planes = [wraw[:, ij // 2, ij % 2, mn // 2, mn % 2, :] for ij in range(PH)]
        wst[pl.ds(mn, mpo, stride=PH), :] = jnp.concatenate(planes + [jnp.zeros((mpo, LN - PH * mpo), F32)], axis=1)
    w0, w1, w2 = split3(wst[:PH * mpo, :PH * mpo])
    none = jnp.zeros_like(w0)
    groups = [jnp.concatenate(g, axis=1) for g in ([w0] * 3, [w1, w1, none], [w2, none, none])]
    wpk[...] = jnp.concatenate(groups, axis=0)

    def l_take(level, *which):
        for u in which:
            n, _, count, _, lanes, j = pieces[u]
            part = members(j)[level]
            came_at(ls.at[n, pl.ds(0, count), pl.ds(0, RB * len(part)), pl.ds(0, lanes)], l_arrival(u, level))
            l_pass(level + 1, u)
            for m in part:
                lf_copy(u, m).start()

    def split_rows(n, lane, lanes, offsets):
        cols = pl.ds(lane, lanes)

        def split_body(l, carry):
            for m in offsets:
                rows = chip_rows(m)
                for k, part in enumerate(split3(ls[n, l, rows, cols])):
                    l3[k, n, l, rows, cols] = part
            return carry

        lax.fori_loop(0, mpo, split_body, 0, unroll=PH)

    def over(phase, part):
        came(l_bytes(phase, RB * len(part)), LF + phase, int(part is FAR))

    def ex_send():
        def turn_body(i, carry):
            for k in SHARES:
                xst[k, i] = ls[1, core * lhalf + fifth * high[k] + i, :, k * LN:(k + 1) * LN].T
            return carry

        lax.fori_loop(0, fifth, turn_body, 0)
        for k in SHARES:
            ex_copy(k).start()

    def ex_take():
        came(l_bytes(SIDE, LN), EX, 0)
        for k in SHARES:
            ex_over(k).start()

    def l_first():
        l_take(2, *SIDES)
        ex_send()
        over(MAIN, NEAR)
        split_rows(0, 0, WID, CLOSE)
        l_take(1, *(MAINS + DIAGS))
        p_send(1)
        ex_take()
        l_take(2, *MAINS)
        for part in (NEAR, FAR):
            over(SIDE, part)
        came(l_bytes(SIDE, LN), EX, 1)
        split_rows(1, 0, 3 * LN, CLOSE + FAR)
        over(MAIN, FAR)
        split_rows(0, 0, WID, FAR)
        p_take(1, 0)
        l_take(2, *DIAGS)

    def l_second():
        for part in (NEAR, FAR):
            over(DIAG, part)
        split_rows(1, 3 * LN, LN, CLOSE + FAR)
        for phase in SHARES:
            sent(l_bytes(phase, 7 * RB), LS + phase, 0)
            for k, part in enumerate((NEAR, FAR)):
                sent(l_bytes(phase, RB * len(part)), LF + phase, k)
        for k in BOTH:
            sent(l_bytes(SIDE, LN), EX, k)

    def ev_init(t):
        rinv = 1.0 / jnp.sqrt(total(t, NORM))
        put(t, BETA, jnp.zeros((1, 1), F32))
        for slot in BOTH:
            put(t, FAC + slot, jnp.ones((1, 1), F32))

        def turn(first):
            def tr_body(b, carry):
                rows = pl.ds(pl.multiple_of(first + b * LN, LN), LN)
                for ij in range(PH):
                    vec[t, 0, rows, ij * LN:(ij + 1) * LN] = pg[t, ij, :, rows].T * rinv
                vec[t, 1, rows] = jnp.zeros((LN, WID), F32)
                return carry

            lax.fori_loop(0, half // LN, tr_body, 0, unroll=PH)

        turn(core * half)
        came(half_psi, PF, t)
        turn(other * half)
        sent(seven_psi, PS, t)
        sent(half_psi, PF, t)

    def ev_sum(t, s, h, more):
        came(rsb.at[t, h], RS + h, t)
        hv = outb[t, 0, half_rows(h)] + sum(rsb[t, h, m - 1] for m in SEVEN)
        gat[t, gat_rows(0, h)] = hv
        if h:
            rows = pl.ds(pl.multiple_of(own, EC), EC)
            hv = gat[t, rows]
            g_send(t, ALPHA, fold(hv * vec[t, s % 2, rows]) * get(t, FAC + s % 2), fold(jnp.abs(hv), jnp.maximum))

        @pl.when(more)
        def _():
            for k, m in ((0, NEAR), (1, FAR[::-1]), (1, NEAR)) if h else ((0, FAR[::-1]),):
                for q in m:
                    g_copy(t, k, q).start()

        sent(rsb.at[t, h], RS + h, t)

    def new_w(t, s, first, count):
        cur, prev = s % 2, (s + 1) % 2
        rows = pl.ds(pl.multiple_of(first, EC), count)
        along, back = wide(scal[ALPHA, t] * scal[FAC + cur, t], count), wide(scal[BETA, t] * scal[FAC + prev, t], count)
        return gat[t, rows] - along * vec[t, cur, rows] - back * vec[t, prev, rows]

    def ev_mid(t):
        row, most = g_sum(t, ALPHA)
        r_send(t, ALPHA, row)
        put(t, SIZE, jnp.max(most, axis=1, keepdims=True))

    def ev_alpha(t, s):
        alpha = total(t, ALPHA)
        put(t, ALPHA, alpha)
        put(t, SIZE, jnp.maximum(get(t, SIZE), jnp.maximum(jnp.abs(alpha), get(t, BETA))))
        record(0, t, s, alpha)
        res = new_w(t, s, own, EC)
        g_send(t, BETA, fold(res * res))

        @pl.when(s == STEPS - 1)
        def _():
            for q in BOTH:
                pair = [res[:, j * LN:(j + 1) * LN] for j in (2 * q, 2 * q + 1)]
                fsend[t, q] = jnp.concatenate(pair, axis=0).T
            for m in SEVEN + (0,):
                f_copy(t, m).start()

    def ev_pass(t):
        r_send(t, BETA, g_sum(t, BETA)[0])

    def ev_fwd(t):
        for h in BOTH:
            came(seven_halves, GA + h, t)
        fw_copy(t).start()

    def ev_beta(t, s):
        beta = jnp.sqrt(total(t, BETA))
        put(t, BETA, beta)
        record(1, t, s, beta)
        put(t, FAC + (s + 1) % 2, get(t, SIZE) / beta)
        return beta

    def ev_scale(t, s):
        ev_beta(t, s - 1)
        fac = get(t, FAC + s % 2)
        for m in EIGHT:
            outb[t, m, half_rows(0)] = outb[t, m, half_rows(0)] * fac

    def vec_rows(t, s, first):
        size = scal[SIZE, t]
        rinv = wide(jnp.where(size > 0, 1.0 / size, 0.0), LN)
        for j in range(0, half, LN):
            vec[t, (s + 1) % 2, pl.ds(pl.multiple_of(first + j, LN), LN)] = new_w(t, s, first + j, LN) * rinv

    def ev_vec(t, s):
        fw_copy(t).wait_recv()
        vec_rows(t, s, other * half)
        fw_copy(t).wait_send()
        for h in BOTH:
            sent(seven_halves, GA + h, t)

    def rel(n, j):
        return FAR[j] + n * (CLOSE[j] - FAR[j])

    def r_phase(t, s, start, count, shift=0):
        xv = jnp.dot(rf[:, pl.ds(start + shift, count), :].reshape(mpo * count, bond), vec[t, s % 2], preferred_element_type=F32, precision=HI)
        for r in range(mpo):
            for ij in range(PH):
                xf[pl.ds((ij * mpo + r) * NX + shift, count), :] = xv[r * count:(r + 1) * count, ij * LN:(ij + 1) * LN]

    def w_phase(start):
        for e in range(0, EH, 2):
            xs = jnp.concatenate([xf[pl.ds(e + q, PH * mpo, stride=NX), :] for q in BOTH], axis=1)
            x0, x1, x2 = split3(xs)
            y0, y1, y2 = jnp.split(jnp.dot(wpk[...], jnp.concatenate([x0, x1, x2], axis=0), preferred_element_type=F32), 3)
            yv = (y2 + y1) + y0
            for q in BOTH:
                yf[pl.ds(start + e + q, PH * mpo, stride=NY), :] = yv[:, q * LN:(q + 1) * LN]

    def l_phase(t, h, n, fac):
        rows = [half_rows(h, (l * PH + mn) * NY) for l in range(mpo) for mn in range(PH)]
        lhs = [jnp.concatenate([yf[r, :] for r in rows[l * PH:l * PH + PH]], axis=0) for l in range(mpo)]
        y0, y1, y2 = split3(jnp.concatenate(lhs, axis=1))
        b0, b1, b2 = [l3[k, n].reshape(mpo * LN, PH * LN) for k in SHARES]
        p0 = jnp.dot(jnp.concatenate([y0, y1, y2], axis=0), b0, preferred_element_type=F32)
        p1 = jnp.dot(jnp.concatenate([y0, y1], axis=0), b1, preferred_element_type=F32)
        p2 = jnp.dot(y0, b2, preferred_element_type=F32)
        ov = ((p0[2 * LN:] + p1[LN:]) + p2) + (p0[LN:2 * LN] + p1[:LN]) + p0[:LN]
        if fac is not None:
            ov = ov * fac
        for j in range(PH):
            for mn in range(PH):
                outb[t, rel(n, j), half_rows(h), mn * LN:(mn + 1) * LN] = ov[mn * EH:(mn + 1) * EH, j * LN:(j + 1) * LN]

    def send_part(t, h, part):
        for m in part:
            rs_copy(t, h, m).start()

    quarter = EH // 2

    def step_body(it, carry):
        t, s = it % 2, it // 2
        ot = 1 - t
        os = (it + 1) // 2 - 1
        more = it < 2 * STEPS - 1
        later = it >= 2

        @pl.when(it == 1)
        def _():
            ev_init(t)

        @pl.when(later)
        def _():
            ev_vec(t, s - 1)

        r_phase(t, s, 0, quarter)

        @pl.when(later)
        def _():
            ev_pass(t)

        ev_sum(ot, os, 0, more)
        r_phase(t, s, 0, quarter, quarter)
        w_phase(0)
        l_phase(t, 0, 0, None)
        ev_sum(ot, os, 1, more)
        l_phase(t, 0, 1, None)
        r_phase(t, s, EH, quarter)
        ev_mid(ot)

        @pl.when(later)
        def _():
            ev_scale(t, s)

        send_part(t, 0, SEVEN)

        r_phase(t, s, EH, quarter, quarter)
        w_phase(EH)
        l_phase(t, 1, 0, get(t, FAC + s % 2))
        ev_alpha(ot, os)

        @pl.when(more)
        def _():
            ev_fwd(ot)

        send_part(t, 1, FAR[::-1])
        vec_rows(ot, os, core * half)
        l_phase(t, 1, 1, get(t, FAC + s % 2))
        send_part(t, 1, NEAR)
        return carry

    p_take(0, 2)
    l_take(0, *SIDES)
    l_pass(0, *(MAINS[1:] + DIAGS))
    ev_init(0)
    r_ld.wait()

    def first_rw(h, carry):
        start = pl.multiple_of(h * EH, EH)
        r_phase(0, 0, start, quarter)

        @pl.when(h == 1)
        def _():
            l_take(0, *(MAINS + DIAGS))

        r_phase(0, 0, start, quarter, quarter)
        w_phase(start)

        @pl.when(h == 0)
        def _():
            l_take(1, *SIDES)

        return carry

    lax.fori_loop(0, 2, first_rw, 0)
    l_first()

    def first_l(q, carry):
        n, h = q // 2, q % 2

        @pl.when(q == 2)
        def _():
            l_second()

        l_phase(0, h, n, None)
        for j in SHARES:
            rs_copy(0, h, rel(n, j)).start()

        @pl.when(n == 0)
        def _():
            rs_copy(0, h, FAR[3]).start()

        @pl.when(q == 1)
        def _():
            p_take(1, 1)

        @pl.when(q == 2)
        def _():
            p_take(1, 2)

        return carry

    lax.fori_loop(0, 4, first_l, 0)
    lax.fori_loop(1, 2 * STEPS, step_body, 0)

    last = STEPS - 1

    def finish(t):
        ev_beta(t, last)
        came(seven_fin, FI, t)
        sent(seven_fin, FI, t)
        f_copy(t, 0).wait()

    ev_pass(0)
    ev_sum(1, last, 0, False)
    ev_sum(1, last, 1, False)
    ev_mid(1)
    finish(0)
    ev_alpha(1, last)
    ev_pass(1)
    finish(1)


def output_kernel(rows_ref, sums_ref, alpha_out, beta_out, psi_out):
    alpha_out[...] = sums_ref[0]
    beta_out[...] = sums_ref[1]
    for t in BOTH:
        rinv = 1.0 / sums_ref[1, t:t + 1, STEPS - 1:STEPS]
        for i in BOTH:
            for j in BOTH:
                psi_out[t, :, i, j, :] = jnp.concatenate([rows_ref[t, g, i][:, j * EC:(j + 1) * EC] for g in EIGHT], axis=1) * rinv


def solution(mesh):
    psi_spec = P(None, "lb", None, None, "rb")

    def local_run(psi_loc, left_loc, right_loc, mpo_pair):
        rows = psi_loc.shape[1]
        mpo, bond = left_loc.shape[1:]
        left_t = jnp.transpose(left_loc, (1, 0, 2))
        right_t = jnp.transpose(right_loc, (1, 0, 2))
        mpo_t = jnp.transpose(mpo_pair, (0, 2, 3, 4, 5, 1))
        dma = pltpu.SemaphoreType.DMA
        any_spec = pl.BlockSpec(memory_space=pl.ANY)
        vm = pl.BlockSpec(memory_space=pltpu.VMEM)
        f32_shapes = [
            (mpo, EC, bond),
            (2, mpo + 1, LN, WID),
            (mpo, rows, bond),
            (2, bond, WID),
            (2, 2, bond, WID),
            (2, PH, LN, bond),
            psi_loc.shape,
            mpo_t.shape,
            (PH * mpo + EC, LN),
            (PH * mpo * NX + EC, LN),
            (PH * mpo * NY + EC, LN),
            (2, 8, EC, WID),
            (2, 2, 7, EH, WID),
            (3, mpo // 4, LN, LN),
        ]
        small = [(3, 2, k, 2, LN) for k in (RB, 8, 2)] + [(SIZE + 1, 2, 8, LN), (2, 2, LN, LN)]
        call = pl.pallas_call(
            functools.partial(kernel, (bond, mpo, float(bond * bond * PH))),
            out_shape=[jax.ShapeDtypeStruct(shape, F32) for shape in ((2, len(EIGHT), 2, rows, LN), (2, 2, STEPS))],
            in_specs=[any_spec] * 4,
            out_specs=[any_spec, vm],
            scratch_shapes=[pltpu.VMEM(shape, F32) for shape in f32_shapes]
            + [pltpu.VMEM((3, 2, mpo, LN, WID), BF16), pltpu.VMEM((3 * PH * mpo, 3 * PH * mpo), BF16)]
            + [pltpu.VMEM(shape, F32) for shape in small]
            + [dma((LS + 3, 2)), dma((KINDS, 2))]
            + [dma((4,))],
            compiler_params=pltpu.CompilerParams(vmem_limit_bytes=63 << 20, has_side_effects=True, collective_id=0),
            name="lanczos",
        )
        last_rows, sums = call(psi_loc, left_t, right_t, mpo_t)
        shapes = [(2, STEPS), (2, STEPS), psi_loc.shape]
        put_out = pl.pallas_call(
            output_kernel,
            out_shape=[jax.ShapeDtypeStruct(shape, F32) for shape in shapes],
            in_specs=[vm] * 2,
            out_specs=[vm] * 3,
            name="outputs",
        )
        return put_out(last_rows, sums)

    return jax.shard_map(local_run, mesh=mesh, in_specs=(psi_spec, P("lb", None, None), P("rb", None, None), P()), out_specs=(P(), P(), psi_spec), check_vma=False)
```
